32 devices in a mesh: dp: 8 (over y, x, core), tp: 4 (over z).
Axes of the slice: x: 2, y: 2, z: 4, core: 2. Of those that a mesh axis runs over, the one named last changes fastest.
Arguments:
- tokens: bfloat16 [4096, 1536], P(('dp', 'tp')), may hold values from -6 to 6
- positions: int32 [4096], P('dp'), may hold values from 0 to 1023, as said below
- attn_gain: float32 [1536], replicated, may hold values from 0.5 to 1.5
- w_query: bfloat16 [1536, 1536], P('dp', 'tp'), may hold values from -1 to 1
- w_key: bfloat16 [1536, 768], P('dp', 'tp'), may hold values from -1 to 1
- w_value: bfloat16 [1536, 768], P('dp', 'tp'), may hold values from -0.15625 to 0.15625
- w_out: bfloat16 [1536, 1536], P('tp', 'dp'), may hold values from -1.25 to 1.25
- ffn_gain: float32 [1536], replicated, may hold values from 0.5 to 1.5
- w_gate: bfloat16 [1536, 4096], P('dp', 'tp'), may hold values from -0.15625 to 0.15625
- w_up: bfloat16 [1536, 4096], P('dp', 'tp'), may hold values from -0.15625 to 0.15625
- w_down: bfloat16 [4096, 1536], P('tp', 'dp'), may hold values from -0.09375 to 0.09375
- out_grad: bfloat16 [4096, 1536], P(('dp', 'tp')), may hold values from -18 to 18
Outputs:
- output: bfloat16 [4096, 1536], P(('dp', 'tp'))
- tokens_grad: float32 [4096, 1536], P(('dp', 'tp'))
- attn_gain_grad: float32 [1536], replicated
- w_query_grad: float32 [1536, 1536], P('dp', 'tp')
- w_key_grad: float32 [1536, 768], P('dp', 'tp')
- w_value_grad: float32 [1536, 768], P('dp', 'tp')
- w_out_grad: float32 [1536, 1536], P('tp', 'dp')
- ffn_gain_grad: float32 [1536], replicated
- w_gate_grad: float32 [1536, 4096], P('dp', 'tp')
- w_up_grad: float32 [1536, 4096], P('dp', 'tp')
- w_down_grad: float32 [4096, 1536], P('tp', 'dp')
The draws below stay inside these ranges and needn't reach their ends.
Inputs may be any that keep to these rules, and one draw needn't show every extreme that they name: `positions`: documents are runs of consecutive tokens; a token at position 0 begins a document, any other follows the token before it in the same document; no document is longer than 1024 tokens and one has exactly 1024.
All inputs are finite; a program needn't handle non-finite values.
Results may differ from the reference program's by a relative error of at most 0.014.
The reference program's roundings to bfloat16 on the way count: a program that leaves them out, or rounds other values in their place, can miss the bound.
Values may be sent and summed in bfloat16 or wider, within the bound.
A program may use at most 128 MiB of HBM per device.

```python
import math
import jax
import jax.numpy as jnp
from jax import lax

D = 1536
HQ = 16
HK = 8
HD = 96
FF = 4096
SPAN = 512
TOKENS = 4096
DOC_MAX = 1024


def drawn_weight(key, salt, columns):
    base_draw = jnp.clip(jax.random.normal(jax.random.fold_in(key, salt), (D, columns), jnp.float32), -4.0, 4.0)
    return base_draw / math.sqrt(D)


def draw_positions(key, part):
    doc_lengths = jax.random.randint(jax.random.fold_in(key, 11), (TOKENS,), 1, DOC_MAX + 1)
    long_doc = jax.random.randint(jax.random.fold_in(key, 12), (), 0, TOKENS // DOC_MAX)
    doc_lengths = jnp.where(jnp.arange(TOKENS) == long_doc, DOC_MAX, doc_lengths).astype(jnp.int32)
    doc_ends = jnp.cumsum(doc_lengths).astype(jnp.int32)
    token_ids = jnp.arange(TOKENS, dtype=jnp.int32)
    doc_index = jnp.searchsorted(doc_ends, token_ids, side='right')
    doc_starts = jnp.take(doc_ends - doc_lengths, doc_index)
    return (token_ids - doc_starts).astype(jnp.int32)


def draw_tokens(key, part):
    base_draw = jnp.clip(jax.random.normal(jax.random.fold_in(key, 21), (TOKENS, D), jnp.float32), -6.0, 6.0)
    return base_draw.astype(jnp.bfloat16)


def draw_w_query(key, part):
    base_draw = drawn_weight(key, 41, HQ * HD)
    return base_draw.astype(jnp.bfloat16)


def draw_w_key(key, part):
    base_draw = drawn_weight(key, 51, HK * HD)
    return base_draw.astype(jnp.bfloat16)


def draw_out_grad(key, part):
    row_ramp = 1.0 + 2.0 * jnp.arange(TOKENS, dtype=jnp.float32) / (TOKENS - 1)
    noise_draw = jnp.clip(jax.random.normal(jax.random.fold_in(key, 31), (TOKENS, D), jnp.float32), -6.0, 6.0)
    return (noise_draw * row_ramp[:, None]).astype(jnp.bfloat16)


def steps_of(rng, shape, cuts, smallest, largest):
    level = 1.0
    for dim, shards_of in cuts:
        steps = jax.random.uniform(jax.random.fold_in(jax.random.fold_in(rng, 6), dim), (shards_of,), jnp.float32, smallest / len(cuts), largest / len(cuts))
        level = level * jnp.repeat(jnp.exp(steps), shape[dim] // shards_of).reshape((-1,) + (1,) * (len(shape) - 1 - dim))
    return level


def noise(stream_key, shape, spread, limit, pieces=(), kind=jnp.bfloat16):
    level = steps_of(stream_key, shape, pieces, -0.22, 0.18) if pieces else 1.0
    array = jax.random.normal(stream_key, shape, jnp.float32) * spread * level
    return jnp.minimum(jnp.maximum(array, -limit), limit).astype(kind)


def setup_inputs(seed: int = 0) -> dict:
    streams_of = jax.random.split(jax.random.key(seed), 13)
    return {
        "tokens": draw_tokens(jax.random.fold_in(streams_of[12], 71), 0),
        "positions": draw_positions(jax.random.fold_in(streams_of[12], 71), 0),
        "attn_gain": jnp.clip(1.0 + 0.1 * jax.random.normal(streams_of[2], (D,), jnp.float32), 0.5, 1.5),
        "w_query": draw_w_query(jax.random.fold_in(streams_of[12], 71), 0),
        "w_key": draw_w_key(jax.random.fold_in(streams_of[12], 71), 0),
        "w_value": noise(streams_of[5], (D, HK * HD), D ** -0.5, 0.15625, ((0, 8), (1, 4))),
        "w_out": noise(streams_of[6], (HQ * HD, D), (D // 64) ** -0.5, 1.25, ((0, 4), (1, 8))),
        "ffn_gain": jnp.clip(1.0 + 0.1 * jax.random.normal(streams_of[7], (D,), jnp.float32), 0.5, 1.5),
        "w_gate": noise(streams_of[8], (D, FF), D ** -0.5, 0.15625, ((0, 8), (1, 4))),
        "w_up": noise(streams_of[9], (D, FF), D ** -0.5, 0.15625, ((0, 8), (1, 4))),
        "w_down": noise(streams_of[10], (FF, D), FF ** -0.5, 0.09375, ((0, 4), (1, 8))),
        "out_grad": draw_out_grad(jax.random.fold_in(streams_of[12], 71), 0),
    }


norm_eps = 1e-05
rope_base = 100000.0
masked_score = -1e+30

def rope_tables(position_ids, head_size):
    half_size = head_size // 2
    inverse = rope_base ** (-(jnp.arange(half_size, dtype=jnp.float32) * 2.0 / head_size))
    angles = position_ids.astype(jnp.float32)[:, None] * inverse[None, :]
    return (jnp.cos(angles), jnp.sin(angles))

def rotate_fwd(values, cosine, sine_part):
    half_size = values.shape[-1] // 2
    first_half = values[..., :half_size]
    second_half = values[..., half_size:]
    cos_rows = cosine[:, None, :]
    sin_rows = sine_part[:, None, :]
    return jnp.concatenate([first_half * cos_rows - second_half * sin_rows, second_half * cos_rows + first_half * sin_rows], axis=-1)

def rotate_back(grad_in, cosine, sine_part):
    half_size = grad_in.shape[-1] // 2
    first_half = grad_in[..., :half_size]
    second_half = grad_in[..., half_size:]
    cos_rows = cosine[:, None, :]
    sin_rows = sine_part[:, None, :]
    return jnp.concatenate([first_half * cos_rows + second_half * sin_rows, second_half * cos_rows - first_half * sin_rows], axis=-1)

def rms_parts(values):
    inverse = lax.rsqrt(lax.optimization_barrier(jnp.mean(values * values, axis=-1, keepdims=True)) + norm_eps)
    return (values * inverse, inverse)

def rms_back(grad_in, normed, inverse, gain_vec):
    scaled = grad_in * gain_vec
    return inverse * (scaled - normed * lax.optimization_barrier(jnp.mean(scaled * normed, axis=-1, keepdims=True)))

def block_scores(query_block, key_window, query_ids, doc_starts, key_ids):
    scale_factor = 1.0 / math.sqrt(query_block.shape[-1])
    scores = jnp.einsum('rkgd,skd->kgrs', query_block.astype(jnp.float32), key_window.astype(jnp.float32)) * scale_factor
    allowed = (key_ids[None, :] >= doc_starts[:, None]) & (key_ids[None, :] <= query_ids[:, None])
    return jnp.where(allowed[None, None], scores, masked_score)

def attend_fwd(query_block, key_window, value_window, query_ids, doc_starts, key_ids):
    scores = block_scores(query_block, key_window, query_ids, doc_starts, key_ids)
    row_max = lax.optimization_barrier(jnp.max(scores, axis=-1, keepdims=True))
    weights = jnp.exp(scores - row_max)
    row_total = lax.optimization_barrier(jnp.sum(weights, axis=-1, keepdims=True))
    probs_low = (weights / row_total).astype(jnp.bfloat16)
    log_total = (row_max + jnp.log(row_total))[..., 0]
    context = jnp.einsum('kgrs,skd->rkgd', probs_low.astype(jnp.float32), value_window.astype(jnp.float32))
    return (context.astype(jnp.bfloat16), log_total)

def attend_back(query_block, key_window, value_window, context, log_total, context_grad, query_ids, doc_starts, key_ids):
    scale_factor = 1.0 / math.sqrt(query_block.shape[-1])
    scores = block_scores(query_block, key_window, query_ids, doc_starts, key_ids)
    probs = jnp.exp(scores - log_total[..., None])
    probs_low = probs.astype(jnp.bfloat16)
    grad_f = context_grad.astype(jnp.float32)
    prob_grad = jnp.einsum('rkgd,skd->kgrs', grad_f, value_window.astype(jnp.float32))
    row_delta = jnp.transpose(lax.optimization_barrier(jnp.sum(grad_f * context.astype(jnp.float32), axis=-1)), (1, 2, 0))
    score_low = (probs * (prob_grad - row_delta[..., None])).astype(jnp.bfloat16)
    query_grad = scale_factor * jnp.einsum('kgrs,skd->rkgd', score_low.astype(jnp.float32), key_window.astype(jnp.float32))
    key_grad = scale_factor * jnp.einsum('kgrs,rkgd->skd', score_low.astype(jnp.float32), query_block.astype(jnp.float32))
    value_grad = jnp.einsum('kgrs,rkgd->skd', probs_low.astype(jnp.float32), grad_f)
    return (query_grad, key_grad, value_grad)

def reference(tokens, positions, attn_gain, w_query, w_key, w_value, w_out, ffn_gain, w_gate, w_up, w_down, out_grad):
    group_size = HQ // HK
    block_rows = min(512, SPAN)
    block_count = TOKENS // block_rows
    tokens_f = tokens.astype(jnp.float32)
    normed1, inverse1 = rms_parts(tokens_f)
    hidden1 = (normed1 * attn_gain).astype(jnp.bfloat16)
    queries = jnp.dot(hidden1, w_query, preferred_element_type=jnp.float32)
    keys_raw = jnp.dot(hidden1, w_key, preferred_element_type=jnp.float32)
    values_raw = jnp.dot(hidden1, w_value, preferred_element_type=jnp.float32)
    cosine, sine_part = rope_tables(positions, HD)
    query_rot = rotate_fwd(queries.reshape(TOKENS, HQ, HD), cosine, sine_part).astype(jnp.bfloat16).reshape(TOKENS, HK, group_size, HD)
    key_rot = rotate_fwd(keys_raw.reshape(TOKENS, HK, HD), cosine, sine_part).astype(jnp.bfloat16)
    value_low = values_raw.reshape(TOKENS, HK, HD).astype(jnp.bfloat16)
    pad_rows = jnp.zeros((2 * SPAN, HK, HD), jnp.bfloat16)
    key_padded = jnp.concatenate([pad_rows, key_rot], axis=0)
    value_padded = jnp.concatenate([pad_rows, value_low], axis=0)
    token_ids = jnp.arange(TOKENS, dtype=jnp.int32)
    doc_begin = token_ids - positions

    def window_of(block_index):
        row_start = (block_index * block_rows).astype(jnp.int32)
        span_start = (row_start // SPAN * SPAN).astype(jnp.int32)
        query_ids = row_start + jnp.arange(block_rows, dtype=jnp.int32)
        key_ids = span_start - 2 * SPAN + jnp.arange(3 * SPAN, dtype=jnp.int32)
        query_block = lax.dynamic_slice_in_dim(query_rot, row_start, block_rows, 0)
        key_window = lax.dynamic_slice_in_dim(key_padded, span_start, 3 * SPAN, 0)
        value_window = lax.dynamic_slice_in_dim(value_padded, span_start, 3 * SPAN, 0)
        doc_starts = lax.dynamic_slice_in_dim(doc_begin, row_start, block_rows, 0)
        return (row_start, span_start, query_block, key_window, value_window, query_ids, doc_starts, key_ids)

    def forward_block(block_index):
        row_start, span_start, query_block, key_window, value_window, query_ids, doc_starts, key_ids = window_of(block_index)
        return attend_fwd(query_block, key_window, value_window, query_ids, doc_starts, key_ids)
    contexts, log_totals = lax.map(forward_block, jnp.arange(block_count, dtype=jnp.int32))
    context = contexts.reshape(TOKENS, HQ * HD)
    attn_out = jnp.dot(context, w_out, preferred_element_type=jnp.float32)
    residual = tokens_f + attn_out
    normed2, inverse2 = rms_parts(residual)
    hidden2 = (normed2 * ffn_gain).astype(jnp.bfloat16)
    gate_pre = jnp.dot(hidden2, w_gate, preferred_element_type=jnp.float32)
    up_proj = jnp.dot(hidden2, w_up, preferred_element_type=jnp.float32)
    sigmoid_gate = jax.nn.sigmoid(gate_pre)
    inner_act = (gate_pre * sigmoid_gate * up_proj).astype(jnp.bfloat16)
    ffn_out = jnp.dot(inner_act, w_down, preferred_element_type=jnp.float32)
    output = (residual + ffn_out).astype(jnp.bfloat16)
    inner_grad = jnp.dot(out_grad, w_down.T, preferred_element_type=jnp.float32)
    w_down_grad = jnp.dot(inner_act.T, out_grad, preferred_element_type=jnp.float32)
    silu_slope = sigmoid_gate * (1.0 + gate_pre * (1.0 - sigmoid_gate))
    gate_low = (inner_grad * up_proj * silu_slope).astype(jnp.bfloat16)
    up_low = (inner_grad * gate_pre * sigmoid_gate).astype(jnp.bfloat16)
    w_gate_grad = jnp.dot(hidden2.T, gate_low, preferred_element_type=jnp.float32)
    w_up_grad = jnp.dot(hidden2.T, up_low, preferred_element_type=jnp.float32)
    hidden2_grad = jnp.dot(gate_low, w_gate.T, preferred_element_type=jnp.float32) + jnp.dot(up_low, w_up.T, preferred_element_type=jnp.float32)
    ffn_gain_grad = lax.optimization_barrier(jnp.sum(hidden2_grad * normed2, axis=0))
    residual_grad = out_grad.astype(jnp.float32) + rms_back(hidden2_grad, normed2, inverse2, ffn_gain)
    residual_low = residual_grad.astype(jnp.bfloat16)
    w_out_grad = jnp.dot(context.T, residual_low, preferred_element_type=jnp.float32)
    context_grad = jnp.dot(residual_low, w_out.T, preferred_element_type=jnp.float32).astype(jnp.bfloat16).reshape(TOKENS, HK, group_size, HD)
    context_heads = contexts.reshape(TOKENS, HK, group_size, HD)

    def backward_block(carry, block_index):
        key_acc, value_acc = carry
        row_start, span_start, query_block, key_window, value_window, query_ids, doc_starts, key_ids = window_of(block_index)
        context_block = lax.dynamic_slice_in_dim(context_heads, row_start, block_rows, 0)
        grad_block = lax.dynamic_slice_in_dim(context_grad, row_start, block_rows, 0)
        query_grad, key_grad, value_grad = attend_back(query_block, key_window, value_window, context_block, log_totals[block_index], grad_block, query_ids, doc_starts, key_ids)
        key_acc = lax.dynamic_update_slice_in_dim(key_acc, lax.dynamic_slice_in_dim(key_acc, span_start, 3 * SPAN, 0) + key_grad, span_start, 0)
        value_acc = lax.dynamic_update_slice_in_dim(value_acc, lax.dynamic_slice_in_dim(value_acc, span_start, 3 * SPAN, 0) + value_grad, span_start, 0)
        return ((key_acc, value_acc), query_grad)
    zero_acc = jnp.zeros((TOKENS + 2 * SPAN, HK, HD), jnp.float32)
    (key_acc, value_acc), query_grads = lax.scan(backward_block, (zero_acc, zero_acc), jnp.arange(block_count, dtype=jnp.int32))
    query_low = rotate_back(query_grads.reshape(TOKENS, HQ, HD), cosine, sine_part).astype(jnp.bfloat16).reshape(TOKENS, HQ * HD)
    key_low = rotate_back(key_acc[2 * SPAN:], cosine, sine_part).astype(jnp.bfloat16).reshape(TOKENS, HK * HD)
    value_grad_low = value_acc[2 * SPAN:].astype(jnp.bfloat16).reshape(TOKENS, HK * HD)
    w_query_grad = jnp.dot(hidden1.T, query_low, preferred_element_type=jnp.float32)
    w_key_grad = jnp.dot(hidden1.T, key_low, preferred_element_type=jnp.float32)
    w_value_grad = jnp.dot(hidden1.T, value_grad_low, preferred_element_type=jnp.float32)
    hidden1_grad = jnp.dot(query_low, w_query.T, preferred_element_type=jnp.float32) + jnp.dot(key_low, w_key.T, preferred_element_type=jnp.float32) + jnp.dot(value_grad_low, w_value.T, preferred_element_type=jnp.float32)
    attn_gain_grad = lax.optimization_barrier(jnp.sum(hidden1_grad * normed1, axis=0))
    tokens_grad = residual_grad + rms_back(hidden1_grad, normed1, inverse1, attn_gain)
    return (output, tokens_grad, attn_gain_grad, w_query_grad, w_key_grad, w_value_grad, w_out_grad, ffn_gain_grad, w_gate_grad, w_up_grad, w_down_grad)
```

```python
import functools
import math

import jax
import jax.numpy as jnp
from jax import lax
from jax.experimental import pallas as pl
from jax.experimental.pallas import tpu as pltpu
from jax.sharding import PartitionSpec as P

HD = 96
norm_eps = 1e-05
rope_base = 100000.0
masked_score = -1e30

MESH = pl.DeviceIdType.MESH
VMEM = pltpu.VMEM
DMA = pltpu.SemaphoreType.DMA
LEVELS = 32000.0


class Stage:
    def __init__(self, name, cid, nd, nt):
        self.name, self.cid, self.nd, self.nt = name, cid, nd, nt
        self.ins, self.outs, self.scr, self.tasks, self.links = [], [], [], [], set()

    def inp(self, x, space=VMEM):
        self.ins.append((x, space))
        return ("i", len(self.ins) - 1)

    def out(self, shape, dtype, space=VMEM):
        self.outs.append((shape, dtype, space))
        return ("o", len(self.outs) - 1)

    def scratch(self, spec):
        self.scr.append(spec)
        return ("s", len(self.scr) - 1)

    def task(self, links, gen):
        self.links |= set(links)
        self.tasks.append(gen)

    def _barrier(self):
        d, t = lax.axis_index("dp"), lax.axis_index("tp")
        nd, nt = self.nd, self.nt
        sem = pltpu.get_barrier_semaphore()
        count = 0

        def greet(ok, where):
            if ok is True:
                pl.semaphore_signal(sem, inc=1, device_id=where, device_id_type=MESH)
                return 1

            @pl.when(ok)
            def _():
                pl.semaphore_signal(sem, inc=1, device_id=where, device_id_type=MESH)

            return ok.astype(jnp.int32)

        if "line" in self.links:
            count += greet(t > 0, {"tp": t - 1})
            count += greet(t < nt - 1, {"tp": t + 1})
        if "chips" in self.links:
            for i in range(1, nd // 2):
                count += greet(True, {"dp": lax.rem(d + 2 * i, nd)})
        if "twin" in self.links:
            count += greet(True, {"dp": d + 1 - 2 * lax.rem(d, 2)})
        if "near" in self.links:
            for i in (1, 2):
                count += greet(d >= i, {"dp": d - i})
                count += greet(d < nd - i, {"dp": d + i})
        if "tp" in self.links:
            for i in range(1, nt):
                count += greet(True, {"tp": lax.rem(t + i, nt)})
        if "dp" in self.links:
            for i in range(1, nd):
                count += greet(True, {"dp": lax.rem(d + i, nd)})
        pl.semaphore_wait(sem, count)

    def run(self):
        n_in, n_out = len(self.ins), len(self.outs)

        def kernel(*refs):
            def get(h):
                kind, i = h
                return refs[i + {"i": 0, "o": n_in, "s": n_in + n_out}[kind]]

            self._barrier()
            live = [g(get) for g in self.tasks]
            while live:
                still = []
                for g in live:
                    try:
                        next(g)
                        still.append(g)
                    except StopIteration:
                        pass
                live = still

        return pl.pallas_call(
            kernel,
            out_shape=[jax.ShapeDtypeStruct(s, t) for s, t, _ in self.outs],
            in_specs=[pl.BlockSpec(memory_space=sp) for _, sp in self.ins],
            out_specs=[pl.BlockSpec(memory_space=sp) for _, _, sp in self.outs],
            scratch_shapes=self.scr,
            compiler_params=pltpu.CompilerParams(
                collective_id=self.cid, has_side_effects=True, vmem_limit_bytes=48 << 20
            ),
            name=self.name,
        )(*[x for x, _ in self.ins])


def remote(src, dst, send, recv, where):
    return pltpu.make_async_remote_copy(
        src_ref=src, dst_ref=dst, send_sem=send, recv_sem=recv, device_id=where, device_id_type=MESH
    )


def when(ok, fn):
    if ok is True:
        fn()
    elif ok is not False:
        pl.when(ok)(fn)


def over_cols(width, fn):
    def body(c, _):
        fn(pl.ds(pl.multiple_of(c * 128, 128), 128))
        return 0

    lax.fori_loop(0, width // 128, body, 0)
    if width % 128:
        fn(pl.ds(width // 128 * 128, width % 128))


def row_encode(read, code, scale, rows):
    step = 16

    def body(i, held):
        r = pl.multiple_of(i * step, step)
        x = read(r, step)
        top = jnp.max(jnp.abs(x), axis=-1, keepdims=True)
        code[pl.ds(r, step), :] = jnp.round(x * (LEVELS / jnp.maximum(top, 1e-30))).astype(jnp.int32).astype(jnp.int16)
        lane = lax.broadcasted_iota(jnp.int32, (step, 128), 1)
        row = lax.broadcasted_iota(jnp.int32, (step, 128), 0) + r
        mine = jnp.sum(jnp.where(lane == row, jnp.maximum(top, 1e-30) * (1.0 / LEVELS), 0.0), axis=0, keepdims=True)
        return held + jnp.broadcast_to(mine, (8, 128))

    scale[...] = lax.fori_loop(0, rows // step, body, jnp.zeros((8, 128), jnp.float32))


def row_decode(code, scale, r, step):
    lane = lax.broadcasted_iota(jnp.int32, (step, 128), 1)
    row = lax.broadcasted_iota(jnp.int32, (step, 128), 0) + r
    col = jnp.sum(jnp.where(lane == row, jnp.broadcast_to(scale[0:1, :], (step, 128)), 0.0), axis=-1, keepdims=True)
    return code[pl.ds(r, step), :].astype(jnp.int32).astype(jnp.float32) * col


def col_encode(x, code, scale, cols):
    top = jnp.maximum(jnp.max(jnp.abs(x), axis=0, keepdims=True), 1e-30)
    code[:, cols] = jnp.round(x * (LEVELS / top)).astype(jnp.int32).astype(jnp.int16)
    scale[:, cols] = top * (1.0 / LEVELS)


def col_decode(code, scale, cols):
    return code[:, cols].astype(jnp.int32).astype(jnp.float32) * scale[:, cols]


def line_gather(st, x):
    nt = st.nt
    rows, width = x.shape
    hx = st.inp(x)
    ho = st.out((nt, rows, width), x.dtype, pl.ANY)
    parts = 2
    hs = st.scratch(DMA((2, nt, parts)))
    hr = st.scratch(DMA((2, nt, parts)))
    hl = st.scratch(DMA((1,)))

    def gen(get):
        x_ref, o_ref, ss, rs, ls = get(hx), get(ho), get(hs), get(hr), get(hl)
        t = lax.axis_index("tp")
        chunk = rows // parts
        own = pltpu.make_async_copy(x_ref, o_ref.at[t], ls.at[0])
        own.start()

        def hop(src, owner, k, s, p, where):
            piece = pl.ds(p * chunk, chunk)
            return remote(src.at[piece], o_ref.at[owner, piece], ss.at[k, s, p], rs.at[k, s, p], {"tp": where})

        def send(s, p, k, way):
            owner, where = t - s * way, t + way
            ok = (owner >= 0) & (owner < nt) & (where >= 0) & (where < nt)
            src = x_ref if s == 0 else o_ref.at[owner]
            when(ok, lambda: hop(src, owner, k, s, p, where).start())

        for p in range(parts):
            for k, way in enumerate((1, -1)):
                send(0, p, k, way)
        yield
        for s in range(nt - 1):
            for p in range(parts):
                for k, way in enumerate((1, -1)):
                    owner = t - way * (s + 1)
                    ok = (owner >= 0) & (owner < nt)
                    when(ok, lambda: hop(x_ref, owner, k, s, p, t).wait_recv())
                    if s < nt - 2:
                        send(s + 1, p, k, way)
                yield
        for s in range(nt - 1):
            for p in range(parts):
                for k, way in enumerate((1, -1)):
                    owner, where = t - s * way, t + way
                    ok = (owner >= 0) & (owner < nt) & (where >= 0) & (where < nt)
                    when(ok, lambda: hop(x_ref, owner, k, s, p, where).wait_send())
        own.wait()

    st.task(("line",), gen)
    return ho


def line_scatter(st, part):
    nt = st.nt
    total, width = part.shape
    rows = total // nt
    parts = 2
    chunk = rows // parts
    hx = st.inp(part)
    ho = st.out((rows, width), jnp.float32)
    hcs = st.scratch(VMEM((2, nt - 1, parts, chunk, width), jnp.int16))
    hcr = st.scratch(VMEM((2, nt - 1, parts, chunk, width), jnp.int16))
    hss = st.scratch(VMEM((2, nt - 1, parts, 8, 128), jnp.float32))
    hsr = st.scratch(VMEM((2, nt - 1, parts, 8, 128), jnp.float32))
    hs = st.scratch(DMA((2, nt - 1, parts, 2)))
    hr = st.scratch(DMA((2, nt - 1, parts, 2)))

    def gen(get):
        x_ref, o_ref, cs, cr, sc, sr, ss, rs = (get(h) for h in (hx, ho, hcs, hcr, hss, hsr, hs, hr))
        t = lax.axis_index("tp")

        def hops(k, s, p, where):
            return (
                remote(cs.at[k, s, p], cr.at[k, s, p], ss.at[k, s, p, 0], rs.at[k, s, p, 0], {"tp": where}),
                remote(sc.at[k, s, p], sr.at[k, s, p], ss.at[k, s, p, 1], rs.at[k, s, p, 1], {"tp": where}),
            )

        def mine(base, r, n):
            return x_ref[pl.ds(pl.multiple_of(base + r, n), n), :]

        for s in range(nt - 1):
            for p in range(parts):
                for k, way in enumerate((1, -1)):
                    j = nt - 1 - s if way == 1 else s
                    base = j * rows + p * chunk
                    first = t == (0 if way == 1 else nt - 1)
                    passing = (t < j) if way == 1 else (t > j)

                    def send():
                        for c in hops(k, s, p, t + way):
                            c.start()

                    def start():
                        row_encode(lambda r, n: mine(base, r, n), cs.at[k, s, p], sc.at[k, s, p], chunk)
                        send()

                    def relay():
                        for c in hops(k, s, p, t):
                            c.wait_recv()
                        row_encode(
                            lambda r, n: mine(base, r, n) + row_decode(cr.at[k, s, p], sr.at[k, s, p], r, n),
                            cs.at[k, s, p],
                            sc.at[k, s, p],
                            chunk,
                        )
                        send()

                    when(first, start)
                    when(passing & jnp.logical_not(first), relay)
                yield
        base = t * rows
        for p in range(parts):
            for k, way in enumerate((1, -1)):
                for s in range(nt - 1):
                    j = nt - 1 - s if way == 1 else s
                    ok = (t == j) & (t > 0 if way == 1 else t < nt - 1)

                    def arrive():
                        for c in hops(k, s, p, t):
                            c.wait_recv()

                    when(ok, arrive)
            s_right, s_left = nt - 1 - t, t

            def total_of(i, _):
                r = pl.multiple_of(i * 16, 16)
                x = mine(base + p * chunk, r, 16)
                o_ref[pl.ds(p * chunk + r, 16), :] = x
                return 0

            lax.fori_loop(0, chunk // 16, total_of, 0)
            for k, way in enumerate((1, -1)):
                at = s_right if way == 1 else s_left

                def add():
                    def body(i, _):
                        r = pl.multiple_of(i * 16, 16)
                        o_ref[pl.ds(p * chunk + r, 16), :] += row_decode(cr.at[k, at, p], sr.at[k, at, p], r, 16)
                        return 0

                    lax.fori_loop(0, chunk // 16, body, 0)

                when(t > 0 if way == 1 else t < nt - 1, add)
            yield
        for s in range(nt - 1):
            for p in range(parts):
                for k, way in enumerate((1, -1)):
                    j = nt - 1 - s if way == 1 else s
                    passing = (t < j) if way == 1 else (t > j)

                    def drain():
                        for c in hops(k, s, p, t + way):
                            c.wait_send()

                    when(passing, drain)

    st.task(("line",), gen)
    return ho


def chip_gather(st, w):
    nd = st.nd
    nc = nd // 2
    hx = st.inp(w)
    ho = st.out((nd,) + w.shape, w.dtype, pl.ANY)
    hs = st.scratch(DMA((nd,)))
    hr = st.scratch(DMA((nd,)))
    hl = st.scratch(DMA((1,)))

    def gen(get):
        x_ref, o_ref, ss, rs, ls = get(hx), get(ho), get(hs), get(hr), get(hl)
        d = lax.axis_index("dp")
        twin = d + 1 - 2 * lax.rem(d, 2)
        own = pltpu.make_async_copy(x_ref, o_ref.at[d], ls.at[0])
        own.start()
        out, fwd = [], []
        for i in range(1, nc):
            out.append(remote(x_ref, o_ref.at[d], ss.at[i], rs.at[i], {"dp": lax.rem(d + 2 * i, nd)}))
            out[-1].start()
        fwd.append(remote(x_ref, o_ref.at[d], ss.at[0], rs.at[0], {"dp": twin}))
        fwd[-1].start()
        yield
        for i in range(1, nc):
            out[i - 1].wait_recv()
            src = lax.rem(d - 2 * i + nd, nd)
            fwd.append(remote(o_ref.at[src], o_ref.at[src], ss.at[nc + i], rs.at[nc + i], {"dp": twin}))
            fwd[-1].start()
            yield
        for c in fwd:
            c.wait()
        for c in out:
            c.wait_send()
        own.wait()

    st.task(("chips", "twin"), gen)
    return ho


def chip_scatter(st, g):
    nd = st.nd
    nc = nd // 2
    _, rows, width = g.shape
    hx = st.inp(g, pl.ANY)
    ho = st.out((rows, width), jnp.float32)
    hm = st.scratch(VMEM((nc, rows, width), jnp.float32))
    ht = st.scratch(VMEM((nc, rows, width), jnp.float32))
    hcs = st.scratch(VMEM((nc - 1, rows, width), jnp.int16))
    hcr = st.scratch(VMEM((nc - 1, rows, width), jnp.int16))
    hss = st.scratch(VMEM((nc - 1, 1, width), jnp.float32))
    hsr = st.scratch(VMEM((nc - 1, 1, width), jnp.float32))
    hl = st.scratch(DMA((nc,)))
    hts = st.scratch(DMA((2, nc)))
    hs = st.scratch(DMA((nc - 1, 2)))
    hr = st.scratch(DMA((nc - 1, 2)))

    def gen(get):
        x_ref, o_ref, m, tw, cs, cr, sc, sr, ls, ts, ss, rs = (
            get(h) for h in (hx, ho, hm, ht, hcs, hcr, hss, hsr, hl, hts, hs, hr)
        )
        d = lax.axis_index("dp")
        core = lax.rem(d, 2)
        chip = d // 2
        twin = d + 1 - 2 * core
        loads, give = [], []
        for i in range(nc):
            g_i = lax.rem(chip + 1 + i, nc)
            loads.append(pltpu.make_async_copy(x_ref.at[2 * g_i + core], m.at[i], ls.at[i]))
            loads[-1].start()
            give.append(remote(x_ref.at[2 * g_i + 1 - core], tw.at[i], ts.at[0, i], ts.at[1, i], {"dp": twin}))
            give[-1].start()
        yield
        sends = []
        for i in range(nc - 1):
            loads[i].wait()
            give[i].wait_recv()

            def body(cols):
                col_encode(m[i, :, cols] + tw[i, :, cols], cs.at[i], sc.at[i], cols)

            over_cols(width, body)
            where = {"dp": lax.rem(d + 2 * (i + 1), nd)}
            pair = (
                remote(cs.at[i], cr.at[i], ss.at[i, 0], rs.at[i, 0], where),
                remote(sc.at[i], sr.at[i], ss.at[i, 1], rs.at[i, 1], where),
            )
            for c in pair:
                c.start()
            sends.append(pair)
            yield
        loads[nc - 1].wait()
        give[nc - 1].wait_recv()
        for i in range(nc - 1):
            for c in sends[i]:
                c.wait_recv()

        def total(cols):
            x = m[nc - 1, :, cols] + tw[nc - 1, :, cols]
            for i in range(nc - 1):
                x = x + col_decode(cr.at[i], sr.at[i], cols)
            o_ref[:, cols] = x

        over_cols(width, total)
        for i in range(nc - 1):
            for c in sends[i]:
                c.wait_send()
        for c in give:
            c.wait_send()

    st.task(("chips", "twin"), gen)
    return ho


def window_gather(st, kv):
    nd = st.nd
    hx = st.inp(kv)
    ho = st.out((3,) + kv.shape, kv.dtype, pl.ANY)
    hz = st.scratch(VMEM(kv.shape, kv.dtype))
    hs = st.scratch(DMA((2,)))
    hr = st.scratch(DMA((2,)))
    hl = st.scratch(DMA((3,)))

    def gen(get):
        x_ref, o_ref, z, ss, rs, ls = (get(h) for h in (hx, ho, hz, hs, hr, hl))
        d = lax.axis_index("dp")
        own = pltpu.make_async_copy(x_ref, o_ref.at[2], ls.at[2])
        own.start()

        def ahead(i):
            return remote(x_ref, o_ref.at[2 - i], ss.at[i - 1], rs.at[i - 1], {"dp": d + i})

        for i in (2, 1):
            when(d + i < nd, lambda: ahead(i).start())
        z[...] = jnp.zeros_like(z)
        for i in (1, 2):
            blank = pltpu.make_async_copy(z, o_ref.at[2 - i], ls.at[2 - i])
            when(d < i, lambda: blank.start())
        yield
        for i in (1, 2):
            blank = pltpu.make_async_copy(z, o_ref.at[2 - i], ls.at[2 - i])
            when(d < i, lambda: blank.wait())
            when(d >= i, lambda: ahead(i).wait_recv())
        for i in (1, 2):
            when(d + i < nd, lambda: ahead(i).wait_send())
        own.wait()

    st.task(("near",), gen)
    return ho


def window_scatter(st, g):
    nd = st.nd
    _, rows, width = g.shape
    hx = st.inp(g)
    ho = st.out((rows, width), jnp.float32)
    hcs = st.scratch(VMEM((2, rows, width), jnp.int16))
    hcr = st.scratch(VMEM((2, rows, width), jnp.int16))
    hss = st.scratch(VMEM((2, 1, width), jnp.float32))
    hsr = st.scratch(VMEM((2, 1, width), jnp.float32))
    hs = st.scratch(DMA((2, 2)))
    hr = st.scratch(DMA((2, 2)))

    def gen(get):
        x_ref, o_ref, cs, cr, sc, sr, ss, rs = (get(h) for h in (hx, ho, hcs, hcr, hss, hsr, hs, hr))
        d = lax.axis_index("dp")

        def back(i):
            where = {"dp": d - i}
            return (
                remote(cs.at[i - 1], cr.at[i - 1], ss.at[i - 1, 0], rs.at[i - 1, 0], where),
                remote(sc.at[i - 1], sr.at[i - 1], ss.at[i - 1, 1], rs.at[i - 1, 1], where),
            )

        for i in (2, 1):

            def send():
                def body(cols):
                    col_encode(x_ref[2 - i, :, cols], cs.at[i - 1], sc.at[i - 1], cols)

                over_cols(width, body)
                for c in back(i):
                    c.start()

            when(d >= i, send)
        yield
        o_ref[...] = x_ref[2]
        for i in (1, 2):

            def take():
                for c in back(i):
                    c.wait_recv()

                def body(cols):
                    o_ref[:, cols] += col_decode(cr.at[i - 1], sr.at[i - 1], cols)

                over_cols(width, body)

            when(d + i < nd, take)
            yield
        for i in (1, 2):

            def drain():
                for c in back(i):
                    c.wait_send()

            when(d >= i, drain)

    st.task(("near",), gen)
    return ho


def full_sum(st, x):
    nd, nt = st.nd, st.nt
    hx = st.inp(x)
    ho = st.out(x.shape, jnp.float32)
    ha = st.scratch(VMEM((nt,) + x.shape, jnp.float32))
    hm = st.scratch(VMEM(x.shape, jnp.float32))
    hb = st.scratch(VMEM((nd,) + x.shape, jnp.float32))
    hs = st.scratch(DMA((2, max(nd, nt))))
    hr = st.scratch(DMA((2, max(nd, nt))))

    def gen(get):
        x_ref, o_ref, a, m, b, ss, rs = (get(h) for h in (hx, ho, ha, hm, hb, hs, hr))
        for k, (axis, n, src, got, dst) in enumerate((("tp", nt, x_ref, a, m), ("dp", nd, m, b, o_ref))):
            me = lax.axis_index(axis)
            cs = [
                remote(src, got.at[me], ss.at[k, i], rs.at[k, i], {axis: lax.rem(me + i, n)})
                for i in range(1, n)
            ]
            for c in cs:
                c.start()
            got[me] = src[...]
            yield
            for c in cs:
                c.wait()
            total = got[0]
            for i in range(1, n):
                total = total + got[i]
            dst[...] = total

    st.task(("tp", "dp"), gen)
    return ho


def rope_tables(position_ids, head_size):
    half_size = head_size // 2
    inverse = rope_base ** (-(jnp.arange(half_size, dtype=jnp.float32) * 2.0 / head_size))
    angles = position_ids.astype(jnp.float32)[:, None] * inverse[None, :]
    return (jnp.cos(angles), jnp.sin(angles))


def rotate_fwd(values, cosine, sine_part):
    half_size = values.shape[-1] // 2
    first_half = values[..., :half_size]
    second_half = values[..., half_size:]
    cos_rows = cosine[:, None, :]
    sin_rows = sine_part[:, None, :]
    return jnp.concatenate(
        [
            first_half * cos_rows - second_half * sin_rows,
            second_half * cos_rows + first_half * sin_rows,
        ],
        axis=-1,
    )


def rms_parts(values):
    inverse = lax.rsqrt(jnp.mean(values * values, axis=-1, keepdims=True) + norm_eps)
    return (values * inverse, inverse)


def rms_back(grad_in, normed, inverse, gain_vec):
    scaled = grad_in * gain_vec
    return inverse * (scaled - normed * jnp.mean(scaled * normed, axis=-1, keepdims=True))


def block_scores(query_block, key_window, query_ids, doc_starts, key_ids):
    scale_factor = 1.0 / math.sqrt(query_block.shape[-1])
    scores = (
        jnp.einsum("rkgd,skd->kgrs", query_block, key_window, preferred_element_type=jnp.float32)
        * scale_factor
    )
    allowed = (key_ids[None, :] >= doc_starts[:, None]) & (key_ids[None, :] <= query_ids[:, None])
    return jnp.where(allowed[None, None], scores, masked_score)


def attend_fwd(query_block, key_window, value_window, query_ids, doc_starts, key_ids):
    scores = block_scores(query_block, key_window, query_ids, doc_starts, key_ids)
    row_max = jnp.max(scores, axis=-1, keepdims=True)
    weights = jnp.exp(scores - row_max)
    row_total = jnp.sum(weights, axis=-1, keepdims=True)
    probs_low = (weights / row_total).astype(jnp.bfloat16)
    log_total = (row_max + jnp.log(row_total))[..., 0]
    context = jnp.einsum("kgrs,skd->rkgd", probs_low, value_window, preferred_element_type=jnp.float32)
    return (context.astype(jnp.bfloat16), log_total)


def attend_back(
    query_block, key_window, value_window, context, log_total, context_grad, query_ids, doc_starts, key_ids
):
    scale_factor = 1.0 / math.sqrt(query_block.shape[-1])
    scores = block_scores(query_block, key_window, query_ids, doc_starts, key_ids)
    probs = jnp.exp(scores - log_total[..., None])
    probs_low = probs.astype(jnp.bfloat16)
    prob_grad = jnp.einsum("rkgd,skd->kgrs", context_grad, value_window, preferred_element_type=jnp.float32)
    row_delta = jnp.transpose(
        jnp.sum(context_grad.astype(jnp.float32) * context.astype(jnp.float32), axis=-1), (1, 2, 0)
    )
    score_low = (probs * (prob_grad - row_delta[..., None])).astype(jnp.bfloat16)
    query_grad = scale_factor * jnp.einsum(
        "kgrs,skd->rkgd", score_low, key_window, preferred_element_type=jnp.float32
    )
    key_grad = scale_factor * jnp.einsum(
        "kgrs,rkgd->skd", score_low, query_block, preferred_element_type=jnp.float32
    )
    value_grad = jnp.einsum("kgrs,rkgd->skd", probs_low, context_grad, preferred_element_type=jnp.float32)
    return (query_grad, key_grad, value_grad)


def dot(a, b):
    return jnp.dot(a, b, preferred_element_type=jnp.float32)


def on_device(
    nd, nt, tokens, positions, attn_gain, w_query, w_key, w_value, w_out, ffn_gain, w_gate, w_up, w_down, out_grad
):
    own_rows, width = tokens.shape
    span_rows = own_rows * nt
    query_heads = w_query.shape[1] // HD
    kv_heads = w_key.shape[1] // HD
    group_size = query_heads // kv_heads
    kv_width = kv_heads * HD
    q_width = query_heads * HD
    units = w_gate.shape[1]
    shard = w_query.shape[0]
    span_begin = lax.axis_index("dp") * span_rows
    low = jnp.bfloat16

    def stage(name, cid):
        return Stage(name, cid, nd, nt)

    def full(w):
        return w.reshape(nd * shard, w.shape[-1])

    def rows_of(x):
        return x.reshape(span_rows, x.shape[-1])

    def blocks(g):
        return g.reshape(nd, shard, g.shape[-1])

    tokens_f = tokens.astype(jnp.float32)
    normed1, inverse1 = rms_parts(tokens_f)
    w_attn = jnp.concatenate([w_query, w_key, w_value, w_out.T], axis=1)
    w_down_t = w_down.T

    st = stage("stage1", 1)
    line_gather(st, (normed1 * attn_gain).astype(low))
    chip_gather(st, w_attn)
    hidden1, attn_full = st.run()
    hidden1, attn_full = rows_of(hidden1), full(attn_full)
    qkv_full = attn_full[:, : q_width + 2 * kv_width]
    out_full_t = attn_full[:, q_width + 2 * kv_width :]

    qkv = dot(hidden1, qkv_full)
    cosine, sine_part = rope_tables(positions, HD)
    query_rot = (
        rotate_fwd(qkv[:, :q_width].reshape(span_rows, query_heads, HD), cosine, sine_part)
        .astype(low)
        .reshape(span_rows, kv_heads, group_size, HD)
    )
    key_rot = (
        rotate_fwd(qkv[:, q_width : q_width + kv_width].reshape(span_rows, kv_heads, HD), cosine, sine_part)
        .astype(low)
        .reshape(span_rows, kv_width)
    )
    value_low = qkv[:, q_width + kv_width :].astype(low)

    st = stage("stage2", 2)
    window_gather(st, jnp.concatenate([key_rot, value_low], axis=1))
    (kv_window,) = st.run()
    kv_window = kv_window.reshape(3 * span_rows, 2 * kv_width)
    key_window = kv_window[:, :kv_width].reshape(3 * span_rows, kv_heads, HD)
    value_window = kv_window[:, kv_width:].reshape(3 * span_rows, kv_heads, HD)
    key_ids = span_begin - 2 * span_rows + jnp.arange(3 * span_rows, dtype=jnp.int32)
    query_ids = span_begin + jnp.arange(span_rows, dtype=jnp.int32)
    doc_begin = query_ids - positions

    context4, log_total = attend_fwd(query_rot, key_window, value_window, query_ids, doc_begin, key_ids)
    context = context4.reshape(span_rows, q_width)
    attn_part = lax.dot_general(context, out_full_t, (((1,), (1,)), ((), ())), preferred_element_type=jnp.float32)

    st = stage("stage3", 3)
    line_scatter(st, attn_part)
    line_gather(st, out_grad)
    chip_gather(st, w_gate)
    chip_gather(st, w_up)
    attn_out, grad_rows, gate_full, up_full = st.run()
    grad_rows, gate_full, up_full = rows_of(grad_rows), full(gate_full), full(up_full)

    residual = tokens_f + attn_out
    normed2, inverse2 = rms_parts(residual)

    st = stage("stage4", 4)
    line_gather(st, (normed2 * ffn_gain).astype(low))
    chip_gather(st, w_down_t)
    hidden2, down_full_t = st.run()
    hidden2, down_full_t = rows_of(hidden2), full(down_full_t)

    gate_pre = dot(hidden2, gate_full)
    up_proj = dot(hidden2, up_full)
    sigmoid_gate = jax.nn.sigmoid(gate_pre)
    inner_act = (gate_pre * sigmoid_gate * up_proj).astype(low)
    inner_grad = dot(grad_rows, down_full_t)
    silu_slope = sigmoid_gate * (1.0 + gate_pre * (1.0 - sigmoid_gate))
    gate_low = (inner_grad * up_proj * silu_slope).astype(low)
    up_low = (inner_grad * gate_pre * sigmoid_gate).astype(low)
    hidden2_part = dot(gate_low, gate_full.T) + dot(up_low, up_full.T)
    down_grad_t = dot(grad_rows.T, inner_act)

    st = stage("stage5", 5)
    line_scatter(st, hidden2_part)
    chip_scatter(st, blocks(down_grad_t))
    hidden2_grad, down_sum_t = st.run()

    ffn_gain_part = jnp.sum(hidden2_grad * normed2, axis=0)
    residual_grad = out_grad.astype(jnp.float32) + rms_back(hidden2_grad, normed2, inverse2, ffn_gain)
    ffn_part = dot(inner_act, down_full_t.T)
    gate_grad = dot(hidden2.T, gate_low)
    up_grad = dot(hidden2.T, up_low)

    st = stage("stage6", 6)
    line_scatter(st, ffn_part)
    line_gather(st, residual_grad.astype(low))
    chip_scatter(st, blocks(gate_grad))
    ffn_out, residual_rows, gate_sum = st.run()
    residual_rows = rows_of(residual_rows)
    output = (residual + ffn_out).astype(low)

    context_grad = dot(residual_rows, out_full_t).astype(low).reshape(span_rows, kv_heads, group_size, HD)
    query_grad, key_grad, value_grad = attend_back(
        query_rot, key_window, value_window, context4, log_total, context_grad, query_ids, doc_begin, key_ids
    )
    kv_grads = jnp.concatenate(
        [key_grad.reshape(3, span_rows, kv_width), value_grad.reshape(3, span_rows, kv_width)], axis=2
    )
    st = stage("stage7", 7)
    window_scatter(st, kv_grads)
    (kv_total,) = st.run()

    key_low = (
        rotate_fwd(kv_total[:, :kv_width].reshape(span_rows, kv_heads, HD), cosine, -sine_part)
        .astype(low)
        .reshape(span_rows, kv_width)
    )
    value_grad_low = kv_total[:, kv_width:].astype(low)
    query_low = (
        rotate_fwd(query_grad.reshape(span_rows, query_heads, HD), cosine, -sine_part)
        .astype(low)
        .reshape(span_rows, q_width)
    )
    qkv_low = jnp.concatenate([query_low, key_low, value_grad_low], axis=1)
    hidden1_part = dot(qkv_low, qkv_full.T)
    qkv_grad = dot(hidden1.T, qkv_low)
    out_grad_t = dot(residual_rows.T, context)
    attn_grad = jnp.concatenate([qkv_grad, out_grad_t], axis=1)

    st = stage("stage8", 8)
    line_scatter(st, hidden1_part)
    chip_scatter(st, blocks(up_grad))
    chip_scatter(st, blocks(attn_grad))
    hidden1_grad, up_sum, attn_sum = st.run()

    attn_gain_part = jnp.sum(hidden1_grad * normed1, axis=0)
    tokens_grad = residual_grad + rms_back(hidden1_grad, normed1, inverse1, attn_gain)
    gains = jnp.concatenate(
        [attn_gain_part[None], ffn_gain_part[None], jnp.zeros((6, width), jnp.float32)], axis=0
    )
    st = stage("stage9", 9)
    full_sum(st, gains)
    (gains,) = st.run()
    cuts = (q_width, q_width + kv_width, q_width + 2 * kv_width)
    return (
        output,
        tokens_grad,
        gains[0],
        attn_sum[:, : cuts[0]],
        attn_sum[:, cuts[0] : cuts[1]],
        attn_sum[:, cuts[1] : cuts[2]],
        attn_sum[:, cuts[2] :].T,
        gains[1],
        gate_sum,
        up_sum,
        down_sum_t.T,
    )


def solution(mesh):
    return jax.shard_map(
        functools.partial(on_device, mesh.shape["dp"], mesh.shape["tp"]),
        mesh=mesh,
        in_specs=(
            P(("dp", "tp"), None),
            P("dp"),
            P(),
            P("dp", "tp"),
            P("dp", "tp"),
            P("dp", "tp"),
            P("tp", "dp"),
            P(),
            P("dp", "tp"),
            P("dp", "tp"),
            P("tp", "dp"),
            P(("dp", "tp"), None),
        ),
        out_specs=(
            P(("dp", "tp"), None),
            P(("dp", "tp"), None),
            P(),
            P("dp", "tp"),
            P("dp", "tp"),
            P("dp", "tp"),
            P("tp", "dp"),
            P(),
            P("dp", "tp"),
            P("dp", "tp"),
            P("tp", "dp"),
        ),
        check_vma=False,
    )
```

```python
import functools
import math

import jax
import jax.numpy as jnp
from jax import lax
from jax.experimental import pallas as pl
from jax.experimental.pallas import tpu as pltpu
from jax.sharding import PartitionSpec as P

HD = 96
norm_eps = 1e-05
rope_base = 100000.0
masked_score = -1e30

MESH = pl.DeviceIdType.MESH
VMEM = pltpu.VMEM
DMA = pltpu.SemaphoreType.DMA
LEVELS = 32000.0


class Stage:
    def __init__(self, name, cid, nd, nt):
        self.name, self.cid, self.nd, self.nt = name, cid, nd, nt
        self.ins, self.outs, self.scr, self.tasks, self.links = [], [], [], [], set()

    def inp(self, x, space=VMEM):
        self.ins.append((x, space))
        return ("i", len(self.ins) - 1)

    def out(self, shape, dtype, space=VMEM):
        self.outs.append((shape, dtype, space))
        return ("o", len(self.outs) - 1)

    def scratch(self, spec):
        self.scr.append(spec)
        return ("s", len(self.scr) - 1)

    def task(self, links, gen):
        self.links |= set(links)
        self.tasks.append(gen)

    def _barrier(self):
        d, t = lax.axis_index("dp"), lax.axis_index("tp")
        nd, nt = self.nd, self.nt
        sem = pltpu.get_barrier_semaphore()
        count = 0

        def greet(ok, where):
            if ok is True:
                pl.semaphore_signal(sem, inc=1, device_id=where, device_id_type=MESH)
                return 1

            @pl.when(ok)
            def _():
                pl.semaphore_signal(sem, inc=1, device_id=where, device_id_type=MESH)

            return ok.astype(jnp.int32)

        if "line" in self.links:
            count += greet(t > 0, {"tp": t - 1})
            count += greet(t < nt - 1, {"tp": t + 1})
        if "chips" in self.links:
            for i in range(1, nd // 2):
                count += greet(True, {"dp": lax.rem(d + 2 * i, nd)})
        if "twin" in self.links:
            count += greet(True, {"dp": d + 1 - 2 * lax.rem(d, 2)})
        if "near" in self.links:
            for i in (1, 2):
                count += greet(d >= i, {"dp": d - i})
                count += greet(d < nd - i, {"dp": d + i})
        if "tp" in self.links:
            for i in range(1, nt):
                count += greet(True, {"tp": lax.rem(t + i, nt)})
        if "dp" in self.links:
            for i in range(1, nd):
                count += greet(True, {"dp": lax.rem(d + i, nd)})
        pl.semaphore_wait(sem, count)

    def run(self):
        n_in, n_out = len(self.ins), len(self.outs)

        def kernel(*refs):
            def get(h):
                kind, i = h
                return refs[i + {"i": 0, "o": n_in, "s": n_in + n_out}[kind]]

            self._barrier()
            live = [g(get) for g in self.tasks]
            while live:
                still = []
                for g in live:
                    try:
                        next(g)
                        still.append(g)
                    except StopIteration:
                        pass
                live = still

        return pl.pallas_call(
            kernel,
            out_shape=[jax.ShapeDtypeStruct(s, t) for s, t, _ in self.outs],
            in_specs=[pl.BlockSpec(memory_space=sp) for _, sp in self.ins],
            out_specs=[pl.BlockSpec(memory_space=sp) for _, _, sp in self.outs],
            scratch_shapes=self.scr,
            compiler_params=pltpu.CompilerParams(
                collective_id=self.cid, has_side_effects=True, vmem_limit_bytes=63 << 20
            ),
            name=self.name,
        )(*[x for x, _ in self.ins])


def remote(src, dst, send, recv, where):
    return pltpu.make_async_remote_copy(
        src_ref=src, dst_ref=dst, send_sem=send, recv_sem=recv, device_id=where, device_id_type=MESH
    )


def when(ok, fn):
    if ok is True:
        fn()
    elif ok is not False:
        pl.when(ok)(fn)


def over_cols(width, fn):
    def body(c, _):
        fn(pl.ds(pl.multiple_of(c * 128, 128), 128))
        return 0

    lax.fori_loop(0, width // 128, body, 0)
    if width % 128:
        fn(pl.ds(width // 128 * 128, width % 128))


def row_encode(read, code, scale, rows):
    step = 16

    def body(i, held):
        r = pl.multiple_of(i * step, step)
        x = read(r, step)
        top = jnp.max(jnp.abs(x), axis=-1, keepdims=True)
        code[pl.ds(r, step), :] = jnp.round(x * (LEVELS / jnp.maximum(top, 1e-30))).astype(jnp.int32).astype(jnp.int16)
        lane = lax.broadcasted_iota(jnp.int32, (step, 128), 1)
        row = lax.broadcasted_iota(jnp.int32, (step, 128), 0) + r
        mine = jnp.sum(jnp.where(lane == row, jnp.maximum(top, 1e-30) * (1.0 / LEVELS), 0.0), axis=0, keepdims=True)
        return held + jnp.broadcast_to(mine, (8, 128))

    scale[...] = lax.fori_loop(0, rows // step, body, jnp.zeros((8, 128), jnp.float32))


def row_decode(code, scale, r, step):
    lane = lax.broadcasted_iota(jnp.int32, (step, 128), 1)
    row = lax.broadcasted_iota(jnp.int32, (step, 128), 0) + r
    col = jnp.sum(jnp.where(lane == row, jnp.broadcast_to(scale[0:1, :], (step, 128)), 0.0), axis=-1, keepdims=True)
    return code[pl.ds(r, step), :].astype(jnp.int32).astype(jnp.float32) * col


def col_encode(x, code, scale, cols):
    top = jnp.maximum(jnp.max(jnp.abs(x), axis=0, keepdims=True), 1e-30)
    code[:, cols] = jnp.round(x * (LEVELS / top)).astype(jnp.int32).astype(jnp.int16)
    scale[:, cols] = top * (1.0 / LEVELS)


def col_decode(code, scale, cols):
    return code[:, cols].astype(jnp.int32).astype(jnp.float32) * scale[:, cols]


class LineGather:
    def __init__(self, st, full, rows, parts):
        self.st, self.full, self.rows, self.parts = st, full, rows, parts
        self.hs = st.scratch(DMA((2, st.nt, parts)))
        self.hr = st.scratch(DMA((2, st.nt, parts)))
        st.links.add("line")

    def bind(self, get):
        self.ref, self.ss, self.rs = get(self.full), get(self.hs), get(self.hr)
        self.t = lax.axis_index("tp")
        return self

    def piece(self, owner, p):
        chunk = self.rows // self.parts
        return self.ref.at[pl.ds(pl.multiple_of(owner * self.rows + p * chunk, chunk), chunk)]

    def hop(self, owner, k, s, p, where):
        at = self.piece(owner, p)
        return remote(at, at, self.ss.at[k, s, p], self.rs.at[k, s, p], {"tp": where})

    def _send(self, s, p, k, way):
        nt, t = self.st.nt, self.t
        owner, where = t - s * way, t + way
        ok = (owner >= 0) & (owner < nt) & (where >= 0) & (where < nt)
        when(ok, lambda: self.hop(owner, k, s, p, where).start())

    def start(self, p):
        for k, way in enumerate((1, -1)):
            self._send(0, p, k, way)

    def arrive(self, s, p):
        nt, t = self.st.nt, self.t
        for k, way in enumerate((1, -1)):
            owner = t - way * (s + 1)
            ok = (owner >= 0) & (owner < nt)
            when(ok, lambda: self.hop(owner, k, s, p, t).wait_recv())
            if s < nt - 2:
                self._send(s + 1, p, k, way)

    def arrivals(self):
        return [
            functools.partial(self.arrive, s, p) for s in range(self.st.nt - 1) for p in range(self.parts)
        ]

    def finish(self):
        nt, t = self.st.nt, self.t
        for s in range(nt - 1):
            for p in range(self.parts):
                for k, way in enumerate((1, -1)):
                    owner, where = t - s * way, t + way
                    ok = (owner >= 0) & (owner < nt) & (where >= 0) & (where < nt)
                    when(ok, lambda: self.hop(owner, k, s, p, where).wait_send())


class LineScatter:
    def __init__(self, st, part, rows, width, parts):
        self.st, self.part, self.rows, self.width, self.parts = st, part, rows, width, parts
        nt = st.nt
        self.chunk = rows // parts
        shape = (2, (nt - 1) * parts, self.chunk, width)
        self.kept = min(2, nt - 1) * parts
        few = (2, self.kept, self.chunk, width)
        self.hc = [st.scratch(VMEM(x, jnp.int16)) for x in (few, shape)]
        self.hk = [st.scratch(VMEM(x[:2] + (8, 128), jnp.float32)) for x in (few, shape)]
        self.hd = [st.scratch(DMA((2, 2, (nt - 1) * parts))) for _ in range(2)]
        st.links.add("line")

    def bind(self, get):
        self.x = get(self.part)
        (self.cs, self.cr), (self.sc, self.sr), (self.ss, self.rs) = (
            [get(h) for h in hs] for hs in (self.hc, self.hk, self.hd)
        )
        self.t = lax.axis_index("tp")
        return self

    def hops(self, k, u, where):
        w = lax.rem(u, self.kept)
        return (
            remote(self.cs.at[k, w], self.cr.at[k, u], self.ss.at[0, k, u], self.rs.at[0, k, u], {"tp": where}),
            remote(self.sc.at[k, w], self.sr.at[k, u], self.ss.at[1, k, u], self.rs.at[1, k, u], {"tp": where}),
        )

    def _rows(self, base, r, n):
        return self.x[pl.ds(pl.multiple_of(base + r, n), n), :]

    def slots(self):
        return 4 * (self.st.nt - 1)

    def step(self, v, produce=None):
        nt, t, chunk = self.st.nt, self.t, self.chunk
        p, v = v // self.slots(), lax.rem(v, self.slots())
        k = lax.rem(v, 2)
        s = v // 2 - jnp.where(k == 0, t, nt - 1 - t)
        j = jnp.where(k == 0, nt - 1 - s, s)
        way = 1 - 2 * k
        u = s * self.parts + p
        first = t == jnp.where(k == 0, 0, nt - 1)
        passing = (s >= 0) & (s < nt - 1) & jnp.where(k == 0, t < j, t > j)

        @pl.when(passing)
        def _():
            if produce is not None:
                pl.when(p == 0)(lambda: produce(j))

            @pl.when(first)
            def _():
                self.cr[k, u] = jnp.zeros((chunk, self.width), jnp.int16)
                self.sr[k, u] = jnp.zeros((8, 128), jnp.float32)

            @pl.when(jnp.logical_not(first))
            def _():
                for c in self.hops(k, u, t):
                    c.wait_recv()

            @pl.when(u >= self.kept)
            def _():
                for c in self.hops(k, u - self.kept, t + way):
                    c.wait_send()

            base, w = j * self.rows + p * chunk, lax.rem(u, self.kept)
            row_encode(
                lambda r, n: self._rows(base, r, n) + row_decode(self.cr.at[k, u], self.sr.at[k, u], r, n),
                self.cs.at[k, w],
                self.sc.at[k, w],
                chunk,
            )
            for c in self.hops(k, u, t + way):
                c.start()

    def relay(self, p, produce=None, beside=None):
        n = self.slots()

        def one(v, _):
            self.step(v, produce)
            if beside is not None:
                beside(v)
            return 0

        lax.fori_loop(p * n, (p + 1) * n, one, 0)

    def total(self, p, put):
        nt, t, chunk = self.st.nt, self.t, self.chunk
        right, left = (nt - 1 - t) * self.parts + p, t * self.parts + p
        from_left, from_right = t > 0, t < nt - 1

        @pl.when(from_left)
        def _():
            for c in self.hops(0, right, t):
                c.wait_recv()

        @pl.when(from_right)
        def _():
            for c in self.hops(1, left, t):
                c.wait_recv()

        at_r = jnp.where(from_left, right, 0)
        at_l = jnp.where(from_right, left, 0)
        base = t * self.rows + p * chunk

        def body(i, _):
            r = pl.multiple_of(i * 16, 16)
            x = self._rows(base, r, 16)
            a = row_decode(self.cr.at[0, at_r], self.sr.at[0, at_r], r, 16)
            b = row_decode(self.cr.at[1, at_l], self.sr.at[1, at_l], r, 16)
            put(r, x + jnp.where(from_left, a, 0.0) + jnp.where(from_right, b, 0.0))
            return 0

        lax.fori_loop(0, chunk // 16, body, 0)

    def finish(self):
        nt, t = self.st.nt, self.t

        def step(v, _):
            s, k = v // 2, lax.rem(v, 2)
            j = jnp.where(k == 0, nt - 1 - s, s)
            later = s + self.kept // self.parts
            i = jnp.where(k == 0, nt - 1 - later, later)
            waited = (later < nt - 1) & jnp.where(k == 0, t < i, t > i)

            @pl.when(jnp.where(k == 0, t < j, t > j) & jnp.logical_not(waited))
            def _():
                for p in range(self.parts):
                    for c in self.hops(k, s * self.parts + p, t + 1 - 2 * k):
                        c.wait_send()

            return 0

        lax.fori_loop(0, 2 * (nt - 1), step, 0)


class ChipGather:
    def __init__(self, st, w, full, rows):
        self.st, self.w, self.full, self.rows = st, w, full, rows
        self.hs = st.scratch(DMA((st.nd,)))
        self.hr = st.scratch(DMA((st.nd,)))
        self.hl = st.scratch(DMA((1,)))
        st.links |= {"chips", "twin"}

    def bind(self, get):
        self.x, self.o, self.ss, self.rs, ls = (get(h) for h in (self.w, self.full, self.hs, self.hr, self.hl))
        nd = self.st.nd
        d = lax.axis_index("dp")
        twin = {"dp": d + 1 - 2 * lax.rem(d, 2)}
        nc = nd // 2

        def at(i):
            return self.o.at[pl.ds(pl.multiple_of(i * self.rows, self.rows), self.rows)]

        self.own = lambda: pltpu.make_async_copy(self.x, at(d), ls.at[0])
        self.out = lambda i: remote(self.x, at(d), self.ss.at[i], self.rs.at[i], {"dp": lax.rem(d + 2 * i, nd)})

        def fwd(i):
            src = self.x if i == 0 else at(lax.rem(d - 2 * i + nd, nd))
            dst = at(lax.rem(d - 2 * i + nd, nd))
            j = 0 if i == 0 else nc + i
            return remote(src, dst, self.ss.at[j], self.rs.at[j], twin)

        self.fwd, self.nc = fwd, nc
        return self

    def start(self):
        for i in range(1, self.nc):
            self.out(i).start()
        self.fwd(0).start()
        self.own().start()

    def forward(self, i):
        self.out(i).wait_recv()
        self.fwd(i).start()

    def forwards(self):
        return [functools.partial(self.forward, i) for i in range(1, self.nc)]

    def arrived(self):
        for i in range(self.nc):
            self.fwd(i).wait_recv()
        self.own().wait()

    def finish(self):
        for i in range(self.nc):
            self.fwd(i).wait_send()
        for i in range(1, self.nc):
            self.out(i).wait_send()


class ChipScatter:
    def __init__(self, st, g, rows, width):
        self.st, self.g, self.rows, self.width = st, g, rows, width
        nc = self.nc = st.nd // 2
        self.hm = st.scratch(VMEM((nc, rows, width), jnp.float32))
        self.hc = [st.scratch(VMEM((nc - 1, rows, width), jnp.int16)) for _ in range(2)]
        self.hk = [st.scratch(VMEM((nc - 1, 1, width), jnp.float32)) for _ in range(2)]
        self.ht = [st.scratch(DMA((nc,))) for _ in range(2)]
        self.hd = [st.scratch(DMA((2, nc - 1))) for _ in range(2)]
        st.links |= {"chips", "twin"}

    def bind(self, get):
        self.x, self.tw = get(self.g), get(self.hm)
        (self.cs, self.cr), (self.sc, self.sr), (self.ts, self.tr), (self.ss, self.rs) = (
            [get(h) for h in hs] for hs in (self.hc, self.hk, self.ht, self.hd)
        )
        self.d = lax.axis_index("dp")
        self.core = lax.rem(self.d, 2)
        return self

    def at(self, i):
        return pl.ds(pl.multiple_of(i * self.rows, self.rows), self.rows)

    def chip(self, i):
        return lax.rem(self.d // 2 + 1 + i, self.nc)

    def gift(self, i):
        twin = {"dp": self.d + 1 - 2 * self.core}
        src = self.x.at[self.at(2 * self.chip(i) + 1 - self.core)]
        return remote(src, self.tw.at[i], self.ts.at[i], self.tr.at[i], twin)

    def sums(self, i):
        where = {"dp": lax.rem(self.d + 2 * (i + 1), self.st.nd)}
        return (
            remote(self.cs.at[i], self.cr.at[i], self.ss.at[0, i], self.rs.at[0, i], where),
            remote(self.sc.at[i], self.sr.at[i], self.ss.at[1, i], self.rs.at[1, i], where),
        )

    def give(self):
        for i in range(self.nc):
            self.gift(i).start()

    def combine(self, i):
        self.gift(i).wait_recv()
        rows = self.at(2 * self.chip(i) + self.core)
        over_cols(
            self.width,
            lambda cols: col_encode(self.x[rows, cols] + self.tw[i, :, cols], self.cs.at[i], self.sc.at[i], cols),
        )
        for c in self.sums(i):
            c.start()

    def combines(self):
        return [functools.partial(self.combine, i) for i in range(self.nc - 1)]

    def total(self, put):
        n = self.nc - 1
        self.gift(n).wait_recv()
        for i in range(n):
            for c in self.sums(i):
                c.wait_recv()

        def tile(cols):
            x = self.x[self.at(self.d), cols] + self.tw[n, :, cols]
            for i in range(n):
                x = x + col_decode(self.cr.at[i], self.sr.at[i], cols)
            put(cols, x)

        over_cols(self.width, tile)

    def finish(self):
        for i in range(self.nc):
            self.gift(i).wait_send()
        for i in range(self.nc - 1):
            for c in self.sums(i):
                c.wait_send()


class FullSum:
    def __init__(self, st, x, out, shape):
        self.st, self.x, self.out = st, x, out
        self.ha = st.scratch(VMEM((st.nt,) + shape, jnp.float32))
        self.hm = st.scratch(VMEM(shape, jnp.float32))
        self.hb = st.scratch(VMEM((st.nd,) + shape, jnp.float32))
        self.hs = st.scratch(DMA((2, max(st.nd, st.nt))))
        self.hr = st.scratch(DMA((2, max(st.nd, st.nt))))
        st.links |= {"tp", "dp"}

    def run(self, get):
        nd, nt = self.st.nd, self.st.nt
        x, o, a, m, b, ss, rs = (get(h) for h in (self.x, self.out, self.ha, self.hm, self.hb, self.hs, self.hr))
        for k, (axis, n, src, got, dst) in enumerate((("tp", nt, x, a, m), ("dp", nd, m, b, o))):
            me = lax.axis_index(axis)
            cs = [
                remote(src, got.at[me], ss.at[k, i], rs.at[k, i], {axis: lax.rem(me + i, n)}) for i in range(1, n)
            ]
            for c in cs:
                c.start()
            got[me] = src[...]
            for c in cs:
                c.wait()
            total = got[0]
            for i in range(1, n):
                total = total + got[i]
            dst[...] = total


def lane_take(x, offset):
    base = offset // 128 * 128
    wide = min(256, x.shape[-1] - base)
    slab = x[:, base : base + wide]
    if wide % 128:
        slab = jnp.concatenate([slab, jnp.zeros((x.shape[0], -wide % 128), x.dtype)], axis=1)
        wide = slab.shape[-1]
    if offset > base:
        slab = pltpu.roll(slab, wide - (offset - base), 1)
    slab = slab[:, :128]
    return jnp.where(lax.broadcasted_iota(jnp.int32, slab.shape, 1) < HD, slab, 0.0)


def lane_place(x, offset, width):
    base = offset // 128 * 128
    wide = min(256, width - base)
    slab = x if wide == 128 else jnp.concatenate([x, jnp.zeros_like(x)], axis=1)
    if offset > base:
        slab = pltpu.roll(slab, offset - base, 1)
    slab = slab[:, :wide]
    pieces = []
    if base:
        pieces.append(jnp.zeros((x.shape[0], base), x.dtype))
    pieces.append(slab)
    if base + wide < width:
        pieces.append(jnp.zeros((x.shape[0], width - base - wide), x.dtype))
    return jnp.concatenate(pieces, axis=1) if len(pieces) > 1 else slab


def turned(u, cosine, sine):
    wide = u.shape[-1]
    lane = lax.rem(lax.broadcasted_iota(jnp.int32, u.shape, 1), HD)
    swap = jnp.where(lane < HD // 2, pltpu.roll(u, wide - HD // 2, 1), pltpu.roll(u, HD // 2, 1))
    return u * cosine + swap * sine


def nt_dot(a, b):
    return lax.dot_general(a, b, (((1,), (1,)), ((), ())), preferred_element_type=jnp.float32)


def per_tile(count, size, fn):
    def body(i, _):
        fn(pl.multiple_of(i * size, size))
        return 0

    lax.fori_loop(0, count, body, 0)


def in_turn(*lists):
    for i in range(max(len(x) for x in lists)):
        for x in lists:
            if i < len(x):
                x[i]()


class Fused(Stage):
    def body(self, fn):
        self.tasks = [lambda get: iter(fn(get) or ())]


def inverse_rms(x):
    return lax.rsqrt(jnp.mean(x * x, axis=-1, keepdims=True) + norm_eps)


def tn_dot(a, b):
    return lax.dot_general(a, b, (((0,), (0,)), ((), ())), preferred_element_type=jnp.float32)


def across(x, count):
    return jnp.concatenate([x] * count, axis=1) if count > 1 else x


def masked_scores(keys, queries, first, begin, span, group):
    s = nt_dot(keys, queries) * (1.0 / math.sqrt(HD))
    key = lax.broadcasted_iota(jnp.int32, s.shape, 0) + first
    own = lax.rem(lax.broadcasted_iota(jnp.int32, s.shape, 1), 128) + (first + 2 * span)
    return s, (key >= across(begin, group)) & (key <= own)


def attention_stage(nd, nt, tokens, attn_gain, ffn_gain, out_grad, begin, cosine, sine, w_attn, w_gate, w_up, w_down_t, heads):
    st = Fused("attend", 1, nd, nt)
    low, f32 = jnp.bfloat16, jnp.float32
    own, width = tokens.shape
    span = own * nt
    shard = w_attn.shape[0]
    n_q, n_kv = heads
    group = n_q // n_kv
    tiles = span // 128
    qw, kvw = n_q * HD, n_kv * HD
    reach = 2 * span + 128
    parts = 2
    piece = own // parts

    h_tok, h_g1, h_g2 = st.inp(tokens), st.inp(attn_gain[None]), st.inp(ffn_gain[None])
    h_og, h_begin = st.inp(out_grad), st.inp(begin)
    h_cos, h_sin = st.inp(cosine), st.inp(sine)
    h_wa, h_wg, h_wu, h_wd = st.inp(w_attn), st.inp(w_gate), st.inp(w_up), st.inp(w_down_t)

    o_h1, o_h2, o_gr = (st.out((span, width), low) for _ in range(3))
    o_wa = st.out((nd * shard, w_attn.shape[1]), low)
    o_wg, o_wu, o_wd = (st.out((nd * shard, w.shape[1]), low, pl.ANY) for w in (w_gate, w_up, w_down_t))
    o_q = st.out((n_kv, tiles, group * 128, 128), low)
    o_k, o_v = (st.out((n_kv, 3 * span, 128), low) for _ in range(2))
    o_kt = st.out((n_kv, 128, 3 * span), low)
    o_ctx = st.out((span, qw), low)
    o_ch = st.out((n_kv, tiles, group * 128, 128), low)
    o_lse = st.out((n_kv, tiles, 1, group * 128), f32)
    o_res = st.out((own, width), f32)

    h_win = st.scratch(VMEM((3, span, 2 * kvw), low))
    h_ks = st.scratch(DMA((2,)))
    h_kr = st.scratch(DMA((2,)))
    h_vt = st.scratch(VMEM((n_kv, 128, 3 * span), low))
    h_part = st.scratch(VMEM((span, width), f32))

    ag1 = LineGather(st, o_h1, own, parts)
    ag2 = LineGather(st, o_h2, own, parts)
    ag3 = LineGather(st, o_gr, own, parts)
    rs1 = LineScatter(st, h_part, own, width, parts)
    wa = ChipGather(st, h_wa, o_wa, shard)
    wg = ChipGather(st, h_wg, o_wg, shard)
    wu = ChipGather(st, h_wu, o_wu, shard)
    wd = ChipGather(st, h_wd, o_wd, shard)
    st.links.add("near")

    def fn(get):
        d, t = lax.axis_index("dp"), lax.axis_index("tp")
        for x in (ag1, ag2, ag3, rs1, wa, wg, wu, wd):
            x.bind(get)
        tok, g1, g2, h1, h2 = get(h_tok), get(h_g1), get(h_g2), get(o_h1), get(o_h2)
        wa_ref, win, q, k, v, kt, vt, ch = (get(h) for h in (o_wa, h_win, o_q, o_k, o_v, o_kt, h_vt, o_ch))
        ctx, lse, res, part = get(o_ctx), get(o_lse), get(o_res), get(h_part)
        cos_ref, sin_ref, begin_ref = get(h_cos), get(h_sin), get(h_begin)

        wa.start()

        def first_norm(p):
            def tile(r):
                x = tok[pl.ds(p * piece + r, 16), :].astype(f32)
                at = pl.ds(pl.multiple_of(t * own + p * piece + r, 16), 16)
                h1[at, :] = (x * inverse_rms(x) * g1[...]).astype(low)

            per_tile(piece // 16, 16, tile)

        for p in range(parts):
            first_norm(p)
            ag1.start(p)
        get(o_gr)[pl.ds(pl.multiple_of(t * own, own), own), :] = get(h_og)[...]
        in_turn(ag1.arrivals(), wa.forwards())
        for p in range(parts):
            ag3.start(p)
        wa.arrived()

        def project(r):
            rows = pl.ds(r, 128)
            x = dot(h1[rows, :], wa_ref[:, : qw + 2 * kvw])
            x = turned(x, cos_ref[rows, :], sin_ref[rows, :])
            for h in range(n_q):
                q[h // group, r // 128, h % group * 128 : (h % group + 1) * 128, :] = lane_take(x, h * HD).astype(low)
            win[2, rows, :] = x[:, qw:].astype(low)

        per_tile(tiles, 128, project)

        def ahead(i):
            return remote(win.at[2], win.at[2 - i], get(h_ks).at[i - 1], get(h_kr).at[i - 1], {"dp": d + i})

        for i in (2, 1):
            when(d + i < nd, lambda: ahead(i).start())

        def unpack(b):
            def tile(r):
                x = win[b, pl.ds(r, 128), :].astype(f32)
                at = pl.ds(pl.multiple_of(b * span + r, 128), 128)
                for g in range(n_kv):
                    y = lane_take(x, g * HD)
                    k[g, at, :] = y.astype(low)
                    kt[g, :, at] = y.T.astype(low)
                    y = lane_take(x, kvw + g * HD)
                    v[g, at, :] = y.astype(low)
                    vt[g, :, at] = y.T.astype(low)

            per_tile(tiles, 128, tile)

        unpack(2)
        for i in (1, 2):

            @pl.when(d < i)
            def _():
                win[2 - i] = jnp.zeros((span, 2 * kvw), low)

            when(d >= i, lambda: ahead(i).wait_recv())
            unpack(2 - i)
        wd.start()
        wg.start()

        def attend(u, _):
            g, i = u // tiles, lax.rem(u, tiles)
            at = pl.multiple_of(i * 128, 128)
            keys = pl.ds(at, reach)
            s, seen = masked_scores(k[g, keys, :], q[g, i], at, begin_ref[:, pl.ds(at, 128)], span, group)
            s = jnp.where(seen, s, masked_score)
            top = jnp.max(s, axis=0, keepdims=True)
            e = jnp.exp(s - top)
            total = jnp.sum(e, axis=0, keepdims=True)
            p = (e * (1.0 / total)).astype(low)
            lse[g, i] = top + jnp.log(total)
            ch[g, i] = dot(vt[g, :, keys], p).T.astype(low)
            return 0

        half = max(1, n_kv * tiles // 2)
        arrive3 = ag3.arrivals()
        lax.fori_loop(0, half, attend, 0)
        cut = len(arrive3) // 2
        for x in arrive3[:cut]:
            x()
        lax.fori_loop(half, n_kv * tiles, attend, 0)
        for x in arrive3[cut:]:
            x()

        def pack(r):
            x = 0.0
            for h in range(n_q):
                at = h % group * 128
                x = x + lane_place(ch[h // group, r // 128, at : at + 128, :].astype(f32), h * HD, qw)
            ctx[pl.ds(r, 128), :] = x.astype(low)

        per_tile(tiles, 128, pack)

        def out_rows(j):
            rows = pl.ds(pl.multiple_of(j * own, own), own)
            for c in range(0, width, 512):
                part[rows, c : c + 512] = nt_dot(ctx[rows, :], wa_ref[c : c + 512, qw + 2 * kvw :])

        rs1.relay(0, out_rows)
        in_turn(wd.forwards(), wg.forwards())
        wu.start()
        out_rows(t)

        def second_norm(p):
            def put(r, x):
                at = pl.ds(p * piece + r, 16)
                x = x + tok[at, :].astype(f32)
                res[at, :] = x
                rows = pl.ds(pl.multiple_of(t * own + p * piece + r, 16), 16)
                h2[rows, :] = (x * inverse_rms(x) * g2[...]).astype(low)

            rs1.total(p, put)
            ag2.start(p)

        for p in range(parts):
            if p:
                rs1.relay(p)
            second_norm(p)
        in_turn(ag2.arrivals(), wu.forwards())
        for x in (wd, wg, wu):
            x.arrived()
        for x in (ag1, ag2, ag3, rs1, wa, wg, wu, wd):
            x.finish()
        for i in (2, 1):
            when(d + i < nd, lambda: ahead(i).wait_send())

    st.body(fn)
    return st.run()


def ffn_stage(nd, nt, hidden2, grad_rows, w_gate, w_up, w_down_t, residual, ffn_gain, out_grad):
    st = Fused("ffn", 2, nd, nt)
    low, f32 = jnp.bfloat16, jnp.float32
    span, width = hidden2.shape
    own = span // nt
    units = w_gate.shape[1]
    shard = width // nd
    parts = 2
    piece = own // parts
    tile_u = 256

    h_h2, h_gr, h_wg, h_wu, h_wd = (st.inp(x) for x in (hidden2, grad_rows, w_gate, w_up, w_down_t))
    h_res, h_gain, h_og = st.inp(residual), st.inp(ffn_gain[None]), st.inp(out_grad)
    o_ia = st.out((span, units), low)
    o_rl = st.out((span, width), low)
    o_rg = st.out((own, width), f32)
    o_fg = st.out((1, width), f32)
    o_dd = st.out((units, shard), f32)
    o_dg, o_du = (st.out((shard, units), f32) for _ in range(2))
    h_gl, h_ul = (st.scratch(VMEM((span, units), low)) for _ in range(2))
    h_part = st.scratch(VMEM((span, width), f32))
    h_ga, h_gb = (st.scratch(VMEM((width, units), f32)) for _ in range(2))
    rs = LineScatter(st, h_part, own, width, parts)
    ag = LineGather(st, o_rl, own, parts)
    sd, sg, su = ChipScatter(st, h_ga, shard, units), ChipScatter(st, h_gb, shard, units), ChipScatter(st, h_ga, shard, units)

    def fn(get):
        t = lax.axis_index("tp")
        for x in (rs, ag, sd, sg, su):
            x.bind(get)
        h2, gr, wg, wu, wd, res, gain, og = (get(h) for h in (h_h2, h_gr, h_wg, h_wu, h_wd, h_res, h_gain, h_og))
        ia, rl, rg, fg, gl, ul, part, ga, gb = (get(h) for h in (o_ia, o_rl, o_rg, o_fg, h_gl, h_ul, h_part, h_ga, h_gb))

        def act(c):
            cols = pl.ds(c, tile_u)
            gate = dot(h2[...], wg[:, cols])
            up = dot(h2[...], wu[:, cols])
            back = dot(gr[...], wd[:, cols])
            sig = jax.nn.sigmoid(gate)
            ia[:, cols] = (gate * sig * up).astype(low)
            gl[:, cols] = (back * up * (sig * (1.0 + gate * (1.0 - sig)))).astype(low)
            ul[:, cols] = (back * gate * sig).astype(low)

        per_tile(units // tile_u, tile_u, act)

        def rows_back(j):
            rows = pl.ds(pl.multiple_of(j * own, own), own)
            for c in range(0, width, 512):
                part[rows, c : c + 512] = nt_dot(gl[rows, :], wg[c : c + 512, :]) + nt_dot(ul[rows, :], wu[c : c + 512, :])

        blocks_w = width // 256

        def weight_part(dst, x, y, v):
            @pl.when(v < blocks_w)
            def _():
                cols = pl.ds(pl.multiple_of(v * 256, 256), 256)
                dst[cols, :] = tn_dot(x[:, cols], y[...])

        n = rs.slots()
        rs.relay(0, rows_back, lambda v: weight_part(ga, gr, ia, v))
        per_tile(max(0, blocks_w - n), 256, lambda r: weight_part(ga, gr, ia, n + r // 256))
        sd.give()
        rows_back(t)
        fg[...] = jnp.zeros_like(fg)

        def joined(p):
            def put(r, x):
                at = pl.ds(p * piece + r, 16)
                y = res[at, :]
                inverse = inverse_rms(y)
                normed = y * inverse
                fg[...] += jnp.sum(x * normed, axis=0, keepdims=True)
                e = x * gain[...]
                back = inverse * (e - normed * jnp.mean(e * normed, axis=-1, keepdims=True))
                y = og[at, :].astype(f32) + back
                rg[at, :] = y
                rl[pl.ds(pl.multiple_of(t * own + p * piece + r, 16), 16), :] = y.astype(low)

            rs.total(p, put)
            ag.start(p)

        joined(0)
        rs.relay(1, None, lambda v: weight_part(gb, h2, gl, v - n))
        per_tile(max(0, blocks_w - n), 256, lambda r: weight_part(gb, h2, gl, n + r // 256))
        sg.give()
        joined(1)
        arrivals = ag.arrivals()
        for x in sd.combines():
            x()
        for i in range(st.nd // 2):
            sd.gift(i).wait_send()
        for x in arrivals[:2]:
            x()

        def put_down(cols, x):
            get(o_dd)[cols, :] = x.T

        in_turn(sg.combines(), arrivals[2:])
        sd.total(put_down)
        per_tile(blocks_w, 256, lambda r: weight_part(ga, h2, ul, r // 256))
        su.give()

        def put_gate(cols, x):
            get(o_dg)[:, cols] = x

        def put_up(cols, x):
            get(o_du)[:, cols] = x

        for x in su.combines():
            x()
        sg.total(put_gate)
        su.total(put_up)
        for i in range(st.nd // 2 - 1):
            for c in sd.sums(i):
                c.wait_send()
        sg.finish()
        su.finish()
        rs.finish()
        ag.finish()

    st.body(fn)
    return st.run()


def back_stage(
    nd, nt, tokens, attn_gain, begin, cosine, sine, w_attn, w_down_t, inner_act, residual, residual_rows, residual_grad,
    ffn_part_sum, hidden1, queries, keys, values, keys_t, context, context_heads, log_total, heads,
):
    st = Fused("back", 3, nd, nt)
    low, f32 = jnp.bfloat16, jnp.float32
    own, width = tokens.shape
    span = own * nt
    shard = width // nd
    units = inner_act.shape[1]
    n_q, n_kv = heads
    group = n_q // n_kv
    tiles = span // 128
    qw, kvw = n_q * HD, n_kv * HD
    qkvw = qw + 2 * kvw
    reach = 2 * span + 128
    parts = 2
    piece = own // parts

    h_tok, h_gain, h_begin, h_cos, h_sin = (st.inp(x) for x in (tokens, attn_gain[None], begin, cosine, sine))
    h_wa, h_wd, h_ia, h_res, h_rl, h_rg = (
        st.inp(x) for x in (w_attn, w_down_t, inner_act, residual, residual_rows, residual_grad)
    )
    h_fg, h_h1, h_q, h_k, h_v, h_kt, h_ctx, h_ch, h_lse = (
        st.inp(x)
        for x in (ffn_part_sum, hidden1, queries, keys, values, keys_t, context, context_heads, log_total)
    )
    o_out = st.out((own, width), low)
    o_tg = st.out((own, width), f32)
    o_gains = st.out((1, 2 * width), f32)
    o_sum = st.out((shard, qkvw + qw), f32)
    h_fp = h_part = st.scratch(VMEM((span, width), f32))
    h_dc = st.scratch(VMEM((n_kv, tiles, group * 128, 128), low))
    h_delta = st.scratch(VMEM((n_kv, tiles, 1, group * 128), f32))
    h_dq = st.scratch(VMEM((n_kv, tiles, group * 128, 128), f32))
    h_dk, h_dv = (st.scratch(VMEM((n_kv, 3 * span, 128), f32)) for _ in range(2))
    h_kvs, h_kvr = (st.scratch(VMEM((2, span, 2 * kvw), jnp.int16)) for _ in range(2))
    h_kss, h_ksr = (st.scratch(VMEM((2, tiles, 1, 2 * kvw), f32)) for _ in range(2))
    h_kd = [st.scratch(DMA((2, 2))) for _ in range(2)]
    h_low = st.scratch(VMEM((span, qkvw), low))
    h_g = st.scratch(VMEM((width, qkvw + qw), f32))
    h_mine = st.scratch(VMEM((1, 2 * width), f32))
    rf = LineScatter(st, h_fp, own, width, parts)
    rs = LineScatter(st, h_part, own, width, parts)
    sa = ChipScatter(st, h_g, shard, qkvw + qw)
    full = FullSum(st, h_mine, o_gains, (1, 2 * width))
    st.links.add("near")

    def fn(get):
        d, t = lax.axis_index("dp"), lax.axis_index("tp")
        for x in (rf, rs, sa):
            x.bind(get)
        tok, gain, begin_ref, cos_ref, sin_ref = (get(h) for h in (h_tok, h_gain, h_begin, h_cos, h_sin))
        wa, wd, ia, res, rl, rg = (get(h) for h in (h_wa, h_wd, h_ia, h_res, h_rl, h_rg))
        h1, q, k, v, kt, ctx, ch, lse = (get(h) for h in (h_h1, h_q, h_k, h_v, h_kt, h_ctx, h_ch, h_lse))
        fp, part, dc, delta, dq, dk, dv = (get(h) for h in (h_fp, h_part, h_dc, h_delta, h_dq, h_dk, h_dv))
        kvs, kvr, kss, ksr, (ks, kr) = get(h_kvs), get(h_kvr), get(h_kss), get(h_ksr), (get(h) for h in h_kd)
        xl, gw, mine = get(h_low), get(h_g), get(h_mine)

        def context_back(r):
            rows = pl.ds(r, 128)
            x = dot(rl[rows, :], wa[:, qkvw:])
            i = r // 128
            for h in range(n_q):
                g, at = h // group, pl.ds(h % group * 128, 128)
                y = lane_take(x, h * HD).astype(low)
                dc[g, i, at, :] = y
                z = y.astype(f32) * ch[g, i, at, :].astype(f32)
                delta[g, i, :, at] = jnp.sum(z.T, axis=0, keepdims=True)

        per_tile(tiles, 128, context_back)

        def ffn_rows(r):
            cols = pl.ds(r, 512)
            fp[:, cols] = nt_dot(ia[...], wd[cols, :])

        per_tile(width // 512, 512, ffn_rows)
        dk[...] = jnp.zeros_like(dk)
        dv[...] = jnp.zeros_like(dv)
        count = n_kv * tiles
        slots = rf.slots() * parts
        per = -(-slots // count)

        def attend(u, _):
            def pump(w, _):
                pl.when(w < slots)(lambda: rf.step(w))
                return 0

            lax.fori_loop(u * per, u * per + per, pump, 0)
            g, i = u // tiles, lax.rem(u, tiles)
            at = pl.multiple_of(i * 128, 128)
            keys = pl.ds(at, reach)
            qq, dd = q[g, i], dc[g, i]
            s, seen = masked_scores(k[g, keys, :], qq, at, begin_ref[:, pl.ds(at, 128)], span, group)
            p = jnp.where(seen, jnp.exp(s - lse[g, i]), 0.0)
            ds = (p * (nt_dot(v[g, keys, :], dd) - delta[g, i])).astype(low)
            dv[g, keys, :] += dot(p.astype(low), dd)
            dk[g, keys, :] += dot(ds, qq)
            dq[g, i] = dot(kt[g, :, keys], ds).T
            return 0

        lax.fori_loop(0, count, attend, 0)
        scale = 1.0 / math.sqrt(HD)

        def kv_rows(b, r):
            at = pl.ds(pl.multiple_of(b * span + r, 128), 128)
            x = 0.0
            for g in range(n_kv):
                x = x + lane_place(dk[g, at, :] * scale, g * HD, 2 * kvw)
                x = x + lane_place(dv[g, at, :], kvw + g * HD, 2 * kvw)
            return x

        def back(i):
            where = {"dp": d - i}
            return (
                remote(kvs.at[i - 1], kvr.at[i - 1], ks.at[0, i - 1], kr.at[0, i - 1], where),
                remote(kss.at[i - 1], ksr.at[i - 1], ks.at[1, i - 1], kr.at[1, i - 1], where),
            )

        for i in (2, 1):

            @pl.when(d >= i)
            def _():
                def tile(r):
                    x = kv_rows(2 - i, r)
                    col_encode(x, kvs.at[i - 1, pl.ds(r, 128)], kss.at[i - 1, r // 128], slice(None))

                per_tile(tiles, 128, tile)
                for c in back(i):
                    c.start()

        def query_rows(r):
            rows = pl.ds(r, 128)
            x = 0.0
            for h in range(n_q):
                at = h % group * 128
                x = x + lane_place(dq[h // group, r // 128, at : at + 128, :] * scale, h * HD, qw)
            pad = jnp.zeros((128, 2 * kvw), f32)
            x = turned(jnp.concatenate([x, pad], axis=1), cos_ref[rows, :], -sin_ref[rows, :])
            xl[rows, :] = x.astype(low)

        per_tile(tiles, 128, query_rows)

        def put_out(p):
            def put(r, x):
                at = pl.ds(p * piece + r, 16)
                get(o_out)[at, :] = (res[at, :] + x).astype(low)

            rf.total(p, put)

        for p in range(parts):
            put_out(p)

        def weight_q(r):
            cols = pl.ds(r, 256)
            gw[cols, qkvw:] = tn_dot(rl[:, cols], ctx[...])

        per_tile(width // 256, 256, weight_q)
        for i in (1, 2):

            @pl.when(d + i < nd)
            def _():
                for c in back(i):
                    c.wait_recv()

        near1, near2 = d + 1 < nd, d + 2 < nd

        def kv_total(r):
            rows = pl.ds(r, 128)
            x = kv_rows(2, r)
            a = col_decode(kvr.at[0, rows], ksr.at[0, r // 128], slice(None))
            b = col_decode(kvr.at[1, rows], ksr.at[1, r // 128], slice(None))
            x = x + jnp.where(near1, a, 0.0) + jnp.where(near2, b, 0.0)
            pad = jnp.zeros((128, qw), f32)
            x = turned(jnp.concatenate([pad, x], axis=1), cos_ref[rows, :], -sin_ref[rows, :])
            xl[rows, qw:] = x[:, qw:].astype(low)

        per_tile(tiles, 128, kv_total)

        def hidden_rows(j):
            rows = pl.ds(pl.multiple_of(j * own, own), own)
            for c in range(0, width, 512):
                part[rows, c : c + 512] = nt_dot(xl[rows, :], wa[c : c + 512, :qkvw])

        blocks_w = width // 256

        def weight_part(v):
            @pl.when(v < blocks_w)
            def _():
                cols = pl.ds(pl.multiple_of(v * 256, 256), 256)
                gw[cols, :qkvw] = tn_dot(h1[:, cols], xl[...])

        n = rs.slots()
        rs.relay(0, hidden_rows, weight_part)
        per_tile(max(0, blocks_w - n), 256, lambda r: weight_part(n + r // 256))
        sa.give()
        hidden_rows(t)
        mine[...] = jnp.zeros_like(mine)
        mine[:, width:] = get(h_fg)[...]

        def last(p):
            def put(r, x):
                at = pl.ds(p * piece + r, 16)
                y = tok[at, :].astype(f32)
                inverse = inverse_rms(y)
                normed = y * inverse
                mine[:, :width] += jnp.sum(x * normed, axis=0, keepdims=True)
                e = x * gain[...]
                e = inverse * (e - normed * jnp.mean(e * normed, axis=-1, keepdims=True))
                get(o_tg)[at, :] = rg[at, :] + e

            rs.total(p, put)

        combines = sa.combines()
        combines[0]()
        last(0)
        for x in combines[1:]:
            x()
        rs.relay(1)
        last(1)
        full.run(get)

        def put_sum(cols, x):
            get(o_sum)[:, cols] = x

        sa.total(put_sum)
        for x in (rf, rs, sa):
            x.finish()
        for i in (2, 1):

            @pl.when(d >= i)
            def _():
                for c in back(i):
                    c.wait_send()

    st.body(fn)
    return st.run()


def rope_tables(position_ids, head_size):
    half_size = head_size // 2
    inverse = rope_base ** (-(jnp.arange(half_size, dtype=jnp.float32) * 2.0 / head_size))
    angles = position_ids.astype(jnp.float32)[:, None] * inverse[None, :]
    return (jnp.cos(angles), jnp.sin(angles))


def dot(a, b):
    return jnp.dot(a, b, preferred_element_type=jnp.float32)


def on_device(
    nd, nt, tokens, positions, attn_gain, w_query, w_key, w_value, w_out, ffn_gain, w_gate, w_up, w_down, out_grad
):
    span = tokens.shape[0] * nt
    width = tokens.shape[1]
    heads = (w_query.shape[1] // HD, w_key.shape[1] // HD)
    qw, kvw = w_query.shape[1], w_key.shape[1]
    w_attn = jnp.concatenate([w_query, w_key, w_value, w_out.T], axis=1)
    w_down_t = w_down.T
    cosine, sine = rope_tables(positions, HD)
    turn = heads[0] + heads[1]
    still = jnp.ones((span, kvw), jnp.float32)
    cosine = jnp.concatenate([jnp.tile(cosine, (1, 2 * turn)), still], axis=1)
    sine = jnp.concatenate([jnp.tile(jnp.concatenate([-sine, sine], axis=1), (1, turn)), 0.0 * still], axis=1)
    begin = (2 * span + jnp.arange(span, dtype=jnp.int32) - positions)[None]
    (hidden1, hidden2, grad_rows, attn_full, gate_full, up_full, down_full_t, queries, keys, values, keys_t, context, context_heads, log_total, residual) = (
        attention_stage(nd, nt, tokens, attn_gain, ffn_gain, out_grad, begin, cosine, sine, w_attn, w_gate, w_up, w_down_t, heads)
    )
    inner_act, residual_rows, residual_grad, ffn_gain_part, down_sum, gate_sum, up_sum = ffn_stage(
        nd, nt, hidden2, grad_rows, gate_full, up_full, down_full_t, residual, ffn_gain, out_grad
    )
    output, tokens_grad, gains, attn_sum = back_stage(
        nd, nt, tokens, attn_gain, begin, cosine, sine, attn_full, down_full_t, inner_act, residual, residual_rows,
        residual_grad, ffn_gain_part, hidden1, queries, keys, values, keys_t, context, context_heads, log_total, heads,
    )
    cuts = (qw, qw + kvw, qw + 2 * kvw)
    return (
        output,
        tokens_grad,
        gains[0, :width],
        attn_sum[:, : cuts[0]],
        attn_sum[:, cuts[0] : cuts[1]],
        attn_sum[:, cuts[1] : cuts[2]],
        attn_sum[:, cuts[2] :].T,
        gains[0, width:],
        gate_sum,
        up_sum,
        down_sum,
    )


def solution(mesh):
    return jax.shard_map(
        functools.partial(on_device, mesh.shape["dp"], mesh.shape["tp"]),
        mesh=mesh,
        in_specs=(
            P(("dp", "tp"), None),
            P("dp"),
            P(),
            P("dp", "tp"),
            P("dp", "tp"),
            P("dp", "tp"),
            P("tp", "dp"),
            P(),
            P("dp", "tp"),
            P("dp", "tp"),
            P("tp", "dp"),
            P(("dp", "tp"), None),
        ),
        out_specs=(
            P(("dp", "tp"), None),
            P(("dp", "tp"), None),
            P(),
            P("dp", "tp"),
            P("dp", "tp"),
            P("dp", "tp"),
            P("tp", "dp"),
            P(),
            P("dp", "tp"),
            P("dp", "tp"),
            P("tp", "dp"),
        ),
        check_vma=False,
    )
```

```python
import functools
import math

import jax
import jax.numpy as jnp
from jax import lax
from jax.experimental import pallas as pl
from jax.experimental.pallas import tpu as pltpu
from jax.sharding import PartitionSpec as P

HD = 96
norm_eps = 1e-05
rope_base = 100000.0
masked_score = -1e30

MESH = pl.DeviceIdType.MESH
VMEM = pltpu.VMEM
DMA = pltpu.SemaphoreType.DMA
LEVELS = 32000.0


class Stage:
    def __init__(self, name, cid, nd, nt):
        self.name, self.cid, self.nd, self.nt = name, cid, nd, nt
        self.ins, self.outs, self.scr, self.tasks, self.links = [], [], [], [], set()

    def inp(self, x, space=VMEM):
        self.ins.append((x, space))
        return ("i", len(self.ins) - 1)

    def out(self, shape, dtype, space=VMEM):
        self.outs.append((shape, dtype, space))
        return ("o", len(self.outs) - 1)

    def scratch(self, spec):
        self.scr.append(spec)
        return ("s", len(self.scr) - 1)

    def task(self, links, gen):
        self.links |= set(links)
        self.tasks.append(gen)

    def _barrier(self):
        d, t = lax.axis_index("dp"), lax.axis_index("tp")
        nd, nt = self.nd, self.nt
        sem = pltpu.get_barrier_semaphore()
        count = 0

        def greet(ok, where):
            if ok is True:
                pl.semaphore_signal(sem, inc=1, device_id=where, device_id_type=MESH)
                return 1

            @pl.when(ok)
            def _():
                pl.semaphore_signal(sem, inc=1, device_id=where, device_id_type=MESH)

            return ok.astype(jnp.int32)

        if "line" in self.links:
            count += greet(t > 0, {"tp": t - 1})
            count += greet(t < nt - 1, {"tp": t + 1})
        if "chips" in self.links:
            for i in range(1, nd // 2):
                count += greet(True, {"dp": lax.rem(d + 2 * i, nd)})
        if "twin" in self.links:
            count += greet(True, {"dp": d + 1 - 2 * lax.rem(d, 2)})
        if "near" in self.links:
            for i in (1, 2):
                count += greet(d >= i, {"dp": d - i})
                count += greet(d < nd - i, {"dp": d + i})
        if "tp" in self.links:
            for i in range(1, nt):
                count += greet(True, {"tp": lax.rem(t + i, nt)})
        if "dp" in self.links:
            for i in range(1, nd):
                count += greet(True, {"dp": lax.rem(d + i, nd)})
        pl.semaphore_wait(sem, count)

    def run(self):
        n_in, n_out = len(self.ins), len(self.outs)

        def kernel(*refs):
            def get(h):
                kind, i = h
                return refs[i + {"i": 0, "o": n_in, "s": n_in + n_out}[kind]]

            self._barrier()
            live = [g(get) for g in self.tasks]
            while live:
                still = []
                for g in live:
                    try:
                        next(g)
                        still.append(g)
                    except StopIteration:
                        pass
                live = still

        return pl.pallas_call(
            kernel,
            out_shape=[jax.ShapeDtypeStruct(s, t) for s, t, _ in self.outs],
            in_specs=[pl.BlockSpec(memory_space=sp) for _, sp in self.ins],
            out_specs=[pl.BlockSpec(memory_space=sp) for _, _, sp in self.outs],
            scratch_shapes=self.scr,
            compiler_params=pltpu.CompilerParams(
                collective_id=self.cid, has_side_effects=True, vmem_limit_bytes=67_000_000
            ),
            name=self.name,
        )(*[x for x, _ in self.ins])


def remote(src, dst, send, recv, where):
    return pltpu.make_async_remote_copy(
        src_ref=src, dst_ref=dst, send_sem=send, recv_sem=recv, device_id=where, device_id_type=MESH
    )


def when(ok, fn):
    if ok is True:
        fn()
    elif ok is not False:
        pl.when(ok)(fn)


def over_cols(width, fn):
    def body(c, _):
        fn(pl.ds(pl.multiple_of(c * 128, 128), 128))
        return 0

    lax.fori_loop(0, width // 128, body, 0)
    if width % 128:
        fn(pl.ds(width // 128 * 128, width % 128))


def row_encode(read, code, scale, rows):
    step = 16

    def body(i, held):
        r = pl.multiple_of(i * step, step)
        x = read(r, step)
        top = jnp.max(jnp.abs(x), axis=-1, keepdims=True)
        code[pl.ds(r, step), :] = jnp.round(x * (LEVELS / jnp.maximum(top, 1e-30))).astype(jnp.int32).astype(jnp.int16)
        lane = lax.broadcasted_iota(jnp.int32, (step, 128), 1)
        row = lax.broadcasted_iota(jnp.int32, (step, 128), 0) + r
        mine = jnp.sum(jnp.where(lane == row, jnp.maximum(top, 1e-30) * (1.0 / LEVELS), 0.0), axis=0, keepdims=True)
        return held + jnp.broadcast_to(mine, (8, 128))

    scale[...] = lax.fori_loop(0, rows // step, body, jnp.zeros((8, 128), jnp.float32))


def row_decode(code, scale, r, step):
    lane = lax.broadcasted_iota(jnp.int32, (step, 128), 1)
    row = lax.broadcasted_iota(jnp.int32, (step, 128), 0) + r
    col = jnp.sum(jnp.where(lane == row, jnp.broadcast_to(scale[0:1, :], (step, 128)), 0.0), axis=-1, keepdims=True)
    return code[pl.ds(r, step), :].astype(jnp.int32).astype(jnp.float32) * col


def col_encode(x, code, scale, cols):
    top = jnp.maximum(jnp.max(jnp.abs(x), axis=0, keepdims=True), 1e-30)
    code[:, cols] = jnp.round(x * (LEVELS / top)).astype(jnp.int32).astype(jnp.int16)
    scale[:, cols] = top * (1.0 / LEVELS)


def col_decode(code, scale, cols):
    return code[:, cols].astype(jnp.int32).astype(jnp.float32) * scale[:, cols]


class LineGather:
    def __init__(self, st, full, rows, parts):
        self.st, self.full, self.rows, self.parts = st, full, rows, parts
        self.hs = st.scratch(DMA((2, st.nt, parts)))
        self.hr = st.scratch(DMA((2, st.nt, parts)))
        st.links.add("line")

    def bind(self, get):
        self.ref, self.ss, self.rs = get(self.full), get(self.hs), get(self.hr)
        self.t = lax.axis_index("tp")
        return self

    def piece(self, owner, p):
        chunk = self.rows // self.parts
        return self.ref.at[pl.ds(pl.multiple_of(owner * self.rows + p * chunk, chunk), chunk)]

    def hop(self, owner, k, s, p, where):
        at = self.piece(owner, p)
        return remote(at, at, self.ss.at[k, s, p], self.rs.at[k, s, p], {"tp": where})

    def _send(self, s, p, k, way):
        nt, t = self.st.nt, self.t
        owner, where = t - s * way, t + way
        ok = (owner >= 0) & (owner < nt) & (where >= 0) & (where < nt)
        when(ok, lambda: self.hop(owner, k, s, p, where).start())

    def start(self, p):
        for k, way in enumerate((1, -1)):
            self._send(0, p, k, way)

    def arrive(self, s, p):
        nt, t = self.st.nt, self.t
        for k, way in enumerate((1, -1)):
            owner = t - way * (s + 1)
            ok = (owner >= 0) & (owner < nt)
            when(ok, lambda: self.hop(owner, k, s, p, t).wait_recv())
            if s < nt - 2:
                self._send(s + 1, p, k, way)

    def arrive_at(self, v):
        nt, t = self.st.nt, self.t
        s, p = v // self.parts, lax.rem(v, self.parts)
        for k, way in enumerate((1, -1)):
            owner = t - way * (s + 1)
            ok = (owner >= 0) & (owner < nt) & (s < nt - 1)
            where = t + way

            @pl.when(ok)
            def _():
                self.hop(owner, k, s, p, t).wait_recv()
                when((where >= 0) & (where < nt) & (s < nt - 2), lambda: self.hop(owner, k, s + 1, p, where).start())

    def arrivals(self):
        return [
            functools.partial(self.arrive, s, p) for s in range(self.st.nt - 1) for p in range(self.parts)
        ]

    def finish(self):
        nt, t = self.st.nt, self.t
        for s in range(nt - 1):
            for p in range(self.parts):
                for k, way in enumerate((1, -1)):
                    owner, where = t - s * way, t + way
                    ok = (owner >= 0) & (owner < nt) & (where >= 0) & (where < nt)
                    when(ok, lambda: self.hop(owner, k, s, p, where).wait_send())


class LineScatter:
    def __init__(self, st, part, rows, width, parts):
        self.st, self.part, self.rows, self.width, self.parts = st, part, rows, width, parts
        nt = st.nt
        self.chunk = rows // parts
        shape = (2, (nt - 1) * parts, self.chunk, width)
        self.kept = min(2, nt - 1) * parts
        few = (2, self.kept, self.chunk, width)
        self.hc = [st.scratch(VMEM(x, jnp.int16)) for x in (few, shape)]
        self.hk = [st.scratch(VMEM(x[:2] + (8, 128), jnp.float32)) for x in (few, shape)]
        self.hd = [st.scratch(DMA((2, 2, (nt - 1) * parts))) for _ in range(2)]
        st.links.add("line")

    def bind(self, get):
        self.x = get(self.part)
        (self.cs, self.cr), (self.sc, self.sr), (self.ss, self.rs) = (
            [get(h) for h in hs] for hs in (self.hc, self.hk, self.hd)
        )
        self.t = lax.axis_index("tp")
        return self

    def hops(self, k, u, where):
        w = lax.rem(u, self.kept)
        return (
            remote(self.cs.at[k, w], self.cr.at[k, u], self.ss.at[0, k, u], self.rs.at[0, k, u], {"tp": where}),
            remote(self.sc.at[k, w], self.sr.at[k, u], self.ss.at[1, k, u], self.rs.at[1, k, u], {"tp": where}),
        )

    def _rows(self, base, r, n):
        return self.x[pl.ds(pl.multiple_of(base + r, n), n), :]

    def slots(self):
        return 4 * (self.st.nt - 1)

    def step(self, v, produce=None):
        nt, t, chunk = self.st.nt, self.t, self.chunk
        p, v = v // self.slots(), lax.rem(v, self.slots())
        k = lax.rem(v, 2)
        s = v // 2 - jnp.where(k == 0, t, nt - 1 - t)
        j = jnp.where(k == 0, nt - 1 - s, s)
        way = 1 - 2 * k
        u = s * self.parts + p
        first = t == jnp.where(k == 0, 0, nt - 1)
        passing = (s >= 0) & (s < nt - 1) & jnp.where(k == 0, t < j, t > j)

        @pl.when(passing)
        def _():
            if produce is not None:
                pl.when(p == 0)(lambda: produce(j))

            @pl.when(first)
            def _():
                self.cr[k, u] = jnp.zeros((chunk, self.width), jnp.int16)
                self.sr[k, u] = jnp.zeros((8, 128), jnp.float32)

            @pl.when(jnp.logical_not(first))
            def _():
                for c in self.hops(k, u, t):
                    c.wait_recv()

            @pl.when(u >= self.kept)
            def _():
                for c in self.hops(k, u - self.kept, t + way):
                    c.wait_send()

            base, w = j * self.rows + p * chunk, lax.rem(u, self.kept)
            row_encode(
                lambda r, n: self._rows(base, r, n) + row_decode(self.cr.at[k, u], self.sr.at[k, u], r, n),
                self.cs.at[k, w],
                self.sc.at[k, w],
                chunk,
            )
            for c in self.hops(k, u, t + way):
                c.start()

    def relay(self, p, produce=None, beside=None):
        n = self.slots()

        def one(v, _):
            self.step(v, produce)
            if beside is not None:
                beside(v)
            return 0

        lax.fori_loop(p * n, (p + 1) * n, one, 0)

    def total(self, p, put):
        nt, t, chunk = self.st.nt, self.t, self.chunk
        right, left = (nt - 1 - t) * self.parts + p, t * self.parts + p
        from_left, from_right = t > 0, t < nt - 1

        @pl.when(from_left)
        def _():
            for c in self.hops(0, right, t):
                c.wait_recv()

        @pl.when(from_right)
        def _():
            for c in self.hops(1, left, t):
                c.wait_recv()

        at_r = jnp.where(from_left, right, 0)
        at_l = jnp.where(from_right, left, 0)
        base = t * self.rows + p * chunk

        def body(i, _):
            r = pl.multiple_of(i * 16, 16)
            x = self._rows(base, r, 16)
            a = row_decode(self.cr.at[0, at_r], self.sr.at[0, at_r], r, 16)
            b = row_decode(self.cr.at[1, at_l], self.sr.at[1, at_l], r, 16)
            put(r, x + jnp.where(from_left, a, 0.0) + jnp.where(from_right, b, 0.0))
            return 0

        lax.fori_loop(0, chunk // 16, body, 0)

    def finish(self):
        nt, t = self.st.nt, self.t

        def step(v, _):
            s, k = v // 2, lax.rem(v, 2)
            j = jnp.where(k == 0, nt - 1 - s, s)
            later = s + self.kept // self.parts
            i = jnp.where(k == 0, nt - 1 - later, later)
            waited = (later < nt - 1) & jnp.where(k == 0, t < i, t > i)

            @pl.when(jnp.where(k == 0, t < j, t > j) & jnp.logical_not(waited))
            def _():
                for p in range(self.parts):
                    for c in self.hops(k, s * self.parts + p, t + 1 - 2 * k):
                        c.wait_send()

            return 0

        lax.fori_loop(0, 2 * (nt - 1), step, 0)


class ChipGather:
    def __init__(self, st, w, full, rows):
        self.st, self.w, self.full, self.rows = st, w, full, rows
        self.hs = st.scratch(DMA((st.nd,)))
        self.hr = st.scratch(DMA((st.nd,)))
        self.hl = st.scratch(DMA((1,)))
        st.links |= {"chips", "twin"}

    def bind(self, get):
        self.x, self.o, self.ss, self.rs, ls = (get(h) for h in (self.w, self.full, self.hs, self.hr, self.hl))
        nd = self.st.nd
        d = lax.axis_index("dp")
        twin = {"dp": d + 1 - 2 * lax.rem(d, 2)}
        nc = nd // 2

        def at(i):
            return self.o.at[pl.ds(pl.multiple_of(i * self.rows, self.rows), self.rows)]

        self.own = lambda: pltpu.make_async_copy(self.x, at(d), ls.at[0])
        self.out = lambda i: remote(self.x, at(d), self.ss.at[i], self.rs.at[i], {"dp": lax.rem(d + 2 * i, nd)})

        def fwd(i):
            src = self.x if i == 0 else at(lax.rem(d - 2 * i + nd, nd))
            dst = at(lax.rem(d - 2 * i + nd, nd))
            j = 0 if i == 0 else nc + i
            return remote(src, dst, self.ss.at[j], self.rs.at[j], twin)

        self.fwd, self.nc = fwd, nc
        return self

    def start(self):
        for i in range(1, self.nc):
            self.out(i).start()
        self.fwd(0).start()
        self.own().start()

    def forward(self, i):
        self.out(i).wait_recv()
        self.fwd(i).start()

    def forwards(self):
        return [functools.partial(self.forward, i) for i in range(1, self.nc)]

    def arrived(self):
        for i in range(self.nc):
            self.fwd(i).wait_recv()
        self.own().wait()

    def finish(self):
        for i in range(self.nc):
            self.fwd(i).wait_send()
        for i in range(1, self.nc):
            self.out(i).wait_send()


class GradScatter:
    def __init__(self, st, shard, widths, sums):
        nc = self.nc = st.nd // 2
        self.st, self.shard, self.widths = st, shard, widths
        self.m = math.lcm(2 * shard, 128) // (2 * shard)
        self.chunks = nc // self.m
        wide = max(widths)
        self.hg = st.scratch(VMEM((2, 2 * self.m * shard, wide), jnp.float32))
        self.ht = st.scratch(VMEM((2, self.m, shard, wide), jnp.float32))
        self.hs = st.scratch(VMEM((2, self.m, shard, wide), jnp.int16))
        self.hk = st.scratch(VMEM((2, self.m, 1, wide), jnp.float32))
        self.hcr = [st.scratch(VMEM((nc - 1, shard, w), jnp.int16)) for w in widths]
        self.hkr = [st.scratch(VMEM((nc - 1, 1, w), jnp.float32)) for w in widths]
        self.ha = sums
        self.hgs = [st.scratch(DMA((2, self.m))) for _ in range(2)]
        self.hss = st.scratch(DMA((2, 2, self.m)))
        self.hsr = st.scratch(DMA((len(widths), 2, nc - 1)))
        self.hf = st.scratch(pltpu.SemaphoreType.REGULAR)
        st.links |= {"chips", "twin"}

    def bind(self, get):
        self.g, self.t, self.cs, self.sc, self.ss, self.sr, self.free = (
            get(h) for h in (self.hg, self.ht, self.hs, self.hk, self.hss, self.hsr, self.hf)
        )
        self.cr, self.kr, self.acc = ([get(h) for h in hs] for hs in (self.hcr, self.hkr, self.ha))
        self.gs, self.gr = (get(h) for h in self.hgs)
        d = self.d = lax.axis_index("dp")
        self.core, self.chip = lax.rem(d, 2), d // 2
        self.twin = {"dp": d + 1 - 2 * self.core}
        return self

    def chunk(self, i):
        return lax.rem(self.chip // self.m + 1 + i, self.chunks)

    def half(self, e, core):
        return pl.ds(pl.multiple_of((2 * e + core) * self.shard, self.shard), self.shard)

    def gift(self, a, r, e):
        cols = pl.ds(0, self.widths[a])
        return remote(
            self.g.at[r, self.half(e, 1 - self.core), cols], self.t.at[r, e, :, cols], self.gs.at[r, e], self.gr.at[r, e],
            self.twin,
        )

    def sums(self, a, r, e, dest):
        cols, nc = pl.ds(0, self.widths[a]), self.nc
        slot = jnp.maximum(lax.rem(dest - self.chip + nc, nc) - 1, 0)
        where = {"dp": 2 * dest + self.core}
        return (
            remote(self.cs.at[r, e, :, cols], self.cr[a].at[slot], self.ss.at[0, r, e], self.sr.at[a, 0, slot], where),
            remote(self.sc.at[r, e, :, cols], self.kr[a].at[slot], self.ss.at[1, r, e], self.sr.at[a, 1, slot], where),
        )

    def compute(self, a, i, pieces):
        n = a * self.chunks + i
        r = lax.rem(n, 2)
        rows = 2 * self.m * self.shard

        @pl.when(n >= 2)
        def _():
            for e in range(self.m):
                self.gift(a, r, e).wait_send() if a == 0 else self._sent(a, i, r, e)
            pl.semaphore_wait(self.free, 1)

        cols = pl.ds(pl.multiple_of(self.chunk(i) * rows, 128), rows)
        at = 0
        for x, y in pieces:
            z = y()
            self.g[r, :, at : at + z.shape[1]] = tn_dot(x[:, cols], z)
            at += z.shape[1]
        for e in range(self.m):
            self.gift(a, r, e).start()

    def _sent(self, a, i, r, e):
        pl.when(i >= 2)(lambda: self.gift(a, r, e).wait_send())
        pl.when(i < 2)(lambda: self.gift(a - 1, r, e).wait_send())

    def combine(self, a, i):
        n = a * self.chunks + i
        r = lax.rem(n, 2)
        for e in range(self.m):
            self.gift(a, r, e).wait_recv()
            dest = self.chunk(i) * self.m + e
            away = dest != self.chip

            def past(b, j):
                old = self.chunk(j) * self.m + e

                @pl.when(old != self.chip)
                def _():
                    for c in self.sums(b, r, e, old):
                        c.wait_send()

            pl.when(i >= 2)(lambda: past(a, i - 2))
            if a:
                pl.when(i < 2)(lambda: past(a - 1, i - 2 + self.chunks))
            own = self.half(e, self.core)

            @pl.when(away)
            def _():
                over_cols(
                    self.widths[a],
                    lambda cols: col_encode(
                        self.g[r, own, cols] + self.t[r, e, :, cols], self.cs.at[r, e], self.sc.at[r, e], cols
                    ),
                )
                for c in self.sums(a, r, e, dest):
                    c.start()

            @pl.when(jnp.logical_not(away))
            def _():
                over_cols(self.widths[a], lambda cols: self._keep(a, r, e, own, cols))

        @pl.when(n + 2 < len(self.widths) * self.chunks)
        def _():
            pl.semaphore_signal(self.free, inc=1, device_id=self.twin, device_id_type=MESH)

    def _keep(self, a, r, e, own, cols):
        self.acc[a][:, cols] = self.g[r, own, cols] + self.t[r, e, :, cols]

    def slot(self, a, w, pieces):
        pl.when(w < self.chunks)(lambda: self.compute(a, w, pieces))
        pl.when((w >= 1) & (w <= self.chunks))(lambda: self.combine(a, w - 1))

    def collect(self, a, put):
        n = self.nc - 1
        for i in range(n):
            for c in self.sums(a, 0, 0, lax.rem(self.chip + 1 + i, self.nc)):
                c.wait_recv()

        def tile(cols):
            x = self.acc[a][:, cols]
            for i in range(n):
                x = x + col_decode(self.cr[a].at[i], self.kr[a].at[i], cols)
            put(cols, x)

        over_cols(self.widths[a], tile)

    def finish(self):
        a = len(self.widths) - 1
        for i in range(max(0, self.chunks - 2), self.chunks):
            r = (a * self.chunks + i) % 2
            for e in range(self.m):
                self.gift(a, r, e).wait_send()
                dest = self.chunk(i) * self.m + e

                @pl.when(dest != self.chip)
                def _():
                    for c in self.sums(a, r, e, dest):
                        c.wait_send()


class FullSum:
    def __init__(self, st, x, out, shape):
        self.st, self.x, self.out = st, x, out
        self.ha = st.scratch(VMEM((st.nt,) + shape, jnp.float32))
        self.hm = st.scratch(VMEM(shape, jnp.float32))
        self.hb = st.scratch(VMEM((st.nd,) + shape, jnp.float32))
        self.hs = st.scratch(DMA((2, max(st.nd, st.nt))))
        self.hr = st.scratch(DMA((2, max(st.nd, st.nt))))
        st.links |= {"tp", "dp"}

    def run(self, get):
        nd, nt = self.st.nd, self.st.nt
        x, o, a, m, b, ss, rs = (get(h) for h in (self.x, self.out, self.ha, self.hm, self.hb, self.hs, self.hr))
        for k, (axis, n, src, got, dst) in enumerate((("tp", nt, x, a, m), ("dp", nd, m, b, o))):
            me = lax.axis_index(axis)
            cs = [
                remote(src, got.at[me], ss.at[k, i], rs.at[k, i], {axis: lax.rem(me + i, n)}) for i in range(1, n)
            ]
            for c in cs:
                c.start()
            got[me] = src[...]
            for c in cs:
                c.wait()
            total = got[0]
            for i in range(1, n):
                total = total + got[i]
            dst[...] = total


def lane_take(x, offset):
    base = offset // 128 * 128
    wide = min(256, x.shape[-1] - base)
    slab = x[:, base : base + wide]
    if wide % 128:
        slab = jnp.concatenate([slab, jnp.zeros((x.shape[0], -wide % 128), x.dtype)], axis=1)
        wide = slab.shape[-1]
    if offset > base:
        slab = pltpu.roll(slab, wide - (offset - base), 1)
    slab = slab[:, :128]
    return jnp.where(lax.broadcasted_iota(jnp.int32, slab.shape, 1) < HD, slab, 0.0)


def lane_place(x, offset, width):
    base = offset // 128 * 128
    wide = min(256, width - base)
    slab = x if wide == 128 else jnp.concatenate([x, jnp.zeros_like(x)], axis=1)
    if offset > base:
        slab = pltpu.roll(slab, offset - base, 1)
    slab = slab[:, :wide]
    pieces = []
    if base:
        pieces.append(jnp.zeros((x.shape[0], base), x.dtype))
    pieces.append(slab)
    if base + wide < width:
        pieces.append(jnp.zeros((x.shape[0], width - base - wide), x.dtype))
    return jnp.concatenate(pieces, axis=1) if len(pieces) > 1 else slab


def turned(u, cosine, sine):
    wide = u.shape[-1]
    lane = lax.rem(lax.broadcasted_iota(jnp.int32, u.shape, 1), HD)
    swap = jnp.where(lane < HD // 2, pltpu.roll(u, wide - HD // 2, 1), pltpu.roll(u, HD // 2, 1))
    return u * cosine + swap * sine


def nt_dot(a, b):
    return lax.dot_general(a, b, (((1,), (1,)), ((), ())), preferred_element_type=jnp.float32)


def per_tile(count, size, fn):
    def body(i, _):
        fn(pl.multiple_of(i * size, size))
        return 0

    lax.fori_loop(0, count, body, 0)


def in_turn(*lists):
    for i in range(max(len(x) for x in lists)):
        for x in lists:
            if i < len(x):
                x[i]()


class Fused(Stage):
    def body(self, fn):
        self.tasks = [lambda get: iter(fn(get) or ())]


def inverse_rms(x):
    return lax.rsqrt(jnp.mean(x * x, axis=-1, keepdims=True) + norm_eps)


def tn_dot(a, b):
    return lax.dot_general(a, b, (((0,), (0,)), ((), ())), preferred_element_type=jnp.float32)


def across(x, count):
    return jnp.concatenate([x] * count, axis=1) if count > 1 else x


def masked_scores(keys, queries, first, begin, span, group):
    s = nt_dot(keys, queries) * (1.0 / math.sqrt(HD))
    key = lax.broadcasted_iota(jnp.int32, s.shape, 0) + first
    own = lax.rem(lax.broadcasted_iota(jnp.int32, s.shape, 1), 128) + (first + 2 * span)
    return s, (key >= across(begin, group)) & (key <= own)


def layer(
    nd, nt, tokens, attn_gain, ffn_gain, out_grad, begin, cosine, sine, w_attn, w_gate, w_up, w_down_t, heads
):
    st = Fused("layer", 1, nd, nt)
    low, f32 = jnp.bfloat16, jnp.float32
    own, width = tokens.shape
    span = own * nt
    shard, units = w_gate.shape
    n_q, n_kv = heads
    group = n_q // n_kv
    tiles = span // 128
    qw, kvw = n_q * HD, n_kv * HD
    qkvw = qw + 2 * kvw
    reach = 2 * span + 128
    parts = 2
    piece = own // parts
    scale = 1.0 / math.sqrt(HD)

    h_tok, h_g1, h_g2 = st.inp(tokens), st.inp(attn_gain[None]), st.inp(ffn_gain[None])
    h_og, h_begin = st.inp(out_grad), st.inp(begin)
    h_cos, h_sin = st.inp(cosine), st.inp(sine)
    s_wa, s_wg, s_wu, s_wd = (st.inp(w, pl.ANY) for w in (w_attn, w_gate, w_up, w_down_t))

    o_out = st.out((own, width), low)
    o_tg = st.out((own, width), f32)
    o_gains = st.out((1, 2 * width), f32)
    o_dd = st.out((units, shard), f32)
    o_dg, o_du = (st.out((shard, units), f32) for _ in range(2))
    o_da = st.out((shard, qkvw + qw), f32)

    def room(shape, dtype=f32):
        return st.scratch(VMEM(shape, dtype))

    h_h1, h_h2, h_gr, h_rl = (room((span, width), low) for _ in range(4))
    h_wa = room((width, qkvw + qw), low)
    h_wg, h_wu, h_wd = (room((width, units), low) for _ in range(3))
    h_q, h_dc, h_ch = (room((n_kv, tiles, group * 128, 128), low) for _ in range(3))
    h_k, h_v = (room((n_kv, 3 * span, 128), low) for _ in range(2))
    h_kt, h_vt = (room((n_kv, 128, 3 * span), low) for _ in range(2))
    h_win = room((3, span, 2 * kvw), low)
    h_ctx = room((span, qw), low)
    h_lse, h_delta = (room((n_kv, tiles, 1, group * 128)) for _ in range(2))
    h_res, h_rg = (room((own, width)) for _ in range(2))
    h_part = room((span, width))
    h_ia, h_gl, h_ul = (room((span, units), low) for _ in range(3))
    h_dq = room((n_kv, tiles, group * 128, 128))
    h_dk, h_dv = (room((n_kv, 3 * span, 128)) for _ in range(2))
    h_kvs, h_kvr = (room((2, span, 2 * kvw), jnp.int16) for _ in range(2))
    h_kss, h_ksr = (room((2, tiles, 1, 2 * kvw)) for _ in range(2))
    h_mine = room((1, 2 * width))
    h_fs, h_fr = (st.scratch(DMA((2,))) for _ in range(2))
    h_bs, h_br = (st.scratch(DMA((2, 2))) for _ in range(2))
    h_ready = st.scratch(pltpu.SemaphoreType.REGULAR)

    ag1 = LineGather(st, h_h1, own, parts)
    ag2 = LineGather(st, h_h2, own, parts)
    ag3 = LineGather(st, h_gr, own, parts)
    ag4 = LineGather(st, h_rl, own, parts)
    rs = LineScatter(st, h_part, own, width, parts)
    wa = ChipGather(st, s_wa, h_wa, shard)
    wg = ChipGather(st, s_wg, h_wg, shard)
    wu = ChipGather(st, s_wu, h_wu, shard)
    wd = ChipGather(st, s_wd, h_wd, shard)
    gs = GradScatter(st, shard, (units, units, units, qkvw + qw), (room((shard, units)), o_dg, o_du, o_da))
    full = FullSum(st, h_mine, o_gains, (1, 2 * width))
    st.links.add("near")

    def fn(get):
        d, t = lax.axis_index("dp"), lax.axis_index("tp")
        for x in (ag1, ag2, ag3, ag4, rs, wa, wg, wu, wd, gs):
            x.bind(get)
        tok, g1, g2, og, begin_ref, cos_ref, sin_ref = (get(h) for h in (h_tok, h_g1, h_g2, h_og, h_begin, h_cos, h_sin))
        h1, h2, gr, rl = (get(h) for h in (h_h1, h_h2, h_gr, h_rl))
        wa_ref, wg_ref, wu_ref, wd_ref = (get(h) for h in (h_wa, h_wg, h_wu, h_wd))
        q, k, v, kt, vt, win, ctx, ch, lse = (get(h) for h in (h_q, h_k, h_v, h_kt, h_vt, h_win, h_ctx, h_ch, h_lse))
        dc, delta, dq, dk, dv = (get(h) for h in (h_dc, h_delta, h_dq, h_dk, h_dv))
        res, rg, part, ia, gl, ul, mine = (get(h) for h in (h_res, h_rg, h_part, h_ia, h_gl, h_ul, h_mine))
        xl = ul.at[:, pl.ds(0, qkvw)]
        kvs, kvr, kss, ksr, fs, fr, bs, br = (
            get(h) for h in (h_kvs, h_kvr, h_kss, h_ksr, h_fs, h_fr, h_bs, h_br)
        )

        def own_rows(p, r, n=16):
            return pl.ds(pl.multiple_of(t * own + p * piece + r, n), n)

        def rows_of(j):
            return pl.ds(pl.multiple_of(j * own, own), own)

        wa.start()
        for p in range(parts):

            def tile(r):
                x = tok[pl.ds(p * piece + r, 16), :].astype(f32)
                h1[own_rows(p, r), :] = (x * inverse_rms(x) * g1[...]).astype(low)

            per_tile(piece // 16, 16, tile)
            ag1.start(p)
        gr[rows_of(t), :] = og[...]
        in_turn(ag1.arrivals(), wa.forwards())
        for p in range(parts):
            ag3.start(p)
        wa.arrived()

        def turn_rows(x, rows, way):
            cosine, sine = across(cos_ref[rows, :], 2), across(sin_ref[rows, :], 2)
            lane = lax.broadcasted_iota(jnp.int32, x.shape, 1)
            return jnp.where(lane < qw + kvw, turned(x, cosine, way * sine), x)

        def project(r):
            rows = pl.ds(r, 128)
            x = turn_rows(dot(h1[rows, :], wa_ref[:, :qkvw]), rows, 1.0)
            for h in range(n_q):
                q[h // group, r // 128, h % group * 128 : (h % group + 1) * 128, :] = lane_take(x, h * HD).astype(low)
            win[2, rows, :] = x[:, qw:].astype(low)

        per_tile(tiles, 128, project)

        def ahead(i):
            return remote(win.at[2], win.at[2 - i], fs.at[i - 1], fr.at[i - 1], {"dp": d + i})

        for i in (2, 1):
            when(d + i < nd, lambda: ahead(i).start())

        def unpack(b):
            def tile(r):
                x = win[b, pl.ds(r, 128), :].astype(f32)
                at = pl.ds(pl.multiple_of(b * span + r, 128), 128)
                for g in range(n_kv):
                    y = lane_take(x, g * HD)
                    k[g, at, :] = y.astype(low)
                    kt[g, :, at] = y.T.astype(low)
                    y = lane_take(x, kvw + g * HD)
                    v[g, at, :] = y.astype(low)
                    vt[g, :, at] = y.T.astype(low)

            per_tile(tiles, 128, tile)

        unpack(2)
        for i in (1, 2):

            @pl.when(d < i)
            def _():
                win[2 - i] = jnp.zeros((span, 2 * kvw), low)

            when(d >= i, lambda: ahead(i).wait_recv())
            unpack(2 - i)
        wd.start()
        wg.start()

        def attend(u, _):
            g, i = u // tiles, lax.rem(u, tiles)
            at = pl.multiple_of(i * 128, 128)
            keys = pl.ds(at, reach)
            s, seen = masked_scores(k[g, keys, :], q[g, i], at, begin_ref[:, pl.ds(at, 128)], span, group)
            s = jnp.where(seen, s, masked_score)
            top = jnp.max(s, axis=0, keepdims=True)
            e = jnp.exp(s - top)
            total = jnp.sum(e, axis=0, keepdims=True)
            p = (e * (1.0 / total)).astype(low)
            lse[g, i] = top + jnp.log(total)
            ch[g, i] = dot(vt[g, :, keys], p).T.astype(low)
            return 0

        half = max(1, n_kv * tiles // 2)
        arrive3 = ag3.arrivals()
        lax.fori_loop(0, half, attend, 0)
        cut = len(arrive3) // 2
        for x in arrive3[:cut]:
            x()
        lax.fori_loop(half, n_kv * tiles, attend, 0)
        for x in arrive3[cut:]:
            x()

        def pack(r):
            x = 0.0
            for h in range(n_q):
                at = h % group * 128
                x = x + lane_place(ch[h // group, r // 128, at : at + 128, :].astype(f32), h * HD, qw)
            ctx[pl.ds(r, 128), :] = x.astype(low)

        per_tile(tiles, 128, pack)

        def out_rows(j):
            for c in range(0, width, 512):
                part[rows_of(j), c : c + 512] = nt_dot(ctx[rows_of(j), :], wa_ref[c : c + 512, qkvw:])

        rs.relay(0, out_rows)
        in_turn(wd.forwards(), wg.forwards())
        wu.start()
        out_rows(t)

        for p in range(parts):

            def put(r, x):
                at = pl.ds(p * piece + r, 16)
                x = x + tok[at, :].astype(f32)
                res[at, :] = x
                h2[own_rows(p, r), :] = (x * inverse_rms(x) * g2[...]).astype(low)

            if p:
                rs.relay(p)
            rs.total(p, put)
            ag2.start(p)
        rs.finish()
        wd.arrived()

        def back_act(c):
            part[:, pl.ds(c, 256)] = dot(gr[...], wd_ref[:, pl.ds(c, 256)])

        arrive2 = ag2.arrivals()
        for x in arrive2[:parts]:
            x()
        per_tile(units // 256, 256, back_act)
        in_turn(arrive2[parts:], wu.forwards())
        wg.arrived()
        wu.arrived()

        def act(c):
            cols = pl.ds(c, 256)
            gate = dot(h2[...], wg_ref[:, cols])
            up = dot(h2[...], wu_ref[:, cols])
            back = part[:, cols]
            sig = jax.nn.sigmoid(gate)
            ia[:, cols] = (gate * sig * up).astype(low)
            gl[:, cols] = (back * up * (sig * (1.0 + gate * (1.0 - sig)))).astype(low)
            ul[:, cols] = (back * gate * sig).astype(low)

        per_tile(units // 256, 256, act)

        def rows_back(j):
            rows = rows_of(j)
            for c in range(0, width, 512):
                part[rows, c : c + 512] = nt_dot(gl[rows, :], wg_ref[c : c + 512, :]) + nt_dot(
                    ul[rows, :], wu_ref[c : c + 512, :]
                )

        n = rs.slots()
        last_slot = gs.chunks + 1
        grads = (
            ((gr, lambda: ia[...]),),
            ((h2, lambda: gl[...]),),
            ((h2, lambda: ul[...]),),
            ((h1, lambda: xl[...]), (rl, lambda: ctx[...])),
        )

        def beside(a, shift=0):
            every = max(1, n // last_slot)

            def go(w):
                w = w - shift
                pl.when((lax.rem(w, every) == 0) & (w < every * last_slot))(lambda: gs.slot(a, w // every, grads[a]))

            return go

        rs.relay(0, rows_back, beside(0))
        rows_back(t)
        mine[...] = jnp.zeros_like(mine)

        for p in range(parts):

            def put(r, x):
                at = pl.ds(p * piece + r, 16)
                y = res[at, :]
                inverse = inverse_rms(y)
                normed = y * inverse
                mine[:, width:] += jnp.sum(x * normed, axis=0, keepdims=True)
                e = x * g2[...]
                back = inverse * (e - normed * jnp.mean(e * normed, axis=-1, keepdims=True))
                y = og[at, :].astype(f32) + back
                rg[at, :] = y
                rl[own_rows(p, r), :] = y.astype(low)

            if p:
                rs.relay(p, None, beside(p, p * n))
            rs.total(p, put)
            ag4.start(p)
        rs.finish()

        def ffn_rows(r):
            cols = pl.ds(r, 512)
            part[:, cols] = nt_dot(ia[...], wd_ref[cols, :])

        def while_gathered(w, _):
            ag4.arrive_at(w)
            pl.when(w < width // 512)(lambda: ffn_rows(pl.multiple_of(w * 512, 512)))
            gs.slot(2, w, grads[2])
            return 0

        lax.fori_loop(0, max((nt - 1) * parts, last_slot, width // 512), while_gathered, 0)

        def context_back(r):
            x = dot(rl[pl.ds(r, 128), :], wa_ref[:, qkvw:])
            i = r // 128
            for h in range(n_q):
                g, at = h // group, pl.ds(h % group * 128, 128)
                y = lane_take(x, h * HD).astype(low)
                dc[g, i, at, :] = y
                z = y.astype(f32) * ch[g, i, at, :].astype(f32)
                delta[g, i, :, at] = jnp.sum(z.T, axis=0, keepdims=True)

        per_tile(tiles, 128, context_back)
        dk[...] = jnp.zeros_like(dk)
        dv[...] = jnp.zeros_like(dv)
        count = n_kv * tiles
        slots = n * parts
        per = -(-slots // count)

        def attend_back(u, _):
            def pump(w, _):
                pl.when(w < slots)(lambda: rs.step(w))
                return 0

            lax.fori_loop(u * per, u * per + per, pump, 0)
            g, i = u // tiles, lax.rem(u, tiles)
            at = pl.multiple_of(i * 128, 128)
            keys = pl.ds(at, reach)
            qq, dd = q[g, i], dc[g, i]
            s, seen = masked_scores(k[g, keys, :], qq, at, begin_ref[:, pl.ds(at, 128)], span, group)
            p = jnp.where(seen, jnp.exp(s - lse[g, i]), 0.0)
            ds = (p * (nt_dot(v[g, keys, :], dd) - delta[g, i])).astype(low)
            dv[g, keys, :] += dot(p.astype(low), dd)
            dk[g, keys, :] += dot(ds, qq)
            dq[g, i] = dot(kt[g, :, keys], ds).T
            return 0

        lax.fori_loop(0, count, attend_back, 0)

        def kv_rows(b, r):
            at = pl.ds(pl.multiple_of(b * span + r, 128), 128)
            x = 0.0
            for g in range(n_kv):
                x = x + lane_place(dk[g, at, :] * scale, g * HD, 2 * kvw)
                x = x + lane_place(dv[g, at, :], kvw + g * HD, 2 * kvw)
            return x

        def behind(i):
            where = {"dp": d - i}
            return (
                remote(kvs.at[i - 1], kvr.at[i - 1], bs.at[0, i - 1], br.at[0, i - 1], where),
                remote(kss.at[i - 1], ksr.at[i - 1], bs.at[1, i - 1], br.at[1, i - 1], where),
            )

        for i in (2, 1):

            @pl.when(d >= i)
            def _():
                def tile(r):
                    at = kvs.at[i - 1, pl.ds(r, 128)]
                    col_encode(kv_rows(2 - i, r), at, kss.at[i - 1, r // 128], slice(None))

                per_tile(tiles, 128, tile)
                for c in behind(i):
                    c.start()

        def query_rows(r):
            rows = pl.ds(r, 128)
            x = 0.0
            for h in range(n_q):
                at = h % group * 128
                x = x + lane_place(dq[h // group, r // 128, at : at + 128, :] * scale, h * HD, qw)
            pad = jnp.zeros((128, 2 * kvw), f32)
            xl[rows, :] = turn_rows(jnp.concatenate([x, pad], axis=1), rows, -1.0).astype(low)

        per_tile(tiles, 128, query_rows)
        for p in range(parts):

            def put(r, x):
                at = pl.ds(p * piece + r, 16)
                get(o_out)[at, :] = (res[at, :] + x).astype(low)

            rs.total(p, put)
        rs.finish()
        ready = get(h_ready)
        for ok, where in ((t > 0, t - 1), (t < nt - 1, t + 1)):
            when(ok, lambda: pl.semaphore_signal(ready, inc=1, device_id={"tp": where}, device_id_type=MESH))

        def put_down(cols, x):
            get(o_dd)[cols, :] = x.T

        gs.collect(0, put_down)
        for i in (1, 2):

            @pl.when(d + i < nd)
            def _():
                for c in behind(i):
                    c.wait_recv()

        near1, near2 = d + 1 < nd, d + 2 < nd

        def kv_total(r):
            rows = pl.ds(r, 128)
            x = kv_rows(2, r)
            a = col_decode(kvr.at[0, rows], ksr.at[0, r // 128], slice(None))
            b = col_decode(kvr.at[1, rows], ksr.at[1, r // 128], slice(None))
            x = x + jnp.where(near1, a, 0.0) + jnp.where(near2, b, 0.0)
            pad = jnp.zeros((128, qw), f32)
            x = turn_rows(jnp.concatenate([pad, x], axis=1), rows, -1.0)
            xl[rows, qw:] = x[:, qw:].astype(low)

        per_tile(tiles, 128, kv_total)

        def hidden_rows(j):
            for c in range(0, width, 512):
                part[rows_of(j), c : c + 512] = nt_dot(xl[rows_of(j), :], wa_ref[c : c + 512, :qkvw])

        pl.semaphore_wait(ready, (t > 0).astype(jnp.int32) + (t < nt - 1).astype(jnp.int32))
        rs.relay(0, hidden_rows, beside(3))
        hidden_rows(t)

        def put_gate(cols, x):
            get(o_dg)[:, cols] = x

        def put_up(cols, x):
            get(o_du)[:, cols] = x

        def put_attn(cols, x):
            get(o_da)[:, cols] = x

        for p in range(parts):

            def put(r, x):
                at = pl.ds(p * piece + r, 16)
                y = tok[at, :].astype(f32)
                inverse = inverse_rms(y)
                normed = y * inverse
                mine[:, :width] += jnp.sum(x * normed, axis=0, keepdims=True)
                e = x * g1[...]
                e = inverse * (e - normed * jnp.mean(e * normed, axis=-1, keepdims=True))
                get(o_tg)[at, :] = rg[at, :] + e

            if p:
                rs.relay(p)
            else:
                gs.collect(1, put_gate)
                gs.collect(2, put_up)
            rs.total(p, put)
        full.run(get)
        gs.collect(3, put_attn)
        for x in (ag1, ag2, ag3, ag4, rs, wa, wg, wu, wd, gs):
            x.finish()
        for i in (2, 1):
            when(d + i < nd, lambda: ahead(i).wait_send())

            @pl.when(d >= i)
            def _():
                for c in behind(i):
                    c.wait_send()

    st.body(fn)
    return st.run()


def rope_tables(position_ids, head_size):
    half_size = head_size // 2
    inverse = rope_base ** (-(jnp.arange(half_size, dtype=jnp.float32) * 2.0 / head_size))
    angles = position_ids.astype(jnp.float32)[:, None] * inverse[None, :]
    return (jnp.cos(angles), jnp.sin(angles))


def dot(a, b):
    return jnp.dot(a, b, preferred_element_type=jnp.float32)


def on_device(
    nd, nt, tokens, positions, attn_gain, w_query, w_key, w_value, w_out, ffn_gain, w_gate, w_up, w_down, out_grad
):
    span = tokens.shape[0] * nt
    width = tokens.shape[1]
    heads = (w_query.shape[1] // HD, w_key.shape[1] // HD)
    qw, kvw = w_query.shape[1], w_key.shape[1]
    w_attn = jnp.concatenate([w_query, w_key, w_value, w_out.T], axis=1)
    w_down_t = w_down.T
    cosine, sine = rope_tables(positions, HD)
    cosine = jnp.tile(cosine, (1, 2 * heads[0]))
    sine = jnp.tile(jnp.concatenate([-sine, sine], axis=1), (1, heads[0]))
    begin = (2 * span + jnp.arange(span, dtype=jnp.int32) - positions)[None]
    output, tokens_grad, gains, down_sum, gate_sum, up_sum, attn_sum = layer(
        nd, nt, tokens, attn_gain, ffn_gain, out_grad, begin, cosine, sine, w_attn, w_gate, w_up, w_down_t, heads
    )
    cuts = (qw, qw + kvw, qw + 2 * kvw)
    return (
        output,
        tokens_grad,
        gains[0, :width],
        attn_sum[:, : cuts[0]],
        attn_sum[:, cuts[0] : cuts[1]],
        attn_sum[:, cuts[1] : cuts[2]],
        attn_sum[:, cuts[2] :].T,
        gains[0, width:],
        gate_sum,
        up_sum,
        down_sum,
    )


def solution(mesh):
    return jax.shard_map(
        functools.partial(on_device, mesh.shape["dp"], mesh.shape["tp"]),
        mesh=mesh,
        in_specs=(
            P(("dp", "tp"), None),
            P("dp"),
            P(),
            P("dp", "tp"),
            P("dp", "tp"),
            P("dp", "tp"),
            P("tp", "dp"),
            P(),
            P("dp", "tp"),
            P("dp", "tp"),
            P("tp", "dp"),
            P(("dp", "tp"), None),
        ),
        out_specs=(
            P(("dp", "tp"), None),
            P(("dp", "tp"), None),
            P(),
            P("dp", "tp"),
            P("dp", "tp"),
            P("dp", "tp"),
            P("tp", "dp"),
            P(),
            P("dp", "tp"),
            P("dp", "tp"),
            P("tp", "dp"),
        ),
        check_vma=False,
    )
```

```python
import functools
import math

import jax
import jax.numpy as jnp
from jax import lax
from jax.experimental import pallas as pl
from jax.experimental.pallas import tpu as pltpu
from jax.sharding import PartitionSpec as P

HD = 96
norm_eps = 1e-05
rope_base = 100000.0
masked_score = -1e30

MESH = pl.DeviceIdType.MESH
VMEM = pltpu.VMEM
DMA = pltpu.SemaphoreType.DMA
LEVELS = 32000.0


class Stage:
    def __init__(self, name, cid, nd, nt):
        self.name, self.cid, self.nd, self.nt = name, cid, nd, nt
        self.ins, self.outs, self.scr, self.tasks, self.links = [], [], [], [], set()

    def inp(self, x, space=VMEM):
        self.ins.append((x, space))
        return ("i", len(self.ins) - 1)

    def out(self, shape, dtype, space=VMEM):
        self.outs.append((shape, dtype, space))
        return ("o", len(self.outs) - 1)

    def scratch(self, spec):
        self.scr.append(spec)
        return ("s", len(self.scr) - 1)

    def task(self, links, gen):
        self.links |= set(links)
        self.tasks.append(gen)

    def _barrier(self):
        d, t = lax.axis_index("dp"), lax.axis_index("tp")
        nd, nt = self.nd, self.nt
        sem = pltpu.get_barrier_semaphore()
        count = 0

        def greet(ok, where):
            if ok is True:
                pl.semaphore_signal(sem, inc=1, device_id=where, device_id_type=MESH)
                return 1

            @pl.when(ok)
            def _():
                pl.semaphore_signal(sem, inc=1, device_id=where, device_id_type=MESH)

            return ok.astype(jnp.int32)

        if "line" in self.links:
            count += greet(t > 0, {"tp": t - 1})
            count += greet(t < nt - 1, {"tp": t + 1})
        if "chips" in self.links:
            for i in range(1, nd // 2):
                count += greet(True, {"dp": lax.rem(d + 2 * i, nd)})
        if "twin" in self.links:
            count += greet(True, {"dp": d + 1 - 2 * lax.rem(d, 2)})
        if "near" in self.links:
            for i in (1, 2):
                count += greet(d >= i, {"dp": d - i})
                count += greet(d < nd - i, {"dp": d + i})
        if "tp" in self.links:
            for i in range(1, nt):
                count += greet(True, {"tp": lax.rem(t + i, nt)})
        if "dp" in self.links:
            for i in range(1, nd):
                count += greet(True, {"dp": lax.rem(d + i, nd)})
        pl.semaphore_wait(sem, count)

    def run(self):
        n_in, n_out = len(self.ins), len(self.outs)

        def kernel(*refs):
            def get(h):
                kind, i = h
                return refs[i + {"i": 0, "o": n_in, "s": n_in + n_out}[kind]]

            self._barrier()
            live = [g(get) for g in self.tasks]
            while live:
                still = []
                for g in live:
                    try:
                        next(g)
                        still.append(g)
                    except StopIteration:
                        pass
                live = still

        return pl.pallas_call(
            kernel,
            out_shape=[jax.ShapeDtypeStruct(s, t) for s, t, _ in self.outs],
            in_specs=[pl.BlockSpec(memory_space=sp) for _, sp in self.ins],
            out_specs=[pl.BlockSpec(memory_space=sp) for _, _, sp in self.outs],
            scratch_shapes=self.scr,
            compiler_params=pltpu.CompilerParams(
                collective_id=self.cid, has_side_effects=True, vmem_limit_bytes=67_000_000
            ),
            name=self.name,
        )(*[x for x, _ in self.ins])


def remote(src, dst, send, recv, where):
    return pltpu.make_async_remote_copy(
        src_ref=src, dst_ref=dst, send_sem=send, recv_sem=recv, device_id=where, device_id_type=MESH
    )


def when(ok, fn):
    if ok is True:
        fn()
    elif ok is not False:
        pl.when(ok)(fn)


def over_cols(width, fn):
    def body(c, _):
        fn(pl.ds(pl.multiple_of(c * 128, 128), 128))
        return 0

    lax.fori_loop(0, width // 128, body, 0)
    if width % 128:
        fn(pl.ds(width // 128 * 128, width % 128))


def row_encode(read, code, scale, rows):
    step = 16

    def body(i, held):
        r = pl.multiple_of(i * step, step)
        x = read(r, step)
        top = jnp.max(jnp.abs(x), axis=-1, keepdims=True)
        code[pl.ds(r, step), :] = jnp.round(x * (LEVELS / jnp.maximum(top, 1e-30))).astype(jnp.int32).astype(jnp.int16)
        lane = lax.broadcasted_iota(jnp.int32, (step, 128), 1)
        row = lax.broadcasted_iota(jnp.int32, (step, 128), 0) + r
        mine = jnp.sum(jnp.where(lane == row, jnp.maximum(top, 1e-30) * (1.0 / LEVELS), 0.0), axis=0, keepdims=True)
        return held + jnp.broadcast_to(mine, (8, 128))

    scale[...] = lax.fori_loop(0, rows // step, body, jnp.zeros((8, 128), jnp.float32))


def row_decode(code, scale, r, step):
    lane = lax.broadcasted_iota(jnp.int32, (step, 128), 1)
    row = lax.broadcasted_iota(jnp.int32, (step, 128), 0) + r
    col = jnp.sum(jnp.where(lane == row, jnp.broadcast_to(scale[0:1, :], (step, 128)), 0.0), axis=-1, keepdims=True)
    return code[pl.ds(r, step), :].astype(jnp.int32).astype(jnp.float32) * col


def col_encode(x, code, scale, cols):
    top = jnp.maximum(jnp.max(jnp.abs(x), axis=0, keepdims=True), 1e-30)
    code[:, cols] = jnp.round(x * (LEVELS / top)).astype(jnp.int32).astype(jnp.int16)
    scale[:, cols] = top * (1.0 / LEVELS)


def col_decode(code, scale, cols):
    return code[:, cols].astype(jnp.int32).astype(jnp.float32) * scale[:, cols]


class LineGather:
    def __init__(self, st, full, rows, parts):
        self.st, self.full, self.rows, self.parts = st, full, rows, parts
        self.hs = st.scratch(DMA((2, st.nt, parts)))
        self.hr = st.scratch(DMA((2, st.nt, parts)))
        st.links.add("line")

    def bind(self, get):
        self.ref, self.ss, self.rs = get(self.full), get(self.hs), get(self.hr)
        self.t = lax.axis_index("tp")
        return self

    def piece(self, owner, p):
        chunk = self.rows // self.parts
        return self.ref.at[pl.ds(pl.multiple_of(owner * self.rows + p * chunk, chunk), chunk)]

    def hop(self, owner, k, s, p, where):
        at = self.piece(owner, p)
        return remote(at, at, self.ss.at[k, s, p], self.rs.at[k, s, p], {"tp": where})

    def _send(self, s, p, k, way):
        nt, t = self.st.nt, self.t
        owner, where = t - s * way, t + way
        ok = (owner >= 0) & (owner < nt) & (where >= 0) & (where < nt)
        when(ok, lambda: self.hop(owner, k, s, p, where).start())

    def start(self, p):
        for k, way in enumerate((1, -1)):
            self._send(0, p, k, way)

    def arrive(self, s, p):
        nt, t = self.st.nt, self.t
        for k, way in enumerate((1, -1)):
            owner = t - way * (s + 1)
            ok = (owner >= 0) & (owner < nt)
            when(ok, lambda: self.hop(owner, k, s, p, t).wait_recv())
            if s < nt - 2:
                self._send(s + 1, p, k, way)

    def arrive_at(self, v):
        nt, t = self.st.nt, self.t
        s, p = v // self.parts, lax.rem(v, self.parts)
        for k, way in enumerate((1, -1)):
            owner = t - way * (s + 1)
            ok = (owner >= 0) & (owner < nt) & (s < nt - 1)
            where = t + way

            @pl.when(ok)
            def _():
                self.hop(owner, k, s, p, t).wait_recv()
                when((where >= 0) & (where < nt) & (s < nt - 2), lambda: self.hop(owner, k, s + 1, p, where).start())

    def arrivals(self):
        return [
            functools.partial(self.arrive, s, p) for s in range(self.st.nt - 1) for p in range(self.parts)
        ]

    def finish(self):
        nt, t = self.st.nt, self.t
        for s in range(nt - 1):
            for p in range(self.parts):
                for k, way in enumerate((1, -1)):
                    owner, where = t - s * way, t + way
                    ok = (owner >= 0) & (owner < nt) & (where >= 0) & (where < nt)
                    when(ok, lambda: self.hop(owner, k, s, p, where).wait_send())


class LineSum:
    def __init__(self, st, part, rows, width, parts):
        self.st, self.part, self.rows, self.width, self.parts = st, part, rows, width, parts
        nt = st.nt
        self.chunk = rows // parts
        shape = (nt, parts, self.chunk, width)
        self.hc = [st.scratch(VMEM(shape, jnp.int16)) for _ in range(2)]
        self.hk = [st.scratch(VMEM(shape[:2] + (8, 128), jnp.float32)) for _ in range(2)]
        self.hd = [st.scratch(DMA((2, nt, parts))) for _ in range(2)]
        st.links.add("tp")

    def bind(self, get):
        self.x = get(self.part)
        (self.cs, self.cr), (self.sc, self.sr), (self.ss, self.rs) = (
            [get(h) for h in hs] for hs in (self.hc, self.hk, self.hd)
        )
        self.t = lax.axis_index("tp")
        return self

    def far(self, i, j):
        return (jnp.abs(i - j) == 3) if self.st.nt == 4 else (i != i)

    def sends(self, j, p):
        t = self.t
        where = jnp.where(self.far(t, j), jnp.where(j > t, t + 1, t - 1), j)
        slot = jnp.where(self.far(t, j), where, t)
        return (
            remote(self.cs.at[j, p], self.cr.at[slot, p], self.ss.at[0, j, p], self.rs.at[0, slot, p], {"tp": where}),
            remote(self.sc.at[j, p], self.sr.at[slot, p], self.ss.at[1, j, p], self.rs.at[1, slot, p], {"tp": where}),
        )

    def arrival(self, slot, p):
        for k, (x, y) in enumerate(((self.cs, self.cr), (self.sc, self.sr))):
            remote(x.at[slot, p], y.at[slot, p], self.ss.at[k, slot, p], self.rs.at[k, slot, p], {"tp": self.t}).wait_recv()

    def dest(self, o):
        nt, t = self.st.nt, self.t
        if nt != 4:
            return lax.rem(t + 1 + o, nt)
        inner = jnp.where(o == 2, 2, 1 + 2 * o)
        x = jnp.where((t == 0) | (t == nt - 1), 3 - o, inner)
        lo = lax.rem(lax.rem(t, 2) + lax.rem(x, 2), 2)
        return 2 * lax.rem(t // 2 + x // 2, 2) + lo

    def _rows(self, base, r, n):
        return self.x[pl.ds(pl.multiple_of(base + r, n), n), :]

    def send(self, p, produce=None, beside=None):
        nt, t, chunk = self.st.nt, self.t, self.chunk

        def one(o, _):
            j = self.dest(o)
            if produce is not None:
                produce(j)
            base = j * self.rows + p * chunk
            if nt == 4:
                relay = ((t == 1) & (j == 3)) | ((t == 2) & (j == 0))

                @pl.when(relay)
                def _():
                    self.arrival(t, p)
                    row_encode(
                        lambda r, n: self._rows(base, r, n) + row_decode(self.cr.at[t, p], self.sr.at[t, p], r, n),
                        self.cs.at[j, p],
                        self.sc.at[j, p],
                        chunk,
                    )

                plain = jnp.logical_not(relay)
            else:
                plain = True
            when(plain, lambda: row_encode(lambda r, n: self._rows(base, r, n), self.cs.at[j, p], self.sc.at[j, p], chunk))
            for c in self.sends(j, p):
                c.start()
            if beside is not None:
                beside(o)
            return 0

        lax.fori_loop(0, nt - 1, one, 0)

    def total(self, p, put):
        nt, t, chunk = self.st.nt, self.t, self.chunk
        sources = [lax.rem(t + 1 + i, nt) for i in range(nt - 1)]
        for i in sources:
            pl.when(jnp.logical_not(self.far(i, t)))(lambda: self.arrival(i, p))
        base = t * self.rows + p * chunk

        def body(n, _):
            r = pl.multiple_of(n * 16, 16)
            x = self._rows(base, r, 16)
            for i in sources:
                y = row_decode(self.cr.at[i, p], self.sr.at[i, p], r, 16)
                x = x + (jnp.where(self.far(i, t), 0.0, y) if nt == 4 else y)
            put(r, x)
            return 0

        lax.fori_loop(0, chunk // 16, body, 0)

    def finish(self):
        def one(o, _):
            for p in range(self.parts):
                for c in self.sends(self.dest(o), p):
                    c.wait_send()
            return 0

        lax.fori_loop(0, self.st.nt - 1, one, 0)


class ChipGather:
    def __init__(self, st, w, full, rows):
        self.st, self.w, self.full, self.rows = st, w, full, rows
        self.square = st.nd == 8
        self.hops = 4 if self.square else st.nd // 2 - 1
        self.hs, self.hr = (st.scratch(DMA((2 * self.hops + 1,))) for _ in range(2))
        self.hl = st.scratch(DMA((1,)))
        st.links |= {"chips", "twin"}

    def bind(self, get):
        self.x, self.o, self.ss, self.rs, ls = (get(h) for h in (self.w, self.full, self.hs, self.hr, self.hl))
        nd, rows, n = self.st.nd, self.rows, self.hops
        d = lax.axis_index("dp")
        core, chip = lax.rem(d, 2), d // 2
        twin = {"dp": d + 1 - 2 * core}

        def at(i, part=None):
            if part is None:
                return self.o.at[pl.ds(pl.multiple_of(i * rows, rows), rows)]
            return self.o.at[pl.ds(pl.multiple_of(i * rows + part * (rows // 2), rows // 2), rows // 2)]

        beside = [chip + 1 - 2 * lax.rem(chip, 2), lax.rem(chip + 2, 4)]
        near = [2 * c + core for c in beside]
        diagonal = 2 * lax.rem(beside[0] + 2, 4) + core

        def came(i):
            if not self.square:
                return at(lax.rem(d - 2 * i - 2 + nd, nd))
            return at(near[i]) if i < 2 else at(diagonal, i - 2)

        def hop(i):
            if not self.square:
                src, dst, where = self.x, at(d), lax.rem(d + 2 * i + 2, nd)
            elif i < 2:
                src, dst, where = self.x, at(d), near[i]
            else:
                src = dst = at(near[i - 2], i - 2)
                where = near[3 - i]
            return remote(src, dst, self.ss.at[i], self.rs.at[i], {"dp": where})

        def landed(i):
            return remote(came(i), came(i), self.ss.at[i], self.rs.at[i], twin)

        def give(i):
            src, dst = (self.x, at(d)) if i == 0 else (came(i - 1), came(i - 1))
            return remote(src, dst, self.ss.at[n + i], self.rs.at[n + i], twin)

        self.own = lambda: pltpu.make_async_copy(self.x, at(d), ls.at[0])
        self.hop, self.landed, self.give = hop, landed, give
        return self

    def start(self):
        for i in range(2 if self.square else self.hops):
            self.hop(i).start()
        self.give(0).start()
        self.own().start()

    def forward(self, i):
        self.landed(i).wait_recv()
        if self.square and i < 2:
            self.hop(i + 2).start()
        self.give(i + 1).start()

    def forwards(self):
        return [functools.partial(self.forward, i) for i in range(self.hops)]

    def arrived(self):
        for i in range(self.hops + 1):
            self.give(i).wait_recv()
        self.own().wait()

    def finish(self):
        for i in range(self.hops + 1):
            self.give(i).wait_send()
        for i in range(self.hops):
            self.hop(i).wait_send()


class GradScatter:
    def __init__(self, st, shard, widths, sums):
        nc = self.nc = st.nd // 2
        self.st, self.shard, self.widths = st, shard, widths
        self.m = math.lcm(2 * shard, 128) // (2 * shard)
        self.chunks = nc // self.m
        wide = max(widths)
        self.hg = st.scratch(VMEM((2, 2 * self.m * shard, wide), jnp.float32))
        self.ht = st.scratch(VMEM((2, self.m, shard, wide), jnp.float32))
        self.slots = self.chunks - (self.m == 1)
        self.hs = st.scratch(VMEM((self.slots, self.m, shard, wide), jnp.int16))
        self.hk = st.scratch(VMEM((self.slots, self.m, 1, wide), jnp.float32))
        self.hcr = [st.scratch(VMEM((nc - 1, shard, w), jnp.int16)) for w in widths]
        self.hkr = [st.scratch(VMEM((nc - 1, 1, w), jnp.float32)) for w in widths]
        self.ha = sums
        self.hgs = [st.scratch(DMA((2, self.m))) for _ in range(2)]
        self.hss = st.scratch(DMA((2, self.slots, self.m)))
        self.hsr = st.scratch(DMA((len(widths), 2, nc - 1)))
        self.hf = st.scratch(pltpu.SemaphoreType.REGULAR)
        st.links |= {"chips", "twin"}

    def bind(self, get):
        self.g, self.t, self.cs, self.sc, self.ss, self.sr, self.free = (
            get(h) for h in (self.hg, self.ht, self.hs, self.hk, self.hss, self.hsr, self.hf)
        )
        self.cr, self.kr, self.acc = ([get(h) for h in hs] for hs in (self.hcr, self.hkr, self.ha))
        self.gs, self.gr = (get(h) for h in self.hgs)
        d = self.d = lax.axis_index("dp")
        self.core, self.chip = lax.rem(d, 2), d // 2
        self.twin = {"dp": d + 1 - 2 * self.core}
        return self

    def chunk(self, i):
        return lax.rem(self.chip // self.m + 1 + i, self.chunks)

    def half(self, e, core):
        return pl.ds(pl.multiple_of((2 * e + core) * self.shard, self.shard), self.shard)

    def gift(self, a, r, e):
        cols = pl.ds(0, self.widths[a])
        return remote(
            self.g.at[r, self.half(e, 1 - self.core), cols], self.t.at[r, e, :, cols], self.gs.at[r, e], self.gr.at[r, e],
            self.twin,
        )

    def sums(self, a, i, e, dest):
        cols, nc = pl.ds(0, self.widths[a]), self.nc
        slot = jnp.maximum(lax.rem(dest - self.chip + nc, nc) - 1, 0)
        where = {"dp": 2 * dest + self.core}
        return (
            remote(self.cs.at[i, e, :, cols], self.cr[a].at[slot], self.ss.at[0, i, e], self.sr.at[a, 0, slot], where),
            remote(self.sc.at[i, e, :, cols], self.kr[a].at[slot], self.ss.at[1, i, e], self.sr.at[a, 1, slot], where),
        )

    def compute(self, a, i, pieces):
        n = a * self.chunks + i
        r = lax.rem(n, 2)
        rows = 2 * self.m * self.shard

        @pl.when(n >= 2)
        def _():
            for e in range(self.m):
                self.gift(a, r, e).wait_send() if a == 0 else self._sent(a, i, r, e)
            pl.semaphore_wait(self.free, 1)

        cols = pl.ds(pl.multiple_of(self.chunk(i) * rows, 128), rows)
        at = 0
        for x, y in pieces:
            z = y()
            self.g[r, :, at : at + z.shape[1]] = tn_dot(x[:, cols], z)
            at += z.shape[1]
        for e in range(self.m):
            self.gift(a, r, e).start()

    def _sent(self, a, i, r, e):
        pl.when(i >= 2)(lambda: self.gift(a, r, e).wait_send())
        pl.when(i < 2)(lambda: self.gift(a - 1, r, e).wait_send())

    def combine(self, a, i):
        n = a * self.chunks + i
        r = lax.rem(n, 2)
        for e in range(self.m):
            self.gift(a, r, e).wait_recv()
            dest = self.chunk(i) * self.m + e
            away = dest != self.chip
            own = self.half(e, self.core)

            @pl.when(away)
            def _():
                if a:
                    for c in self.sums(a - 1, i, e, dest):
                        c.wait_send()
                over_cols(
                    self.widths[a],
                    lambda cols: col_encode(
                        self.g[r, own, cols] + self.t[r, e, :, cols], self.cs.at[i, e], self.sc.at[i, e], cols
                    ),
                )
                for c in self.sums(a, i, e, dest):
                    c.start()

            @pl.when(jnp.logical_not(away))
            def _():
                over_cols(self.widths[a], lambda cols: self._keep(a, r, e, own, cols))

        @pl.when(n + 2 < len(self.widths) * self.chunks)
        def _():
            pl.semaphore_signal(self.free, inc=1, device_id=self.twin, device_id_type=MESH)

    def _keep(self, a, r, e, own, cols):
        self.acc[a][:, cols] = self.g[r, own, cols] + self.t[r, e, :, cols]

    def slot(self, a, w, pieces):
        pl.when(w < self.chunks)(lambda: self.compute(a, w, pieces))
        pl.when((w >= 1) & (w <= self.chunks))(lambda: self.combine(a, w - 1))

    def collect(self, a, put):
        n = self.nc - 1
        for i in range(n):
            for c in self.sums(a, 0, 0, lax.rem(self.chip + 1 + i, self.nc)):
                c.wait_recv()

        def tile(cols):
            x = self.acc[a][:, cols]
            for i in range(n):
                x = x + col_decode(self.cr[a].at[i], self.kr[a].at[i], cols)
            put(cols, x)

        over_cols(self.widths[a], tile)

    def finish(self):
        a = len(self.widths) - 1
        for i in range(self.chunks):
            for e in range(self.m):
                if i >= self.chunks - 2:
                    self.gift(a, (a * self.chunks + i) % 2, e).wait_send()
                if i < self.slots:
                    dest = self.chunk(i) * self.m + e

                    @pl.when(dest != self.chip)
                    def _():
                        for c in self.sums(a, i, e, dest):
                            c.wait_send()


class FullSum:
    def __init__(self, st, x, out, shape):
        self.st, self.x, self.out = st, x, out
        self.ha = st.scratch(VMEM((st.nt,) + shape, jnp.float32))
        self.hm = st.scratch(VMEM(shape, jnp.float32))
        self.hb = st.scratch(VMEM((st.nd,) + shape, jnp.float32))
        self.hs = st.scratch(DMA((2, max(st.nd, st.nt))))
        self.hr = st.scratch(DMA((2, max(st.nd, st.nt))))
        st.links |= {"tp", "dp"}

    def run(self, get):
        nd, nt = self.st.nd, self.st.nt
        x, o, a, m, b, ss, rs = (get(h) for h in (self.x, self.out, self.ha, self.hm, self.hb, self.hs, self.hr))
        for k, (axis, n, src, got, dst) in enumerate((("tp", nt, x, a, m), ("dp", nd, m, b, o))):
            me = lax.axis_index(axis)
            cs = [
                remote(src, got.at[me], ss.at[k, i], rs.at[k, i], {axis: lax.rem(me + i, n)}) for i in range(1, n)
            ]
            for c in cs:
                c.start()
            got[me] = src[...]
            for c in cs:
                c.wait()
            total = got[0]
            for i in range(1, n):
                total = total + got[i]
            dst[...] = total


def lane_take(x, offset):
    base = offset // 128 * 128
    wide = min(256, x.shape[-1] - base)
    slab = x[:, base : base + wide]
    if wide % 128:
        slab = jnp.concatenate([slab, jnp.zeros((x.shape[0], -wide % 128), x.dtype)], axis=1)
        wide = slab.shape[-1]
    if offset > base:
        slab = pltpu.roll(slab, wide - (offset - base), 1)
    slab = slab[:, :128]
    return jnp.where(lax.broadcasted_iota(jnp.int32, slab.shape, 1) < HD, slab, 0.0)


def lane_place(x, offset, width):
    base = offset // 128 * 128
    wide = min(256, width - base)
    slab = x if wide == 128 else jnp.concatenate([x, jnp.zeros_like(x)], axis=1)
    if offset > base:
        slab = pltpu.roll(slab, offset - base, 1)
    slab = slab[:, :wide]
    pieces = []
    if base:
        pieces.append(jnp.zeros((x.shape[0], base), x.dtype))
    pieces.append(slab)
    if base + wide < width:
        pieces.append(jnp.zeros((x.shape[0], width - base - wide), x.dtype))
    return jnp.concatenate(pieces, axis=1) if len(pieces) > 1 else slab


def turned(u, cosine, sine):
    wide = u.shape[-1]
    lane = lax.rem(lax.broadcasted_iota(jnp.int32, u.shape, 1), HD)
    swap = jnp.where(lane < HD // 2, pltpu.roll(u, wide - HD // 2, 1), pltpu.roll(u, HD // 2, 1))
    return u * cosine + swap * sine


def nt_dot(a, b):
    return lax.dot_general(a, b, (((1,), (1,)), ((), ())), preferred_element_type=jnp.float32)


def per_tile(count, size, fn):
    def body(i, _):
        fn(pl.multiple_of(i * size, size))
        return 0

    lax.fori_loop(0, count, body, 0)


def in_turn(*lists):
    for i in range(max(len(x) for x in lists)):
        for x in lists:
            if i < len(x):
                x[i]()


class Fused(Stage):
    def body(self, fn):
        self.tasks = [lambda get: iter(fn(get) or ())]


def inverse_rms(x):
    return lax.rsqrt(jnp.mean(x * x, axis=-1, keepdims=True) + norm_eps)


def tn_dot(a, b):
    return lax.dot_general(a, b, (((0,), (0,)), ((), ())), preferred_element_type=jnp.float32)


def across(x, count):
    return jnp.concatenate([x] * count, axis=1) if count > 1 else x


def masked_scores(keys, queries, first, begin, span, group):
    s = nt_dot(keys, queries) * (1.0 / math.sqrt(HD))
    key = lax.broadcasted_iota(jnp.int32, s.shape, 0) + first
    own = lax.rem(lax.broadcasted_iota(jnp.int32, s.shape, 1), 128) + (first + 2 * span)
    return s, (key >= across(begin, group)) & (key <= own)


def layer(
    nd, nt, tokens, attn_gain, ffn_gain, out_grad, begin, cosine, sine, w_attn, w_gate, w_up, w_down_t, heads
):
    st = Fused("layer", 1, nd, nt)
    low, f32 = jnp.bfloat16, jnp.float32
    own, width = tokens.shape
    span = own * nt
    shard, units = w_gate.shape
    n_q, n_kv = heads
    group = n_q // n_kv
    tiles = span // 128
    qw, kvw = n_q * HD, n_kv * HD
    qkvw = qw + 2 * kvw
    reach = 2 * span + 128
    parts = 2
    piece = own // parts
    scale = 1.0 / math.sqrt(HD)

    h_tok, h_g1, h_g2 = st.inp(tokens), st.inp(attn_gain[None]), st.inp(ffn_gain[None])
    h_og, h_begin = st.inp(out_grad), st.inp(begin)
    h_cos, h_sin = st.inp(cosine), st.inp(sine)
    s_wa, s_wg, s_wu, s_wd = (st.inp(w, pl.ANY) for w in (w_attn, w_gate, w_up, w_down_t))

    o_out = st.out((own, width), low)
    o_tg = st.out((own, width), f32)
    o_gains = st.out((1, 2 * width), f32)
    o_dd = st.out((units, shard), f32)
    o_dg, o_du = (st.out((shard, units), f32) for _ in range(2))
    o_da = st.out((shard, qkvw + qw), f32)

    def room(shape, dtype=f32):
        return st.scratch(VMEM(shape, dtype))

    h_h1, h_h2, h_gr, h_rl = (room((span, width), low) for _ in range(4))
    h_wa = room((width, qkvw + qw), low)
    h_wg, h_wu, h_wd = (room((width, units), low) for _ in range(3))
    h_q, h_dc, h_ch = (room((n_kv, tiles, group * 128, 128), low) for _ in range(3))
    h_k, h_v = (room((n_kv, 3 * span, 128), low) for _ in range(2))
    h_vt = room((n_kv, 128, 3 * span), low)
    h_win = room((3, span, 2 * kvw), low)
    h_ctx = room((span, qw), low)
    h_lse, h_delta = (room((n_kv, tiles, 1, group * 128)) for _ in range(2))
    h_res, h_rg = (room((own, width)) for _ in range(2))
    h_part = room((span, width))
    h_ia, h_gl, h_ul = (room((span, units), low) for _ in range(3))
    h_dq = room((n_kv, tiles, group * 128, 128))
    h_dk, h_dv = (room((n_kv, 3 * span, 128)) for _ in range(2))
    h_kvs, h_kvr = (room((2, span, 2 * kvw), jnp.int16) for _ in range(2))
    h_kss, h_ksr = (room((2, tiles, 1, 2 * kvw)) for _ in range(2))
    h_mine = room((1, 2 * width))
    h_fs, h_fr = (st.scratch(DMA((2,))) for _ in range(2))
    h_bs, h_br = (st.scratch(DMA((2, 2))) for _ in range(2))
    h_ready = st.scratch(pltpu.SemaphoreType.REGULAR)

    ag1 = LineGather(st, h_h1, own, parts)
    ag2 = LineGather(st, h_h2, own, parts)
    ag3 = LineGather(st, h_gr, own, parts)
    ag4 = LineGather(st, h_rl, own, parts)
    rs = LineSum(st, h_part, own, width, parts)
    wa = ChipGather(st, s_wa, h_wa, shard)
    wg = ChipGather(st, s_wg, h_wg, shard)
    wu = ChipGather(st, s_wu, h_wu, shard)
    wd = ChipGather(st, s_wd, h_wd, shard)
    gs = GradScatter(st, shard, (units, units, units, qkvw + qw), (room((shard, units)), o_dg, o_du, o_da))
    full = FullSum(st, h_mine, o_gains, (1, 2 * width))
    st.links.add("near")

    def fn(get):
        d, t = lax.axis_index("dp"), lax.axis_index("tp")
        for x in (ag1, ag2, ag3, ag4, rs, wa, wg, wu, wd, gs):
            x.bind(get)
        tok, g1, g2, og, begin_ref, cos_ref, sin_ref = (get(h) for h in (h_tok, h_g1, h_g2, h_og, h_begin, h_cos, h_sin))
        h1, h2, gr, rl = (get(h) for h in (h_h1, h_h2, h_gr, h_rl))
        wa_ref, wg_ref, wu_ref, wd_ref = (get(h) for h in (h_wa, h_wg, h_wu, h_wd))
        q, k, v, vt, win, ctx, ch, lse = (get(h) for h in (h_q, h_k, h_v, h_vt, h_win, h_ctx, h_ch, h_lse))
        dc, delta, dq, dk, dv = (get(h) for h in (h_dc, h_delta, h_dq, h_dk, h_dv))
        res, rg, part, ia, gl, ul, mine = (get(h) for h in (h_res, h_rg, h_part, h_ia, h_gl, h_ul, h_mine))
        xl = ul.at[:, pl.ds(0, qkvw)]
        kvs, kvr, kss, ksr, fs, fr, bs, br = (
            get(h) for h in (h_kvs, h_kvr, h_kss, h_ksr, h_fs, h_fr, h_bs, h_br)
        )

        def own_rows(p, r, n=16):
            return pl.ds(pl.multiple_of(t * own + p * piece + r, n), n)

        def rows_of(j):
            return pl.ds(pl.multiple_of(j * own, own), own)

        wa.start()
        for p in range(parts):

            def tile(r):
                x = tok[pl.ds(p * piece + r, 16), :].astype(f32)
                h1[own_rows(p, r), :] = (x * inverse_rms(x) * g1[...]).astype(low)

            per_tile(piece // 16, 16, tile)
            ag1.start(p)
        gr[rows_of(t), :] = og[...]
        in_turn(ag1.arrivals(), wa.forwards() + [wd.start])
        for p in range(parts):
            ag3.start(p)
        wa.arrived()

        def turn_rows(x, rows, way):
            cosine, sine = across(cos_ref[rows, :], 2), across(sin_ref[rows, :], 2)
            lane = lax.broadcasted_iota(jnp.int32, x.shape, 1)
            return jnp.where(lane < qw + kvw, turned(x, cosine, way * sine), x)

        def project(r):
            rows = pl.ds(r, 128)
            x = turn_rows(dot(h1[rows, :], wa_ref[:, :qkvw]), rows, 1.0)
            for h in range(n_q):
                q[h // group, r // 128, h % group * 128 : (h % group + 1) * 128, :] = lane_take(x, h * HD).astype(low)
            win[2, rows, :] = x[:, qw:].astype(low)

        per_tile(tiles, 128, project)

        def ahead(i):
            return remote(win.at[2], win.at[2 - i], fs.at[i - 1], fr.at[i - 1], {"dp": d + i})

        for i in (2, 1):
            when(d + i < nd, lambda: ahead(i).start())

        def unpack(b):
            def tile(r):
                x = win[b, pl.ds(r, 128), :].astype(f32)
                at = pl.ds(pl.multiple_of(b * span + r, 128), 128)
                for g in range(n_kv):
                    k[g, at, :] = lane_take(x, g * HD).astype(low)
                    y = lane_take(x, kvw + g * HD)
                    v[g, at, :] = y.astype(low)
                    vt[g, :, at] = y.T.astype(low)

            per_tile(tiles, 128, tile)

        unpack(2)
        pass_d, pass_g, pass_u = wd.forwards(), wg.forwards(), wu.forwards()
        for x in pass_d[:2]:
            x()
        for i in (1, 2):

            @pl.when(d < i)
            def _():
                win[2 - i] = jnp.zeros((span, 2 * kvw), low)

            when(d >= i, lambda: ahead(i).wait_recv())
            unpack(2 - i)
        wg.start()
        wu.start()
        for x in pass_d[2:]:
            x()

        def attend(u, _):
            g, i = u // tiles, lax.rem(u, tiles)
            at = pl.multiple_of(i * 128, 128)
            keys = pl.ds(at, reach)
            s, seen = masked_scores(k[g, keys, :], q[g, i], at, begin_ref[:, pl.ds(at, 128)], span, group)
            s = jnp.where(seen, s, masked_score)
            top = jnp.max(s, axis=0, keepdims=True)
            e = jnp.exp(s - top)
            total = jnp.sum(e, axis=0, keepdims=True)
            p = (e * (1.0 / total)).astype(low)
            lse[g, i] = top + jnp.log(total)
            ch[g, i] = dot(vt[g, :, keys], p).T.astype(low)
            return 0

        half = max(1, n_kv * tiles // 2)
        arrive3 = ag3.arrivals()
        lax.fori_loop(0, half, attend, 0)
        cut = len(arrive3) // 2
        in_turn(arrive3[:cut], pass_g[:2])
        lax.fori_loop(half, n_kv * tiles, attend, 0)
        in_turn(arrive3[cut:], pass_u[:2])

        def pack(r):
            x = 0.0
            for h in range(n_q):
                at = h % group * 128
                x = x + lane_place(ch[h // group, r // 128, at : at + 128, :].astype(f32), h * HD, qw)
            ctx[pl.ds(r, 128), :] = x.astype(low)

        per_tile(tiles, 128, pack)

        def out_rows(j):
            for c in range(0, width, 512):
                part[rows_of(j), c : c + 512] = nt_dot(ctx[rows_of(j), :], wa_ref[c : c + 512, qkvw:])

        rs.send(0, out_rows)
        rs.send(1)
        out_rows(t)
        kt = vt

        def keys_back(r):
            for g in range(n_kv):
                kt[g, :, pl.ds(r, 128)] = k[g, pl.ds(r, 128), :].T

        per_tile(3 * tiles, 128, keys_back)
        in_turn(pass_g[2:], pass_u[2:])

        for p in range(parts):

            def put(r, x):
                at = pl.ds(p * piece + r, 16)
                x = x + tok[at, :].astype(f32)
                res[at, :] = x
                h2[own_rows(p, r), :] = (x * inverse_rms(x) * g2[...]).astype(low)

            rs.total(p, put)
            ag2.start(p)
        wd.arrived()

        def back_act(c):
            part[:, pl.ds(c, 256)] = dot(gr[...], wd_ref[:, pl.ds(c, 256)])

        arrive2 = ag2.arrivals()
        for x in arrive2[:parts]:
            x()
        per_tile(units // 256, 256, back_act)
        for x in arrive2[parts:]:
            x()
        wg.arrived()
        wu.arrived()

        def act(c):
            cols = pl.ds(c, 256)
            gate = dot(h2[...], wg_ref[:, cols])
            up = dot(h2[...], wu_ref[:, cols])
            back = part[:, cols]
            sig = jax.nn.sigmoid(gate)
            ia[:, cols] = (gate * sig * up).astype(low)
            gl[:, cols] = (back * up * (sig * (1.0 + gate * (1.0 - sig)))).astype(low)
            ul[:, cols] = (back * gate * sig).astype(low)

        per_tile(units // 256, 256, act)

        def rows_back(j):
            rows = rows_of(j)
            for c in range(0, width, 512):
                part[rows, c : c + 512] = nt_dot(gl[rows, :], wg_ref[c : c + 512, :]) + nt_dot(
                    ul[rows, :], wu_ref[c : c + 512, :]
                )

        last_slot = gs.chunks + 1
        grads = (
            ((gr, lambda: ia[...]),),
            ((h2, lambda: gl[...]),),
            ((h2, lambda: ul[...]),),
            ((h1, lambda: xl[...]), (rl, lambda: ctx[...])),
        )

        def weight_grads(a, first=0):
            def one(w, _):
                gs.slot(a, w, grads[a])
                return 0

            lax.fori_loop(first, last_slot, one, 0)

        rs.finish()
        rs.send(0, rows_back, lambda o: gs.slot(0, o, grads[0]))
        rs.send(1)
        rows_back(t)
        weight_grads(0, nt - 1)
        mine[...] = jnp.zeros_like(mine)

        for p in range(parts):

            def put(r, x):
                at = pl.ds(p * piece + r, 16)
                y = res[at, :]
                inverse = inverse_rms(y)
                normed = y * inverse
                mine[:, width:] += jnp.sum(x * normed, axis=0, keepdims=True)
                e = x * g2[...]
                back = inverse * (e - normed * jnp.mean(e * normed, axis=-1, keepdims=True))
                y = og[at, :].astype(f32) + back
                rg[at, :] = y
                rl[own_rows(p, r), :] = y.astype(low)

            rs.total(p, put)
            ag4.start(p)

        def ffn_rows(r):
            cols = pl.ds(r, 512)
            part[:, cols] = nt_dot(ia[...], wd_ref[cols, :])

        def while_gathered(w, _):
            ag4.arrive_at(w)
            pl.when(w < width // 512)(lambda: ffn_rows(pl.multiple_of(w * 512, 512)))
            gs.slot(1, w, grads[1])
            return 0

        lax.fori_loop(0, max((nt - 1) * parts, last_slot, width // 512), while_gathered, 0)

        def context_back(r):
            x = dot(rl[pl.ds(r, 128), :], wa_ref[:, qkvw:])
            i = r // 128
            for h in range(n_q):
                g, at = h // group, pl.ds(h % group * 128, 128)
                y = lane_take(x, h * HD).astype(low)
                dc[g, i, at, :] = y
                z = y.astype(f32) * ch[g, i, at, :].astype(f32)
                delta[g, i, :, at] = jnp.sum(z.T, axis=0, keepdims=True)

        rs.finish()
        for p in range(parts):
            rs.send(p)
        per_tile(tiles, 128, context_back)
        dk[...] = jnp.zeros_like(dk)
        dv[...] = jnp.zeros_like(dv)
        count = n_kv * tiles

        def attend_back(u, _):
            g, i = u // tiles, lax.rem(u, tiles)
            at = pl.multiple_of(i * 128, 128)
            keys = pl.ds(at, reach)
            qq, dd = q[g, i], dc[g, i]
            s, seen = masked_scores(k[g, keys, :], qq, at, begin_ref[:, pl.ds(at, 128)], span, group)
            p = jnp.where(seen, jnp.exp(s - lse[g, i]), 0.0)
            ds = (p * (nt_dot(v[g, keys, :], dd) - delta[g, i])).astype(low)
            dv[g, keys, :] += dot(p.astype(low), dd)
            dk[g, keys, :] += dot(ds, qq)
            dq[g, i] = dot(kt[g, :, keys], ds).T
            gs.slot(2, u, grads[2])
            return 0

        lax.fori_loop(0, count, attend_back, 0)
        weight_grads(2, count)

        def kv_rows(b, r):
            at = pl.ds(pl.multiple_of(b * span + r, 128), 128)
            x = 0.0
            for g in range(n_kv):
                x = x + lane_place(dk[g, at, :] * scale, g * HD, 2 * kvw)
                x = x + lane_place(dv[g, at, :], kvw + g * HD, 2 * kvw)
            return x

        def behind(i):
            where = {"dp": d - i}
            return (
                remote(kvs.at[i - 1], kvr.at[i - 1], bs.at[0, i - 1], br.at[0, i - 1], where),
                remote(kss.at[i - 1], ksr.at[i - 1], bs.at[1, i - 1], br.at[1, i - 1], where),
            )

        for i in (2, 1):

            @pl.when(d >= i)
            def _():
                def tile(r):
                    at = kvs.at[i - 1, pl.ds(r, 128)]
                    col_encode(kv_rows(2 - i, r), at, kss.at[i - 1, r // 128], slice(None))

                per_tile(tiles, 128, tile)
                for c in behind(i):
                    c.start()

        def query_rows(r):
            rows = pl.ds(r, 128)
            x = 0.0
            for h in range(n_q):
                at = h % group * 128
                x = x + lane_place(dq[h // group, r // 128, at : at + 128, :] * scale, h * HD, qw)
            pad = jnp.zeros((128, 2 * kvw), f32)
            xl[rows, :] = turn_rows(jnp.concatenate([x, pad], axis=1), rows, -1.0).astype(low)

        per_tile(tiles, 128, query_rows)
        for p in range(parts):

            def put(r, x):
                at = pl.ds(p * piece + r, 16)
                get(o_out)[at, :] = (res[at, :] + x).astype(low)

            rs.total(p, put)
        ready = get(h_ready)
        for i in range(1, nt):
            pl.semaphore_signal(ready, inc=1, device_id={"tp": lax.rem(t + i, nt)}, device_id_type=MESH)

        def put_down(cols, x):
            get(o_dd)[cols, :] = x.T

        def put_gate(cols, x):
            get(o_dg)[:, cols] = x

        def put_up(cols, x):
            get(o_du)[:, cols] = x

        def put_attn(cols, x):
            get(o_da)[:, cols] = x

        gs.collect(0, put_down)
        gs.collect(1, put_gate)
        gs.collect(2, put_up)
        for i in (1, 2):

            @pl.when(d + i < nd)
            def _():
                for c in behind(i):
                    c.wait_recv()

        near1, near2 = d + 1 < nd, d + 2 < nd

        def kv_total(r):
            rows = pl.ds(r, 128)
            x = kv_rows(2, r)
            a = col_decode(kvr.at[0, rows], ksr.at[0, r // 128], slice(None))
            b = col_decode(kvr.at[1, rows], ksr.at[1, r // 128], slice(None))
            x = x + jnp.where(near1, a, 0.0) + jnp.where(near2, b, 0.0)
            pad = jnp.zeros((128, qw), f32)
            x = turn_rows(jnp.concatenate([pad, x], axis=1), rows, -1.0)
            xl[rows, qw:] = x[:, qw:].astype(low)

        per_tile(tiles, 128, kv_total)

        def hidden_rows(j):
            for c in range(0, width, 512):
                part[rows_of(j), c : c + 512] = nt_dot(xl[rows_of(j), :], wa_ref[c : c + 512, :qkvw])

        rs.finish()
        pl.semaphore_wait(ready, nt - 1)
        rs.send(0, hidden_rows)
        rs.send(1)
        hidden_rows(t)
        weight_grads(3)

        for p in range(parts):

            def put(r, x):
                at = pl.ds(p * piece + r, 16)
                y = tok[at, :].astype(f32)
                inverse = inverse_rms(y)
                normed = y * inverse
                mine[:, :width] += jnp.sum(x * normed, axis=0, keepdims=True)
                e = x * g1[...]
                e = inverse * (e - normed * jnp.mean(e * normed, axis=-1, keepdims=True))
                get(o_tg)[at, :] = rg[at, :] + e

            rs.total(p, put)
        full.run(get)
        gs.collect(3, put_attn)
        for x in (ag1, ag2, ag3, ag4, rs, wa, wg, wu, wd, gs):
            x.finish()
        for i in (2, 1):
            when(d + i < nd, lambda: ahead(i).wait_send())

            @pl.when(d >= i)
            def _():
                for c in behind(i):
                    c.wait_send()

    st.body(fn)
    return st.run()


def rope_tables(position_ids, head_size):
    half_size = head_size // 2
    inverse = rope_base ** (-(jnp.arange(half_size, dtype=jnp.float32) * 2.0 / head_size))
    angles = position_ids.astype(jnp.float32)[:, None] * inverse[None, :]
    return (jnp.cos(angles), jnp.sin(angles))


def dot(a, b):
    return jnp.dot(a, b, preferred_element_type=jnp.float32)


def on_device(
    nd, nt, tokens, positions, attn_gain, w_query, w_key, w_value, w_out, ffn_gain, w_gate, w_up, w_down, out_grad
):
    span = tokens.shape[0] * nt
    width = tokens.shape[1]
    heads = (w_query.shape[1] // HD, w_key.shape[1] // HD)
    qw, kvw = w_query.shape[1], w_key.shape[1]
    w_attn = jnp.concatenate([w_query, w_key, w_value, w_out.T], axis=1)
    w_down_t = w_down.T
    cosine, sine = rope_tables(positions, HD)
    cosine = jnp.tile(cosine, (1, 2 * heads[0]))
    sine = jnp.tile(jnp.concatenate([-sine, sine], axis=1), (1, heads[0]))
    begin = (2 * span + jnp.arange(span, dtype=jnp.int32) - positions)[None]
    output, tokens_grad, gains, down_sum, gate_sum, up_sum, attn_sum = layer(
        nd, nt, tokens, attn_gain, ffn_gain, out_grad, begin, cosine, sine, w_attn, w_gate, w_up, w_down_t, heads
    )
    cuts = (qw, qw + kvw, qw + 2 * kvw)
    return (
        output,
        tokens_grad,
        gains[0, :width],
        attn_sum[:, : cuts[0]],
        attn_sum[:, cuts[0] : cuts[1]],
        attn_sum[:, cuts[1] : cuts[2]],
        attn_sum[:, cuts[2] :].T,
        gains[0, width:],
        gate_sum,
        up_sum,
        down_sum,
    )


def solution(mesh):
    return jax.shard_map(
        functools.partial(on_device, mesh.shape["dp"], mesh.shape["tp"]),
        mesh=mesh,
        in_specs=(
            P(("dp", "tp"), None),
            P("dp"),
            P(),
            P("dp", "tp"),
            P("dp", "tp"),
            P("dp", "tp"),
            P("tp", "dp"),
            P(),
            P("dp", "tp"),
            P("dp", "tp"),
            P("tp", "dp"),
            P(("dp", "tp"), None),
        ),
        out_specs=(
            P(("dp", "tp"), None),
            P(("dp", "tp"), None),
            P(),
            P("dp", "tp"),
            P("dp", "tp"),
            P("dp", "tp"),
            P("tp", "dp"),
            P(),
            P("dp", "tp"),
            P("dp", "tp"),
            P("tp", "dp"),
        ),
        check_vma=False,
    )
```

```python
import functools
import math

import jax
import jax.numpy as jnp
from jax import lax
from jax.experimental import pallas as pl
from jax.experimental.pallas import tpu as pltpu
from jax.sharding import PartitionSpec as P

HD = 96
norm_eps = 1e-05
rope_base = 100000.0
masked_score = -1e30

MESH = pl.DeviceIdType.MESH
VMEM = pltpu.VMEM
DMA = pltpu.SemaphoreType.DMA
LEVELS = 32000.0


class Stage:
    def __init__(self, name, cid, nd, nt):
        self.name, self.cid, self.nd, self.nt = name, cid, nd, nt
        self.ins, self.outs, self.scr, self.tasks, self.links = [], [], [], [], set()

    def inp(self, x, space=VMEM):
        self.ins.append((x, space))
        return ("i", len(self.ins) - 1)

    def out(self, shape, dtype, space=VMEM):
        self.outs.append((shape, dtype, space))
        return ("o", len(self.outs) - 1)

    def scratch(self, spec):
        self.scr.append(spec)
        return ("s", len(self.scr) - 1)

    def task(self, links, gen):
        self.links |= set(links)
        self.tasks.append(gen)

    def _barrier(self):
        d, t = lax.axis_index("dp"), lax.axis_index("tp")
        nd, nt = self.nd, self.nt
        sem = pltpu.get_barrier_semaphore()
        count = 0

        def greet(ok, where):
            if ok is True:
                pl.semaphore_signal(sem, inc=1, device_id=where, device_id_type=MESH)
                return 1

            @pl.when(ok)
            def _():
                pl.semaphore_signal(sem, inc=1, device_id=where, device_id_type=MESH)

            return ok.astype(jnp.int32)

        if "line" in self.links:
            count += greet(t > 0, {"tp": t - 1})
            count += greet(t < nt - 1, {"tp": t + 1})
        if "chips" in self.links:
            for i in range(1, nd // 2):
                count += greet(True, {"dp": lax.rem(d + 2 * i, nd)})
        if "twin" in self.links:
            count += greet(True, {"dp": d + 1 - 2 * lax.rem(d, 2)})
        if "near" in self.links:
            for i in (1, 2):
                count += greet(d >= i, {"dp": d - i})
                count += greet(d < nd - i, {"dp": d + i})
        if "tp" in self.links:
            for i in range(1, nt):
                count += greet(True, {"tp": lax.rem(t + i, nt)})
        if "dp" in self.links:
            for i in range(1, nd):
                count += greet(True, {"dp": lax.rem(d + i, nd)})
        pl.semaphore_wait(sem, count)

    def run(self):
        n_in, n_out = len(self.ins), len(self.outs)

        def kernel(*refs):
            def get(h):
                kind, i = h
                return refs[i + {"i": 0, "o": n_in, "s": n_in + n_out}[kind]]

            self._barrier()
            live = [g(get) for g in self.tasks]
            while live:
                still = []
                for g in live:
                    try:
                        next(g)
                        still.append(g)
                    except StopIteration:
                        pass
                live = still

        return pl.pallas_call(
            kernel,
            out_shape=[jax.ShapeDtypeStruct(s, t) for s, t, _ in self.outs],
            in_specs=[pl.BlockSpec(memory_space=sp) for _, sp in self.ins],
            out_specs=[pl.BlockSpec(memory_space=sp) for _, _, sp in self.outs],
            scratch_shapes=self.scr,
            compiler_params=pltpu.CompilerParams(
                collective_id=self.cid, has_side_effects=True, vmem_limit_bytes=67_000_000
            ),
            name=self.name,
        )(*[x for x, _ in self.ins])


def remote(src, dst, send, recv, where):
    return pltpu.make_async_remote_copy(
        src_ref=src, dst_ref=dst, send_sem=send, recv_sem=recv, device_id=where, device_id_type=MESH
    )


def when(ok, fn):
    if ok is True:
        fn()
    elif ok is not False:
        pl.when(ok)(fn)


def over_cols(width, fn):
    def body(c, _):
        fn(pl.ds(pl.multiple_of(c * 128, 128), 128))
        return 0

    lax.fori_loop(0, width // 128, body, 0)
    if width % 128:
        fn(pl.ds(width // 128 * 128, width % 128))


def row_encode(read, code, scale, rows):
    step = 16

    def body(i, held):
        r = pl.multiple_of(i * step, step)
        x = read(r, step)
        top = jnp.max(jnp.abs(x), axis=-1, keepdims=True)
        code[pl.ds(r, step), :] = jnp.round(x * (LEVELS / jnp.maximum(top, 1e-30))).astype(jnp.int32).astype(jnp.int16)
        lane = lax.broadcasted_iota(jnp.int32, (step, 128), 1)
        row = lax.broadcasted_iota(jnp.int32, (step, 128), 0) + r
        mine = jnp.sum(jnp.where(lane == row, jnp.maximum(top, 1e-30) * (1.0 / LEVELS), 0.0), axis=0, keepdims=True)
        return held + jnp.broadcast_to(mine, (8, 128))

    scale[...] = lax.fori_loop(0, rows // step, body, jnp.zeros((8, 128), jnp.float32))


def row_decode(code, scale, r, step):
    lane = lax.broadcasted_iota(jnp.int32, (step, 128), 1)
    row = lax.broadcasted_iota(jnp.int32, (step, 128), 0) + r
    col = jnp.sum(jnp.where(lane == row, jnp.broadcast_to(scale[0:1, :], (step, 128)), 0.0), axis=-1, keepdims=True)
    return code[pl.ds(r, step), :].astype(jnp.int32).astype(jnp.float32) * col


def col_encode(x, code, scale, cols):
    top = jnp.maximum(jnp.max(jnp.abs(x), axis=0, keepdims=True), 1e-30)
    code[:, cols] = jnp.round(x * (LEVELS / top)).astype(jnp.int32).astype(jnp.int16)
    scale[:, cols] = top * (1.0 / LEVELS)


def col_decode(code, scale, cols):
    return code[:, cols].astype(jnp.int32).astype(jnp.float32) * scale[:, cols]


class LineGather:
    def __init__(self, st, full, rows, parts):
        self.st, self.full, self.rows, self.parts = st, full, rows, parts
        self.hs = st.scratch(DMA((2, st.nt, parts)))
        self.hr = st.scratch(DMA((2, st.nt, parts)))
        st.links.add("line")

    def bind(self, get):
        self.ref, self.ss, self.rs = get(self.full), get(self.hs), get(self.hr)
        self.t = lax.axis_index("tp")
        return self

    def piece(self, owner, p):
        chunk = self.rows // self.parts
        return self.ref.at[pl.ds(pl.multiple_of(owner * self.rows + p * chunk, chunk), chunk)]

    def hop(self, owner, k, s, p, where):
        at = self.piece(owner, p)
        return remote(at, at, self.ss.at[k, s, p], self.rs.at[k, s, p], {"tp": where})

    def _send(self, s, p, k, way):
        nt, t = self.st.nt, self.t
        owner, where = t - s * way, t + way
        ok = (owner >= 0) & (owner < nt) & (where >= 0) & (where < nt)
        when(ok, lambda: self.hop(owner, k, s, p, where).start())

    def start(self, p):
        for k, way in enumerate((1, -1)):
            self._send(0, p, k, way)

    def arrive(self, s, p):
        nt, t = self.st.nt, self.t
        for k, way in enumerate((1, -1)):
            owner = t - way * (s + 1)
            ok = (owner >= 0) & (owner < nt)
            when(ok, lambda: self.hop(owner, k, s, p, t).wait_recv())
            if s < nt - 2:
                self._send(s + 1, p, k, way)

    def arrive_at(self, v):
        nt, t = self.st.nt, self.t
        s, p = v // self.parts, lax.rem(v, self.parts)
        for k, way in enumerate((1, -1)):
            owner = t - way * (s + 1)
            ok = (owner >= 0) & (owner < nt) & (s < nt - 1)
            where = t + way

            @pl.when(ok)
            def _():
                self.hop(owner, k, s, p, t).wait_recv()
                when((where >= 0) & (where < nt) & (s < nt - 2), lambda: self.hop(owner, k, s + 1, p, where).start())

    def arrivals(self):
        return [
            functools.partial(self.arrive, s, p) for s in range(self.st.nt - 1) for p in range(self.parts)
        ]

    def finish(self):
        nt, t = self.st.nt, self.t
        for s in range(nt - 1):
            for p in range(self.parts):
                for k, way in enumerate((1, -1)):
                    owner, where = t - s * way, t + way
                    ok = (owner >= 0) & (owner < nt) & (where >= 0) & (where < nt)
                    when(ok, lambda: self.hop(owner, k, s, p, where).wait_send())


class LineSum:
    def __init__(self, st, part, rows, width, parts):
        self.st, self.part, self.rows, self.width, self.parts = st, part, rows, width, parts
        nt = st.nt
        self.chunk = rows // parts
        shape = (nt, parts, self.chunk, width)
        self.hc = [st.scratch(VMEM(shape, jnp.int16)) for _ in range(2)]
        self.hk = [st.scratch(VMEM(shape[:2] + (8, 128), jnp.float32)) for _ in range(2)]
        self.hd = [st.scratch(DMA((2, nt, parts))) for _ in range(2)]
        st.links.add("tp")

    def bind(self, get):
        self.x = get(self.part)
        (self.cs, self.cr), (self.sc, self.sr), (self.ss, self.rs) = (
            [get(h) for h in hs] for hs in (self.hc, self.hk, self.hd)
        )
        self.t = lax.axis_index("tp")
        return self

    def far(self, i, j):
        return (jnp.abs(i - j) == 3) if self.st.nt == 4 else (i != i)

    def sends(self, j, p):
        t = self.t
        where = jnp.where(self.far(t, j), jnp.where(j > t, t + 1, t - 1), j)
        slot = jnp.where(self.far(t, j), where, t)
        return (
            remote(self.cs.at[j, p], self.cr.at[slot, p], self.ss.at[0, j, p], self.rs.at[0, slot, p], {"tp": where}),
            remote(self.sc.at[j, p], self.sr.at[slot, p], self.ss.at[1, j, p], self.rs.at[1, slot, p], {"tp": where}),
        )

    def arrival(self, slot, p):
        for k, (x, y) in enumerate(((self.cs, self.cr), (self.sc, self.sr))):
            remote(x.at[slot, p], y.at[slot, p], self.ss.at[k, slot, p], self.rs.at[k, slot, p], {"tp": self.t}).wait_recv()

    def dest(self, o):
        nt, t = self.st.nt, self.t
        if nt != 4:
            return lax.rem(t + 1 + o, nt)
        inner = jnp.where(o == 2, 2, 1 + 2 * o)
        x = jnp.where((t == 0) | (t == nt - 1), 3 - o, inner)
        lo = lax.rem(lax.rem(t, 2) + lax.rem(x, 2), 2)
        return 2 * lax.rem(t // 2 + x // 2, 2) + lo

    def _rows(self, base, r, n):
        return self.x[pl.ds(pl.multiple_of(base + r, n), n), :]

    def send(self, p, produce=None, beside=None):
        nt, t, chunk = self.st.nt, self.t, self.chunk

        def one(o, _):
            j = self.dest(o)
            if produce is not None:
                produce(j)
            base = j * self.rows + p * chunk
            if nt == 4:
                relay = ((t == 1) & (j == 3)) | ((t == 2) & (j == 0))

                @pl.when(relay)
                def _():
                    self.arrival(t, p)
                    row_encode(
                        lambda r, n: self._rows(base, r, n) + row_decode(self.cr.at[t, p], self.sr.at[t, p], r, n),
                        self.cs.at[j, p],
                        self.sc.at[j, p],
                        chunk,
                    )

                plain = jnp.logical_not(relay)
            else:
                plain = True
            when(plain, lambda: row_encode(lambda r, n: self._rows(base, r, n), self.cs.at[j, p], self.sc.at[j, p], chunk))
            for c in self.sends(j, p):
                c.start()
            if beside is not None:
                beside(o)
            return 0

        lax.fori_loop(0, nt - 1, one, 0)

    def total(self, p, put):
        nt, t, chunk = self.st.nt, self.t, self.chunk
        sources = [lax.rem(t + 1 + i, nt) for i in range(nt - 1)]
        for i in sources:
            pl.when(jnp.logical_not(self.far(i, t)))(lambda: self.arrival(i, p))
        base = t * self.rows + p * chunk

        def body(n, _):
            r = pl.multiple_of(n * 16, 16)
            x = self._rows(base, r, 16)
            for i in sources:
                y = row_decode(self.cr.at[i, p], self.sr.at[i, p], r, 16)
                x = x + (jnp.where(self.far(i, t), 0.0, y) if nt == 4 else y)
            put(r, x)
            return 0

        lax.fori_loop(0, chunk // 16, body, 0)

    def finish(self):
        def one(o, _):
            for p in range(self.parts):
                for c in self.sends(self.dest(o), p):
                    c.wait_send()
            return 0

        lax.fori_loop(0, self.st.nt - 1, one, 0)


class ChipGather:
    def __init__(self, st, w, full, rows):
        self.st, self.w, self.full, self.rows = st, w, full, rows
        self.square = st.nd == 8
        self.hops = 4 if self.square else st.nd // 2 - 1
        self.hs, self.hr = (st.scratch(DMA((2 * self.hops + 1,))) for _ in range(2))
        self.hl = st.scratch(DMA((1,)))
        st.links |= {"chips", "twin"}

    def bind(self, get):
        self.x, self.o, self.ss, self.rs, ls = (get(h) for h in (self.w, self.full, self.hs, self.hr, self.hl))
        nd, rows, n = self.st.nd, self.rows, self.hops
        d = lax.axis_index("dp")
        core, chip = lax.rem(d, 2), d // 2
        twin = {"dp": d + 1 - 2 * core}

        def at(i, part=None):
            if part is None:
                return self.o.at[pl.ds(pl.multiple_of(i * rows, rows), rows)]
            return self.o.at[pl.ds(pl.multiple_of(i * rows + part * (rows // 2), rows // 2), rows // 2)]

        beside = [chip + 1 - 2 * lax.rem(chip, 2), lax.rem(chip + 2, 4)]
        near = [2 * c + core for c in beside]
        diagonal = 2 * lax.rem(beside[0] + 2, 4) + core

        def came(i):
            if not self.square:
                return at(lax.rem(d - 2 * i - 2 + nd, nd))
            return at(near[i]) if i < 2 else at(diagonal, i - 2)

        def hop(i):
            if not self.square:
                src, dst, where = self.x, at(d), lax.rem(d + 2 * i + 2, nd)
            elif i < 2:
                src, dst, where = self.x, at(d), near[i]
            else:
                src = dst = at(near[i - 2], i - 2)
                where = near[3 - i]
            return remote(src, dst, self.ss.at[i], self.rs.at[i], {"dp": where})

        def landed(i):
            return remote(came(i), came(i), self.ss.at[i], self.rs.at[i], twin)

        def give(i):
            src, dst = (self.x, at(d)) if i == 0 else (came(i - 1), came(i - 1))
            return remote(src, dst, self.ss.at[n + i], self.rs.at[n + i], twin)

        self.own = lambda: pltpu.make_async_copy(self.x, at(d), ls.at[0])
        self.hop, self.landed, self.give = hop, landed, give
        return self

    def start(self):
        for i in range(2 if self.square else self.hops):
            self.hop(i).start()
        self.give(0).start()
        self.own().start()

    def forward(self, i):
        self.landed(i).wait_recv()
        if self.square and i < 2:
            self.hop(i + 2).start()
        self.give(i + 1).start()

    def forwards(self):
        return [functools.partial(self.forward, i) for i in range(self.hops)]

    def arrived(self):
        for i in range(self.hops + 1):
            self.give(i).wait_recv()
        self.own().wait()

    def finish(self):
        for i in range(self.hops + 1):
            self.give(i).wait_send()
        for i in range(self.hops):
            self.hop(i).wait_send()


class GradScatter:
    def __init__(self, st, shard, widths, sums):
        nc = self.nc = st.nd // 2
        self.st, self.shard, self.widths = st, shard, widths
        self.m = math.lcm(2 * shard, 128) // (2 * shard)
        self.chunks = nc // self.m
        self.padded = [-(-w // 128) * 128 for w in widths]
        wide = max(self.padded)
        self.hg = st.scratch(VMEM((2, 2 * self.m * shard, wide), jnp.float32))
        self.ht = st.scratch(VMEM((2, self.m, shard, wide), jnp.float32))
        self.slots = self.chunks - (self.m == 1)
        self.hs = st.scratch(VMEM((self.slots, self.m, shard, wide), jnp.int16))
        self.hk = st.scratch(VMEM((self.slots, self.m, 1, wide), jnp.float32))
        self.hcr = [st.scratch(VMEM((nc - 1, shard, w), jnp.int16)) for w in self.padded]
        self.hkr = [st.scratch(VMEM((nc - 1, 1, w), jnp.float32)) for w in self.padded]
        self.ha = sums
        self.hgs = [st.scratch(DMA((2, self.m))) for _ in range(2)]
        self.hss = st.scratch(DMA((2, self.slots, self.m)))
        self.hsr = st.scratch(DMA((len(widths), 2, nc - 1)))
        self.hf = st.scratch(pltpu.SemaphoreType.REGULAR)
        st.links |= {"chips", "twin"}

    def bind(self, get):
        self.g, self.t, self.cs, self.sc, self.ss, self.sr, self.free = (
            get(h) for h in (self.hg, self.ht, self.hs, self.hk, self.hss, self.hsr, self.hf)
        )
        self.cr, self.kr, self.acc = ([get(h) for h in hs] for hs in (self.hcr, self.hkr, self.ha))
        self.gs, self.gr = (get(h) for h in self.hgs)
        d = self.d = lax.axis_index("dp")
        self.core, self.chip = lax.rem(d, 2), d // 2
        self.twin = {"dp": d + 1 - 2 * self.core}
        return self

    def chunk(self, i):
        return lax.rem(self.chip // self.m + 1 + i, self.chunks)

    def half(self, e, core):
        return pl.ds(pl.multiple_of((2 * e + core) * self.shard, self.shard), self.shard)

    def gift(self, a, r, e):
        cols = pl.ds(0, self.padded[a])
        return remote(
            self.g.at[r, self.half(e, 1 - self.core), cols], self.t.at[r, e, :, cols], self.gs.at[r, e], self.gr.at[r, e],
            self.twin,
        )

    def sums(self, a, i, e, dest):
        cols, nc = pl.ds(0, self.padded[a]), self.nc
        slot = jnp.maximum(lax.rem(dest - self.chip + nc, nc) - 1, 0)
        where = {"dp": 2 * dest + self.core}
        return (
            remote(self.cs.at[i, e, :, cols], self.cr[a].at[slot], self.ss.at[0, i, e], self.sr.at[a, 0, slot], where),
            remote(self.sc.at[i, e, :, cols], self.kr[a].at[slot], self.ss.at[1, i, e], self.sr.at[a, 1, slot], where),
        )

    def compute(self, a, i, pieces):
        n = a * self.chunks + i
        r = lax.rem(n, 2)
        rows = 2 * self.m * self.shard

        @pl.when(n >= 2)
        def _():
            for e in range(self.m):
                self.gift(a, r, e).wait_send() if a == 0 else self._sent(a, i, r, e)
            pl.semaphore_wait(self.free, 1)

        cols = pl.ds(pl.multiple_of(self.chunk(i) * rows, 128), rows)
        at = 0
        for x, y in pieces:
            z = y()
            self.g[r, :, at : at + z.shape[1]] = tn_dot(x[:, cols], z)
            at += z.shape[1]
        for e in range(self.m):
            self.gift(a, r, e).start()

    def _sent(self, a, i, r, e):
        pl.when(i >= 2)(lambda: self.gift(a, r, e).wait_send())
        pl.when(i < 2)(lambda: self.gift(a - 1, r, e).wait_send())

    def combine(self, a, i):
        n = a * self.chunks + i
        r = lax.rem(n, 2)
        for e in range(self.m):
            self.gift(a, r, e).wait_recv()
            dest = self.chunk(i) * self.m + e
            away = dest != self.chip
            own = self.half(e, self.core)

            @pl.when(away)
            def _():
                if a:
                    for c in self.sums(a - 1, i, e, dest):
                        c.wait_send()
                over_cols(
                    self.widths[a],
                    lambda cols: col_encode(
                        self.g[r, own, cols] + self.t[r, e, :, cols], self.cs.at[i, e], self.sc.at[i, e], cols
                    ),
                )
                for c in self.sums(a, i, e, dest):
                    c.start()

            @pl.when(jnp.logical_not(away))
            def _():
                over_cols(self.widths[a], lambda cols: self._keep(a, r, e, own, cols))

        @pl.when(n + 2 < len(self.widths) * self.chunks)
        def _():
            pl.semaphore_signal(self.free, inc=1, device_id=self.twin, device_id_type=MESH)

    def _keep(self, a, r, e, own, cols):
        self.acc[a][:, cols] = self.g[r, own, cols] + self.t[r, e, :, cols]

    def slot(self, a, w, pieces):
        pl.when(w < self.chunks)(lambda: self.compute(a, w, pieces))
        pl.when((w >= 1) & (w <= self.chunks))(lambda: self.combine(a, w - 1))

    def collect(self, a, put):
        n = self.nc - 1
        for i in range(n):
            for c in self.sums(a, 0, 0, lax.rem(self.chip + 1 + i, self.nc)):
                c.wait_recv()

        def tile(cols):
            x = self.acc[a][:, cols]
            for i in range(n):
                x = x + col_decode(self.cr[a].at[i], self.kr[a].at[i], cols)
            put(cols, x)

        over_cols(self.widths[a], tile)

    def finish(self):
        a = len(self.widths) - 1
        for i in range(self.chunks):
            for e in range(self.m):
                if i >= self.chunks - 2:
                    self.gift(a, (a * self.chunks + i) % 2, e).wait_send()
                if i < self.slots:
                    dest = self.chunk(i) * self.m + e

                    @pl.when(dest != self.chip)
                    def _():
                        for c in self.sums(a, i, e, dest):
                            c.wait_send()


class FullSum:
    def __init__(self, st, x, out, shape):
        self.st, self.x, self.out = st, x, out
        self.ha = st.scratch(VMEM((st.nt,) + shape, jnp.float32))
        self.hm = st.scratch(VMEM(shape, jnp.float32))
        self.hb = st.scratch(VMEM((st.nd,) + shape, jnp.float32))
        self.hs = st.scratch(DMA((2, max(st.nd, st.nt))))
        self.hr = st.scratch(DMA((2, max(st.nd, st.nt))))
        st.links |= {"tp", "dp"}

    def run(self, get):
        nd, nt = self.st.nd, self.st.nt
        x, o, a, m, b, ss, rs = (get(h) for h in (self.x, self.out, self.ha, self.hm, self.hb, self.hs, self.hr))
        for k, (axis, n, src, got, dst) in enumerate((("tp", nt, x, a, m), ("dp", nd, m, b, o))):
            me = lax.axis_index(axis)
            cs = [
                remote(src, got.at[me], ss.at[k, i], rs.at[k, i], {axis: lax.rem(me + i, n)}) for i in range(1, n)
            ]
            for c in cs:
                c.start()
            got[me] = src[...]
            for c in cs:
                c.wait()
            total = got[0]
            for i in range(1, n):
                total = total + got[i]
            dst[...] = total


def lane_take(x, offset):
    base = offset // 128 * 128
    wide = min(256, x.shape[-1] - base)
    slab = x[:, base : base + wide]
    if wide % 128:
        slab = jnp.concatenate([slab, jnp.zeros((x.shape[0], -wide % 128), x.dtype)], axis=1)
        wide = slab.shape[-1]
    if offset > base:
        slab = pltpu.roll(slab, wide - (offset - base), 1)
    slab = slab[:, :128]
    return jnp.where(lax.broadcasted_iota(jnp.int32, slab.shape, 1) < HD, slab, 0.0)


def lane_place(x, offset, width):
    base = offset // 128 * 128
    wide = min(256, width - base)
    slab = x if wide == 128 else jnp.concatenate([x, jnp.zeros_like(x)], axis=1)
    if offset > base:
        slab = pltpu.roll(slab, offset - base, 1)
    slab = slab[:, :wide]
    pieces = []
    if base:
        pieces.append(jnp.zeros((x.shape[0], base), x.dtype))
    pieces.append(slab)
    if base + wide < width:
        pieces.append(jnp.zeros((x.shape[0], width - base - wide), x.dtype))
    return jnp.concatenate(pieces, axis=1) if len(pieces) > 1 else slab


def turned(u, cosine, sine):
    wide = u.shape[-1]
    lane = lax.rem(lax.broadcasted_iota(jnp.int32, u.shape, 1), HD)
    swap = jnp.where(lane < HD // 2, pltpu.roll(u, wide - HD // 2, 1), pltpu.roll(u, HD // 2, 1))
    return u * cosine + swap * sine


def nt_dot(a, b):
    return lax.dot_general(a, b, (((1,), (1,)), ((), ())), preferred_element_type=jnp.float32)


def per_tile(count, size, fn):
    def body(i, _):
        fn(pl.multiple_of(i * size, size))
        return 0

    lax.fori_loop(0, count, body, 0)


def in_turn(*lists):
    for i in range(max(len(x) for x in lists)):
        for x in lists:
            if i < len(x):
                x[i]()


class Fused(Stage):
    def body(self, fn):
        self.tasks = [lambda get: iter(fn(get) or ())]


def inverse_rms(x):
    return lax.rsqrt(jnp.mean(x * x, axis=-1, keepdims=True) + norm_eps)


def tn_dot(a, b):
    return lax.dot_general(a, b, (((0,), (0,)), ((), ())), preferred_element_type=jnp.float32)


def across(x, count):
    return jnp.concatenate([x] * count, axis=1) if count > 1 else x


def masked_scores(keys, queries, first, begin, span, group):
    s = nt_dot(keys, queries) * (1.0 / math.sqrt(HD))
    key = lax.broadcasted_iota(jnp.int32, s.shape, 0) + first
    own = lax.rem(lax.broadcasted_iota(jnp.int32, s.shape, 1), 128) + (first + 2 * span)
    return s, (key >= across(begin, group)) & (key <= own)


def layer(
    nd, nt, tokens, attn_gain, ffn_gain, out_grad, begin, cosine, sine, w_attn, w_gate, w_up, w_down_t, heads
):
    st = Fused("layer", 1, nd, nt)
    low, f32 = jnp.bfloat16, jnp.float32
    own, width = tokens.shape
    span = own * nt
    shard, units = w_gate.shape
    n_q, n_kv = heads
    group = n_q // n_kv
    tiles = span // 128
    qw, kvw = n_q * HD, n_kv * HD
    qkvw = qw + 2 * kvw
    reach = 2 * span + 128
    parts = 2
    piece = own // parts
    scale = 1.0 / math.sqrt(HD)

    h_tok, h_g1, h_g2 = st.inp(tokens), st.inp(attn_gain[None]), st.inp(ffn_gain[None])
    h_og, h_begin = st.inp(out_grad), st.inp(begin)
    h_cos, h_sin = st.inp(cosine), st.inp(sine)
    s_wa, s_wg, s_wu, s_wd = (st.inp(w, pl.ANY) for w in (w_attn, w_gate, w_up, w_down_t))

    o_out = st.out((own, width), low)
    o_tg = st.out((own, width), f32)
    o_gains = st.out((1, 2 * width), f32)
    o_dd = st.out((units, shard), f32)
    o_dg, o_du = (st.out((shard, units), f32) for _ in range(2))
    o_da, o_db = (st.out((shard, w), f32) for w in (2 * qw, 2 * kvw))

    def room(shape, dtype=f32):
        return st.scratch(VMEM(shape, dtype))

    h_h1, h_h2, h_gr, h_rl = (room((span, width), low) for _ in range(4))
    h_wa = room((width, qkvw + qw), low)
    h_wg, h_wu, h_wd = (room((width, units), low) for _ in range(3))
    h_q, h_dc, h_ch = (room((n_kv, tiles, group * 128, 128), low) for _ in range(3))
    h_k, h_v = (room((n_kv, 3 * span, 128), low) for _ in range(2))
    h_vt = room((n_kv, 128, 3 * span), low)
    h_win = room((3, span, 2 * kvw), low)
    h_ctx = room((span, qw), low)
    h_lse, h_delta = (room((n_kv, tiles, 1, group * 128)) for _ in range(2))
    h_res, h_rg = (room((own, width)) for _ in range(2))
    h_part = room((span, width))
    h_ia, h_gl, h_ul = (room((span, units), low) for _ in range(3))
    h_dq = room((n_kv, tiles, group * 128, 128))
    h_dk, h_dv = (room((n_kv, 3 * span, 128)) for _ in range(2))
    h_kvs, h_kvr = (room((2, span, 2 * kvw), jnp.int16) for _ in range(2))
    h_kss, h_ksr = (room((2, tiles, 1, 2 * kvw)) for _ in range(2))
    h_mine = room((1, 2 * width))
    h_fs, h_fr = (st.scratch(DMA((2,))) for _ in range(2))
    h_bs, h_br = (st.scratch(DMA((2, 2))) for _ in range(2))
    h_ready = st.scratch(pltpu.SemaphoreType.REGULAR)

    ag1 = LineGather(st, h_h1, own, parts)
    ag2 = LineGather(st, h_h2, own, parts)
    ag3 = LineGather(st, h_gr, own, parts)
    ag4 = LineGather(st, h_rl, own, parts)
    rs = LineSum(st, h_part, own, width, parts)
    wa = ChipGather(st, s_wa, h_wa, shard)
    wg = ChipGather(st, s_wg, h_wg, shard)
    wu = ChipGather(st, s_wu, h_wu, shard)
    wd = ChipGather(st, s_wd, h_wd, shard)
    gs = GradScatter(st, shard, (units, units, units, 2 * qw, 2 * kvw), (room((shard, units)), o_dg, o_du, o_da, o_db))
    full = FullSum(st, h_mine, o_gains, (1, 2 * width))
    st.links.add("near")

    def fn(get):
        d, t = lax.axis_index("dp"), lax.axis_index("tp")
        for x in (ag1, ag2, ag3, ag4, rs, wa, wg, wu, wd, gs):
            x.bind(get)
        tok, g1, g2, og, begin_ref, cos_ref, sin_ref = (get(h) for h in (h_tok, h_g1, h_g2, h_og, h_begin, h_cos, h_sin))
        h1, h2, gr, rl = (get(h) for h in (h_h1, h_h2, h_gr, h_rl))
        wa_ref, wg_ref, wu_ref, wd_ref = (get(h) for h in (h_wa, h_wg, h_wu, h_wd))
        q, k, v, vt, win, ctx, ch, lse = (get(h) for h in (h_q, h_k, h_v, h_vt, h_win, h_ctx, h_ch, h_lse))
        dc, delta, dq, dk, dv = (get(h) for h in (h_dc, h_delta, h_dq, h_dk, h_dv))
        res, rg, part, ia, gl, ul, mine = (get(h) for h in (h_res, h_rg, h_part, h_ia, h_gl, h_ul, h_mine))
        xl = ul.at[:, pl.ds(0, qkvw)]
        kvs, kvr, kss, ksr, fs, fr, bs, br = (
            get(h) for h in (h_kvs, h_kvr, h_kss, h_ksr, h_fs, h_fr, h_bs, h_br)
        )

        def own_rows(p, r, n=16):
            return pl.ds(pl.multiple_of(t * own + p * piece + r, n), n)

        def rows_of(j):
            return pl.ds(pl.multiple_of(j * own, own), own)

        wa.start()
        wd.start()
        for p in range(parts):

            def tile(r):
                x = tok[pl.ds(p * piece + r, 16), :].astype(f32)
                h1[own_rows(p, r), :] = (x * inverse_rms(x) * g1[...]).astype(low)

            per_tile(piece // 16, 16, tile)
            ag1.start(p)
        gr[rows_of(t), :] = og[...]
        pass_a, pass_d, pass_g, pass_u = (x.forwards() for x in (wa, wd, wg, wu))
        in_turn(ag1.arrivals(), pass_a[:2] + pass_d[:2] + pass_a[2:])
        for p in range(parts):
            ag3.start(p)
        wa.arrived()

        def turn_rows(x, rows, way):
            cosine, sine = across(cos_ref[rows, :], 2), across(sin_ref[rows, :], 2)
            lane = lax.broadcasted_iota(jnp.int32, x.shape, 1)
            return jnp.where(lane < qw + kvw, turned(x, cosine, way * sine), x)

        def project(r):
            rows = pl.ds(r, 128)
            x = turn_rows(dot(h1[rows, :], wa_ref[:, :qkvw]), rows, 1.0)
            for h in range(n_q):
                q[h // group, r // 128, h % group * 128 : (h % group + 1) * 128, :] = lane_take(x, h * HD).astype(low)
            win[2, rows, :] = x[:, qw:].astype(low)

        per_tile(tiles, 128, project)

        def ahead(i):
            return remote(win.at[2], win.at[2 - i], fs.at[i - 1], fr.at[i - 1], {"dp": d + i})

        for i in (2, 1):
            when(d + i < nd, lambda: ahead(i).start())

        def unpack(b):
            def tile(r):
                x = win[b, pl.ds(r, 128), :].astype(f32)
                at = pl.ds(pl.multiple_of(b * span + r, 128), 128)
                for g in range(n_kv):
                    k[g, at, :] = lane_take(x, g * HD).astype(low)
                    y = lane_take(x, kvw + g * HD)
                    v[g, at, :] = y.astype(low)
                    vt[g, :, at] = y.T.astype(low)

            per_tile(tiles, 128, tile)

        unpack(2)
        for x in pass_d[2:]:
            x()
        for i in (1, 2):

            @pl.when(d < i)
            def _():
                win[2 - i] = jnp.zeros((span, 2 * kvw), low)

            when(d >= i, lambda: ahead(i).wait_recv())
            unpack(2 - i)
        wg.start()
        wu.start()

        def attend(u, _):
            g, i = u // tiles, lax.rem(u, tiles)
            at = pl.multiple_of(i * 128, 128)
            keys = pl.ds(at, reach)
            s, seen = masked_scores(k[g, keys, :], q[g, i], at, begin_ref[:, pl.ds(at, 128)], span, group)
            s = jnp.where(seen, s, masked_score)
            top = jnp.max(s, axis=0, keepdims=True)
            e = jnp.exp(s - top)
            total = jnp.sum(e, axis=0, keepdims=True)
            p = (e * (1.0 / total)).astype(low)
            lse[g, i] = top + jnp.log(total)
            ch[g, i] = dot(vt[g, :, keys], p).T.astype(low)
            return 0

        half = max(1, n_kv * tiles // 2)
        arrive3 = ag3.arrivals()
        lax.fori_loop(0, half, attend, 0)
        cut = len(arrive3) // 2
        in_turn(arrive3[:cut], pass_g[:2])
        lax.fori_loop(half, n_kv * tiles, attend, 0)
        in_turn(arrive3[cut:], pass_u[:2])

        def pack(r):
            x = 0.0
            for h in range(n_q):
                at = h % group * 128
                x = x + lane_place(ch[h // group, r // 128, at : at + 128, :].astype(f32), h * HD, qw)
            ctx[pl.ds(r, 128), :] = x.astype(low)

        per_tile(tiles, 128, pack)

        def out_rows(j):
            for c in range(0, width, 512):
                part[rows_of(j), c : c + 512] = nt_dot(ctx[rows_of(j), :], wa_ref[c : c + 512, qkvw:])

        rs.send(0, out_rows)
        rs.send(1)
        out_rows(t)
        kt = vt

        def keys_back(r):
            for g in range(n_kv):
                kt[g, :, pl.ds(r, 128)] = k[g, pl.ds(r, 128), :].T

        per_tile(3 * tiles, 128, keys_back)
        in_turn(pass_g[2:], pass_u[2:])

        for p in range(parts):

            def put(r, x):
                at = pl.ds(p * piece + r, 16)
                x = x + tok[at, :].astype(f32)
                res[at, :] = x
                h2[own_rows(p, r), :] = (x * inverse_rms(x) * g2[...]).astype(low)

            rs.total(p, put)
            ag2.start(p)
        wd.arrived()

        def back_act(c):
            part[:, pl.ds(c, 256)] = dot(gr[...], wd_ref[:, pl.ds(c, 256)])

        arrive2 = ag2.arrivals()
        for x in arrive2[:parts]:
            x()
        per_tile(units // 256, 256, back_act)
        for x in arrive2[parts:]:
            x()
        wg.arrived()
        wu.arrived()

        def act(c):
            cols = pl.ds(c, 256)
            gate = dot(h2[...], wg_ref[:, cols])
            up = dot(h2[...], wu_ref[:, cols])
            back = part[:, cols]
            sig = jax.nn.sigmoid(gate)
            ia[:, cols] = (gate * sig * up).astype(low)
            gl[:, cols] = (back * up * (sig * (1.0 + gate * (1.0 - sig)))).astype(low)
            ul[:, cols] = (back * gate * sig).astype(low)

        per_tile(units // 256, 256, act)

        def rows_back(j):
            rows = rows_of(j)
            for c in range(0, width, 512):
                part[rows, c : c + 512] = nt_dot(gl[rows, :], wg_ref[c : c + 512, :]) + nt_dot(
                    ul[rows, :], wu_ref[c : c + 512, :]
                )

        last_slot = gs.chunks + 1
        grads = (
            ((gr, lambda: ia[...]),),
            ((h2, lambda: gl[...]),),
            ((h2, lambda: ul[...]),),
            ((h1, lambda: xl[:, :qw]), (rl, lambda: ctx[...])),
            ((h1, lambda: xl[:, qw:]),),
        )

        def weight_grads(a, first=0):
            def one(w, _):
                gs.slot(a, w, grads[a])
                return 0

            lax.fori_loop(first, last_slot, one, 0)

        rs.finish()
        rs.send(0, rows_back, lambda o: gs.slot(0, o, grads[0]))
        rs.send(1)
        rows_back(t)
        weight_grads(0, nt - 1)
        mine[...] = jnp.zeros_like(mine)

        for p in range(parts):

            def put(r, x):
                at = pl.ds(p * piece + r, 16)
                y = res[at, :]
                inverse = inverse_rms(y)
                normed = y * inverse
                mine[:, width:] += jnp.sum(x * normed, axis=0, keepdims=True)
                e = x * g2[...]
                back = inverse * (e - normed * jnp.mean(e * normed, axis=-1, keepdims=True))
                y = og[at, :].astype(f32) + back
                rg[at, :] = y
                rl[own_rows(p, r), :] = y.astype(low)

            rs.total(p, put)
            ag4.start(p)

        def ffn_rows(r):
            cols = pl.ds(r, 512)
            part[:, cols] = nt_dot(ia[...], wd_ref[cols, :])

        def while_gathered(w, _):
            ag4.arrive_at(w)
            pl.when(w < width // 512)(lambda: ffn_rows(pl.multiple_of(w * 512, 512)))
            gs.slot(1, w, grads[1])
            return 0

        lax.fori_loop(0, max((nt - 1) * parts, last_slot, width // 512), while_gathered, 0)

        def context_back(r):
            x = dot(rl[pl.ds(r, 128), :], wa_ref[:, qkvw:])
            i = r // 128
            for h in range(n_q):
                g, at = h // group, pl.ds(h % group * 128, 128)
                y = lane_take(x, h * HD).astype(low)
                dc[g, i, at, :] = y
                z = y.astype(f32) * ch[g, i, at, :].astype(f32)
                delta[g, i, :, at] = jnp.sum(z.T, axis=0, keepdims=True)

        rs.finish()
        for p in range(parts):
            rs.send(p)
        per_tile(tiles, 128, context_back)
        dk[...] = jnp.zeros_like(dk)
        dv[...] = jnp.zeros_like(dv)
        count = n_kv * tiles

        def attend_back(u, _):
            g, i = u // tiles, lax.rem(u, tiles)
            at = pl.multiple_of(i * 128, 128)
            keys = pl.ds(at, reach)
            qq, dd = q[g, i], dc[g, i]
            s, seen = masked_scores(k[g, keys, :], qq, at, begin_ref[:, pl.ds(at, 128)], span, group)
            p = jnp.where(seen, jnp.exp(s - lse[g, i]), 0.0)
            ds = (p * (nt_dot(v[g, keys, :], dd) - delta[g, i])).astype(low)
            dv[g, keys, :] += dot(p.astype(low), dd)
            dk[g, keys, :] += dot(ds, qq)
            dq[g, i] = dot(kt[g, :, keys], ds).T
            gs.slot(2, u, grads[2])
            return 0

        lax.fori_loop(0, count, attend_back, 0)
        weight_grads(2, count)

        def kv_rows(b, r):
            at = pl.ds(pl.multiple_of(b * span + r, 128), 128)
            x = 0.0
            for g in range(n_kv):
                x = x + lane_place(dk[g, at, :] * scale, g * HD, 2 * kvw)
                x = x + lane_place(dv[g, at, :], kvw + g * HD, 2 * kvw)
            return x

        def behind(i):
            where = {"dp": d - i}
            return (
                remote(kvs.at[i - 1], kvr.at[i - 1], bs.at[0, i - 1], br.at[0, i - 1], where),
                remote(kss.at[i - 1], ksr.at[i - 1], bs.at[1, i - 1], br.at[1, i - 1], where),
            )

        for i in (2, 1):

            @pl.when(d >= i)
            def _():
                def tile(r):
                    at = kvs.at[i - 1, pl.ds(r, 128)]
                    col_encode(kv_rows(2 - i, r), at, kss.at[i - 1, r // 128], slice(None))

                per_tile(tiles, 128, tile)
                for c in behind(i):
                    c.start()

        def query_rows(r):
            rows = pl.ds(r, 128)
            x = 0.0
            for h in range(n_q):
                at = h % group * 128
                x = x + lane_place(dq[h // group, r // 128, at : at + 128, :] * scale, h * HD, qw)
            pad = jnp.zeros((128, 2 * kvw), f32)
            xl[rows, :] = turn_rows(jnp.concatenate([x, pad], axis=1), rows, -1.0).astype(low)

        per_tile(tiles, 128, query_rows)
        for p in range(parts):

            def put(r, x):
                at = pl.ds(p * piece + r, 16)
                get(o_out)[at, :] = (res[at, :] + x).astype(low)

            rs.total(p, put)
        ready = get(h_ready)
        for i in range(1, nt):
            pl.semaphore_signal(ready, inc=1, device_id={"tp": lax.rem(t + i, nt)}, device_id_type=MESH)

        def put_down(cols, x):
            get(o_dd)[cols, :] = x.T

        def put_gate(cols, x):
            get(o_dg)[:, cols] = x

        def put_up(cols, x):
            get(o_du)[:, cols] = x

        def put_query(cols, x):
            get(o_da)[:, cols] = x

        def put_key(cols, x):
            get(o_db)[:, cols] = x

        gs.collect(0, put_down)
        gs.collect(1, put_gate)
        gs.collect(2, put_up)
        weight_grads(3)
        for i in (1, 2):

            @pl.when(d + i < nd)
            def _():
                for c in behind(i):
                    c.wait_recv()

        near1, near2 = d + 1 < nd, d + 2 < nd

        def kv_total(r):
            rows = pl.ds(r, 128)
            x = kv_rows(2, r)
            a = col_decode(kvr.at[0, rows], ksr.at[0, r // 128], slice(None))
            b = col_decode(kvr.at[1, rows], ksr.at[1, r // 128], slice(None))
            x = x + jnp.where(near1, a, 0.0) + jnp.where(near2, b, 0.0)
            pad = jnp.zeros((128, qw), f32)
            x = turn_rows(jnp.concatenate([pad, x], axis=1), rows, -1.0)
            xl[rows, qw:] = x[:, qw:].astype(low)

        per_tile(tiles, 128, kv_total)

        def hidden_rows(j):
            for c in range(0, width, 512):
                part[rows_of(j), c : c + 512] = nt_dot(xl[rows_of(j), :], wa_ref[c : c + 512, :qkvw])

        rs.finish()
        pl.semaphore_wait(ready, nt - 1)
        rs.send(0, hidden_rows)
        rs.send(1)
        hidden_rows(t)
        weight_grads(4)

        for p in range(parts):

            def put(r, x):
                at = pl.ds(p * piece + r, 16)
                y = tok[at, :].astype(f32)
                inverse = inverse_rms(y)
                normed = y * inverse
                mine[:, :width] += jnp.sum(x * normed, axis=0, keepdims=True)
                e = x * g1[...]
                e = inverse * (e - normed * jnp.mean(e * normed, axis=-1, keepdims=True))
                get(o_tg)[at, :] = rg[at, :] + e

            rs.total(p, put)
        full.run(get)
        gs.collect(3, put_query)
        gs.collect(4, put_key)
        for x in (ag1, ag2, ag3, ag4, rs, wa, wg, wu, wd, gs):
            x.finish()
        for i in (2, 1):
            when(d + i < nd, lambda: ahead(i).wait_send())

            @pl.when(d >= i)
            def _():
                for c in behind(i):
                    c.wait_send()

    st.body(fn)
    return st.run()


def rope_tables(position_ids, head_size):
    half_size = head_size // 2
    inverse = rope_base ** (-(jnp.arange(half_size, dtype=jnp.float32) * 2.0 / head_size))
    angles = position_ids.astype(jnp.float32)[:, None] * inverse[None, :]
    return (jnp.cos(angles), jnp.sin(angles))


def dot(a, b):
    return jnp.dot(a, b, preferred_element_type=jnp.float32)


def finished(output, tokens_grad, down_sum, gate_sum, up_sum, query_sum, key_sum):
    shard, qw, kvw = query_sum.shape[0], query_sum.shape[1] // 2, key_sum.shape[1] // 2

    def columns(x, at, n):
        base = at // 128 * 128
        slab = x[:, base : base + -(-(at - base + n) // 128) * 128]
        if slab.shape[1] % 128:
            slab = jnp.concatenate([slab, jnp.zeros((shard, -slab.shape[1] % 128), slab.dtype)], axis=1)
        if at > base:
            slab = pltpu.roll(slab, slab.shape[1] - (at - base), 1)
        return slab[:, :n]

    def kernel(*refs):
        (*same, qs, ks), outs = refs[:7], refs[7:]
        for src, dst in zip(same, outs):
            dst[...] = src[...]
        q, k, v, o = outs[5:]
        q[...] = qs[:, :qw]
        o[...] = columns(qs, qw, qw).T
        k[...] = ks[:, :kvw]
        v[...] = columns(ks, kvw, kvw)

    like = [output, tokens_grad, down_sum, gate_sum, up_sum]
    shapes = [(x.shape, x.dtype) for x in like]
    shapes += [((shard, qw), jnp.float32), ((shard, kvw), jnp.float32), ((shard, kvw), jnp.float32), ((qw, shard), jnp.float32)]
    return pl.pallas_call(
        kernel,
        out_shape=[jax.ShapeDtypeStruct(*x) for x in shapes],
        in_specs=[pl.BlockSpec(memory_space=VMEM)] * 7,
        out_specs=[pl.BlockSpec(memory_space=VMEM)] * 9,
        compiler_params=pltpu.CompilerParams(vmem_limit_bytes=66_000_000),
        name="finish",
    )(*like, query_sum, key_sum)


def on_device(
    nd, nt, tokens, positions, attn_gain, w_query, w_key, w_value, w_out, ffn_gain, w_gate, w_up, w_down, out_grad
):
    span = tokens.shape[0] * nt
    width = tokens.shape[1]
    heads = (w_query.shape[1] // HD, w_key.shape[1] // HD)
    qw, kvw = w_query.shape[1], w_key.shape[1]
    w_attn = jnp.concatenate([w_query, w_key, w_value, w_out.T], axis=1)
    w_down_t = w_down.T
    cosine, sine = rope_tables(positions, HD)
    cosine = jnp.tile(cosine, (1, 2 * heads[0]))
    sine = jnp.tile(jnp.concatenate([-sine, sine], axis=1), (1, heads[0]))
    begin = (2 * span + jnp.arange(span, dtype=jnp.int32) - positions)[None]
    output, tokens_grad, gains, down_sum, gate_sum, up_sum, query_sum, key_sum = layer(
        nd, nt, tokens, attn_gain, ffn_gain, out_grad, begin, cosine, sine, w_attn, w_gate, w_up, w_down_t, heads
    )
    output, tokens_grad, down_sum, gate_sum, up_sum, wq, wk, wv, wo = finished(
        output, tokens_grad, down_sum, gate_sum, up_sum, query_sum, key_sum
    )
    return (output, tokens_grad, gains[0, :width], wq, wk, wv, wo, gains[0, width:], gate_sum, up_sum, down_sum)


def solution(mesh):
    return jax.shard_map(
        functools.partial(on_device, mesh.shape["dp"], mesh.shape["tp"]),
        mesh=mesh,
        in_specs=(
            P(("dp", "tp"), None),
            P("dp"),
            P(),
            P("dp", "tp"),
            P("dp", "tp"),
            P("dp", "tp"),
            P("tp", "dp"),
            P(),
            P("dp", "tp"),
            P("dp", "tp"),
            P("tp", "dp"),
            P(("dp", "tp"), None),
        ),
        out_specs=(
            P(("dp", "tp"), None),
            P(("dp", "tp"), None),
            P(),
            P("dp", "tp"),
            P("dp", "tp"),
            P("dp", "tp"),
            P("tp", "dp"),
            P(),
            P("dp", "tp"),
            P("dp", "tp"),
            P("tp", "dp"),
        ),
        check_vma=False,
    )
```

```python
import functools
import math

import jax
import jax.numpy as jnp
from jax import lax
from jax.experimental import pallas as pl
from jax.experimental.pallas import tpu as pltpu
from jax.sharding import PartitionSpec as P

HD = 96
norm_eps = 1e-05
rope_base = 100000.0
masked_score = -1e30

MESH = pl.DeviceIdType.MESH
VMEM = pltpu.VMEM
DMA = pltpu.SemaphoreType.DMA
LEVELS = 32000.0


class Stage:
    def __init__(self, name, cid, nd, nt):
        self.name, self.cid, self.nd, self.nt = name, cid, nd, nt
        self.ins, self.outs, self.scr, self.tasks, self.links = [], [], [], [], set()

    def inp(self, x, space=VMEM):
        self.ins.append((x, space))
        return ("i", len(self.ins) - 1)

    def out(self, shape, dtype, space=VMEM):
        self.outs.append((shape, dtype, space))
        return ("o", len(self.outs) - 1)

    def scratch(self, spec):
        self.scr.append(spec)
        return ("s", len(self.scr) - 1)

    def task(self, links, gen):
        self.links |= set(links)
        self.tasks.append(gen)

    def _barrier(self):
        d, t = lax.axis_index("dp"), lax.axis_index("tp")
        nd, nt = self.nd, self.nt
        sem = pltpu.get_barrier_semaphore()
        count = 0

        def greet(ok, where):
            if ok is True:
                pl.semaphore_signal(sem, inc=1, device_id=where, device_id_type=MESH)
                return 1

            @pl.when(ok)
            def _():
                pl.semaphore_signal(sem, inc=1, device_id=where, device_id_type=MESH)

            return ok.astype(jnp.int32)

        if "line" in self.links:
            count += greet(t > 0, {"tp": t - 1})
            count += greet(t < nt - 1, {"tp": t + 1})
        if "chips" in self.links:
            for i in range(1, nd // 2):
                count += greet(True, {"dp": lax.rem(d + 2 * i, nd)})
        if "twin" in self.links:
            count += greet(True, {"dp": d + 1 - 2 * lax.rem(d, 2)})
        if "near" in self.links:
            for i in (1, 2):
                count += greet(d >= i, {"dp": d - i})
                count += greet(d < nd - i, {"dp": d + i})
        if "tp" in self.links:
            for i in range(1, nt):
                count += greet(True, {"tp": lax.rem(t + i, nt)})
        if "dp" in self.links:
            for i in range(1, nd):
                count += greet(True, {"dp": lax.rem(d + i, nd)})
        pl.semaphore_wait(sem, count)

    def run(self):
        n_in, n_out = len(self.ins), len(self.outs)

        def kernel(*refs):
            def get(h):
                kind, i = h
                return refs[i + {"i": 0, "o": n_in, "s": n_in + n_out}[kind]]

            self._barrier()
            live = [g(get) for g in self.tasks]
            while live:
                still = []
                for g in live:
                    try:
                        next(g)
                        still.append(g)
                    except StopIteration:
                        pass
                live = still

        return pl.pallas_call(
            kernel,
            out_shape=[jax.ShapeDtypeStruct(s, t) for s, t, _ in self.outs],
            in_specs=[pl.BlockSpec(memory_space=sp) for _, sp in self.ins],
            out_specs=[pl.BlockSpec(memory_space=sp) for _, _, sp in self.outs],
            scratch_shapes=self.scr,
            compiler_params=pltpu.CompilerParams(
                collective_id=self.cid, has_side_effects=True, vmem_limit_bytes=67_000_000
            ),
            name=self.name,
        )(*[x for x, _ in self.ins])


def remote(src, dst, send, recv, where):
    return pltpu.make_async_remote_copy(
        src_ref=src, dst_ref=dst, send_sem=send, recv_sem=recv, device_id=where, device_id_type=MESH
    )


def when(ok, fn):
    if ok is True:
        fn()
    elif ok is not False:
        pl.when(ok)(fn)


def over_cols(width, fn):
    def body(c, _):
        fn(pl.ds(pl.multiple_of(c * 128, 128), 128))
        return 0

    lax.fori_loop(0, width // 128, body, 0)
    if width % 128:
        fn(pl.ds(width // 128 * 128, width % 128))


def row_encode(read, code, scale, rows):
    step = 16

    def body(i, held):
        r = pl.multiple_of(i * step, step)
        x = read(r, step)
        top = jnp.max(jnp.abs(x), axis=-1, keepdims=True)
        code[pl.ds(r, step), :] = jnp.round(x * (LEVELS / jnp.maximum(top, 1e-30))).astype(jnp.int32).astype(jnp.int16)
        lane = lax.broadcasted_iota(jnp.int32, (step, 128), 1)
        row = lax.broadcasted_iota(jnp.int32, (step, 128), 0) + r
        mine = jnp.sum(jnp.where(lane == row, jnp.maximum(top, 1e-30) * (1.0 / LEVELS), 0.0), axis=0, keepdims=True)
        return held + jnp.broadcast_to(mine, (8, 128))

    scale[...] = lax.fori_loop(0, rows // step, body, jnp.zeros((8, 128), jnp.float32))


def row_decode(code, scale, r, step):
    lane = lax.broadcasted_iota(jnp.int32, (step, 128), 1)
    row = lax.broadcasted_iota(jnp.int32, (step, 128), 0) + r
    col = jnp.sum(jnp.where(lane == row, jnp.broadcast_to(scale[0:1, :], (step, 128)), 0.0), axis=-1, keepdims=True)
    return code[pl.ds(r, step), :].astype(jnp.int32).astype(jnp.float32) * col


def col_encode(x, code, scale, cols):
    top = jnp.maximum(jnp.max(jnp.abs(x), axis=0, keepdims=True), 1e-30)
    code[:, cols] = jnp.round(x * (LEVELS / top)).astype(jnp.int32).astype(jnp.int16)
    scale[:, cols] = top * (1.0 / LEVELS)


def col_decode(code, scale, cols):
    return code[:, cols].astype(jnp.int32).astype(jnp.float32) * scale[:, cols]


class LineGather:
    def __init__(self, st, full, rows, parts):
        self.st, self.full, self.rows, self.parts = st, full, rows, parts
        self.hs = st.scratch(DMA((2, st.nt, parts)))
        self.hr = st.scratch(DMA((2, st.nt, parts)))
        st.links.add("line")

    def bind(self, get):
        self.ref, self.ss, self.rs = get(self.full), get(self.hs), get(self.hr)
        self.t = lax.axis_index("tp")
        return self

    def piece(self, owner, p):
        chunk = self.rows // self.parts
        return self.ref.at[pl.ds(pl.multiple_of(owner * self.rows + p * chunk, chunk), chunk)]

    def hop(self, owner, k, s, p, where):
        at = self.piece(owner, p)
        return remote(at, at, self.ss.at[k, s, p], self.rs.at[k, s, p], {"tp": where})

    def _send(self, s, p, k, way):
        nt, t = self.st.nt, self.t
        owner, where = t - s * way, t + way
        ok = (owner >= 0) & (owner < nt) & (where >= 0) & (where < nt)
        when(ok, lambda: self.hop(owner, k, s, p, where).start())

    def start(self, p):
        for k, way in enumerate((1, -1)):
            self._send(0, p, k, way)

    def arrive(self, s, p):
        nt, t = self.st.nt, self.t
        for k, way in enumerate((1, -1)):
            owner = t - way * (s + 1)
            ok = (owner >= 0) & (owner < nt)
            when(ok, lambda: self.hop(owner, k, s, p, t).wait_recv())
            if s < nt - 2:
                self._send(s + 1, p, k, way)

    def arrive_at(self, v):
        nt, t = self.st.nt, self.t
        s, p = v // self.parts, lax.rem(v, self.parts)
        for k, way in enumerate((1, -1)):
            owner = t - way * (s + 1)
            ok = (owner >= 0) & (owner < nt) & (s < nt - 1)
            where = t + way

            @pl.when(ok)
            def _():
                self.hop(owner, k, s, p, t).wait_recv()
                when((where >= 0) & (where < nt) & (s < nt - 2), lambda: self.hop(owner, k, s + 1, p, where).start())

    def arrivals(self):
        return [
            functools.partial(self.arrive, s, p) for s in range(self.st.nt - 1) for p in range(self.parts)
        ]

    def finish(self):
        nt, t = self.st.nt, self.t
        for s in range(nt - 1):
            for p in range(self.parts):
                for k, way in enumerate((1, -1)):
                    owner, where = t - s * way, t + way
                    ok = (owner >= 0) & (owner < nt) & (where >= 0) & (where < nt)
                    when(ok, lambda: self.hop(owner, k, s, p, where).wait_send())


class LineSum:
    def __init__(self, st, part, rows, width, parts):
        self.st, self.part, self.rows, self.width, self.parts = st, part, rows, width, parts
        nt = st.nt
        self.chunk = rows // parts
        shape = (nt, parts, self.chunk, width)
        self.hc = [st.scratch(VMEM(shape, jnp.int16)) for _ in range(2)]
        self.hk = [st.scratch(VMEM(shape[:2] + (8, 128), jnp.float32)) for _ in range(2)]
        self.hd = [st.scratch(DMA((2, nt, parts))) for _ in range(2)]
        st.links.add("tp")

    def bind(self, get):
        self.x = get(self.part)
        (self.cs, self.cr), (self.sc, self.sr), (self.ss, self.rs) = (
            [get(h) for h in hs] for hs in (self.hc, self.hk, self.hd)
        )
        self.t = lax.axis_index("tp")
        return self

    def far(self, i, j):
        return (jnp.abs(i - j) == 3) if self.st.nt == 4 else (i != i)

    def sends(self, j, p):
        t = self.t
        where = jnp.where(self.far(t, j), jnp.where(j > t, t + 1, t - 1), j)
        slot = jnp.where(self.far(t, j), where, t)
        return (
            remote(self.cs.at[j, p], self.cr.at[slot, p], self.ss.at[0, j, p], self.rs.at[0, slot, p], {"tp": where}),
            remote(self.sc.at[j, p], self.sr.at[slot, p], self.ss.at[1, j, p], self.rs.at[1, slot, p], {"tp": where}),
        )

    def arrival(self, slot, p):
        for k, (x, y) in enumerate(((self.cs, self.cr), (self.sc, self.sr))):
            remote(x.at[slot, p], y.at[slot, p], self.ss.at[k, slot, p], self.rs.at[k, slot, p], {"tp": self.t}).wait_recv()

    def dest(self, o):
        nt, t = self.st.nt, self.t
        if nt != 4:
            return lax.rem(t + 1 + o, nt)
        inner = jnp.where(o == 2, 2, 1 + 2 * o)
        x = jnp.where((t == 0) | (t == nt - 1), 3 - o, inner)
        lo = lax.rem(lax.rem(t, 2) + lax.rem(x, 2), 2)
        return 2 * lax.rem(t // 2 + x // 2, 2) + lo

    def _rows(self, base, r, n):
        return self.x[pl.ds(pl.multiple_of(base + r, n), n), :]

    def send(self, p, produce=None, beside=None):
        nt, t, chunk = self.st.nt, self.t, self.chunk

        def one(o, _):
            j = self.dest(o)
            if produce is not None:
                produce(j)
            base = j * self.rows + p * chunk
            if nt == 4:
                relay = ((t == 1) & (j == 3)) | ((t == 2) & (j == 0))

                @pl.when(relay)
                def _():
                    self.arrival(t, p)
                    row_encode(
                        lambda r, n: self._rows(base, r, n) + row_decode(self.cr.at[t, p], self.sr.at[t, p], r, n),
                        self.cs.at[j, p],
                        self.sc.at[j, p],
                        chunk,
                    )

                plain = jnp.logical_not(relay)
            else:
                plain = True
            when(plain, lambda: row_encode(lambda r, n: self._rows(base, r, n), self.cs.at[j, p], self.sc.at[j, p], chunk))
            for c in self.sends(j, p):
                c.start()
            if beside is not None:
                beside(o)
            return 0

        lax.fori_loop(0, nt - 1, one, 0)

    def total(self, p, put):
        nt, t, chunk = self.st.nt, self.t, self.chunk
        sources = [lax.rem(t + 1 + i, nt) for i in range(nt - 1)]
        for i in sources:
            pl.when(jnp.logical_not(self.far(i, t)))(lambda: self.arrival(i, p))
        base = t * self.rows + p * chunk

        def body(n, _):
            r = pl.multiple_of(n * 16, 16)
            x = self._rows(base, r, 16)
            for i in sources:
                y = row_decode(self.cr.at[i, p], self.sr.at[i, p], r, 16)
                x = x + (jnp.where(self.far(i, t), 0.0, y) if nt == 4 else y)
            put(r, x)
            return 0

        lax.fori_loop(0, chunk // 16, body, 0)

    def finish(self):
        def one(o, _):
            for p in range(self.parts):
                for c in self.sends(self.dest(o), p):
                    c.wait_send()
            return 0

        lax.fori_loop(0, self.st.nt - 1, one, 0)


class ChipGather:
    def __init__(self, st, w, full, rows):
        self.st, self.w, self.full, self.rows = st, w, full, rows
        self.square = st.nd == 8
        self.hops = 4 if self.square else st.nd // 2 - 1
        self.hs, self.hr = (st.scratch(DMA((2 * self.hops + 1,))) for _ in range(2))
        self.hl = st.scratch(DMA((1,)))
        st.links |= {"chips", "twin"}

    def bind(self, get):
        self.x, self.o, self.ss, self.rs, ls = (get(h) for h in (self.w, self.full, self.hs, self.hr, self.hl))
        nd, rows, n = self.st.nd, self.rows, self.hops
        d = lax.axis_index("dp")
        core, chip = lax.rem(d, 2), d // 2
        twin = {"dp": d + 1 - 2 * core}

        def at(i, part=None):
            if part is None:
                return self.o.at[pl.ds(pl.multiple_of(i * rows, rows), rows)]
            return self.o.at[pl.ds(pl.multiple_of(i * rows + part * (rows // 2), rows // 2), rows // 2)]

        beside = [chip + 1 - 2 * lax.rem(chip, 2), lax.rem(chip + 2, 4)]
        near = [2 * c + core for c in beside]
        diagonal = 2 * lax.rem(beside[0] + 2, 4) + core

        def came(i):
            if not self.square:
                return at(lax.rem(d - 2 * i - 2 + nd, nd))
            return at(near[i]) if i < 2 else at(diagonal, i - 2)

        def hop(i):
            if not self.square:
                src, dst, where = self.x, at(d), lax.rem(d + 2 * i + 2, nd)
            elif i < 2:
                src, dst, where = self.x, at(d), near[i]
            else:
                src = dst = at(near[i - 2], i - 2)
                where = near[3 - i]
            return remote(src, dst, self.ss.at[i], self.rs.at[i], {"dp": where})

        def landed(i):
            return remote(came(i), came(i), self.ss.at[i], self.rs.at[i], twin)

        def give(i):
            src, dst = (self.x, at(d)) if i == 0 else (came(i - 1), came(i - 1))
            return remote(src, dst, self.ss.at[n + i], self.rs.at[n + i], twin)

        self.own = lambda: pltpu.make_async_copy(self.x, at(d), ls.at[0])
        self.hop, self.landed, self.give = hop, landed, give
        return self

    def start(self):
        for i in range(2 if self.square else self.hops):
            self.hop(i).start()
        self.give(0).start()
        self.own().start()

    def forward(self, i):
        self.landed(i).wait_recv()
        if self.square and i < 2:
            self.hop(i + 2).start()
        self.give(i + 1).start()

    def forwards(self):
        return [functools.partial(self.forward, i) for i in range(self.hops)]

    def arrived(self):
        for i in range(self.hops + 1):
            self.give(i).wait_recv()
        self.own().wait()

    def finish(self):
        for i in range(self.hops + 1):
            self.give(i).wait_send()
        for i in range(self.hops):
            self.hop(i).wait_send()


class GradScatter:
    def __init__(self, st, shard, widths, sums):
        nc = self.nc = st.nd // 2
        self.st, self.shard, self.widths = st, shard, widths
        self.m = math.lcm(2 * shard, 128) // (2 * shard)
        self.chunks = nc // self.m
        self.padded = [-(-w // 128) * 128 for w in widths]
        wide = max(self.padded)
        self.hg = st.scratch(VMEM((2, 2 * self.m * shard, wide), jnp.float32))
        self.ht = st.scratch(VMEM((2, self.m, shard, wide), jnp.float32))
        self.slots = self.chunks - (self.m == 1)
        self.hs = st.scratch(VMEM((self.slots, self.m, shard, wide), jnp.int16))
        self.hk = st.scratch(VMEM((self.slots, self.m, 1, wide), jnp.float32))
        self.hcr = [st.scratch(VMEM((nc - 1, shard, w), jnp.int16)) for w in self.padded]
        self.hkr = [st.scratch(VMEM((nc - 1, 1, w), jnp.float32)) for w in self.padded]
        self.ha = sums
        self.hgs = [st.scratch(DMA((2, self.m))) for _ in range(2)]
        self.hss = st.scratch(DMA((2, self.slots, self.m)))
        self.hsr = st.scratch(DMA((len(widths), 2, nc - 1)))
        self.hf = st.scratch(pltpu.SemaphoreType.REGULAR)
        st.links |= {"chips", "twin"}

    def bind(self, get):
        self.g, self.t, self.cs, self.sc, self.ss, self.sr, self.free = (
            get(h) for h in (self.hg, self.ht, self.hs, self.hk, self.hss, self.hsr, self.hf)
        )
        self.cr, self.kr, self.acc = ([get(h) for h in hs] for hs in (self.hcr, self.hkr, self.ha))
        self.gs, self.gr = (get(h) for h in self.hgs)
        d = self.d = lax.axis_index("dp")
        self.core, self.chip = lax.rem(d, 2), d // 2
        self.twin = {"dp": d + 1 - 2 * self.core}
        return self

    def chunk(self, i):
        return lax.rem(self.chip // self.m + 1 + i, self.chunks)

    def half(self, e, core):
        return pl.ds(pl.multiple_of((2 * e + core) * self.shard, self.shard), self.shard)

    def gift(self, a, r, e):
        cols = pl.ds(0, self.padded[a])
        return remote(
            self.g.at[r, self.half(e, 1 - self.core), cols], self.t.at[r, e, :, cols], self.gs.at[r, e], self.gr.at[r, e],
            self.twin,
        )

    def sums(self, a, i, e, dest):
        cols, nc = pl.ds(0, self.padded[a]), self.nc
        slot = jnp.maximum(lax.rem(dest - self.chip + nc, nc) - 1, 0)
        where = {"dp": 2 * dest + self.core}
        return (
            remote(self.cs.at[i, e, :, cols], self.cr[a].at[slot], self.ss.at[0, i, e], self.sr.at[a, 0, slot], where),
            remote(self.sc.at[i, e, :, cols], self.kr[a].at[slot], self.ss.at[1, i, e], self.sr.at[a, 1, slot], where),
        )

    def compute(self, a, i, pieces):
        n = a * self.chunks + i
        r = lax.rem(n, 2)
        rows = 2 * self.m * self.shard

        @pl.when(n >= 2)
        def _():
            for e in range(self.m):
                self.gift(a, r, e).wait_send() if a == 0 else self._sent(a, i, r, e)
            pl.semaphore_wait(self.free, 1)

        cols = pl.ds(pl.multiple_of(self.chunk(i) * rows, 128), rows)
        at = 0
        for x, y in pieces:
            z = y()
            self.g[r, :, at : at + z.shape[1]] = tn_dot(x[:, cols], z)
            at += z.shape[1]
        for e in range(self.m):
            self.gift(a, r, e).start()

    def _sent(self, a, i, r, e):
        pl.when(i >= 2)(lambda: self.gift(a, r, e).wait_send())
        pl.when(i < 2)(lambda: self.gift(a - 1, r, e).wait_send())

    def combine(self, a, i):
        n = a * self.chunks + i
        r = lax.rem(n, 2)
        for e in range(self.m):
            self.gift(a, r, e).wait_recv()
            dest = self.chunk(i) * self.m + e
            away = dest != self.chip
            own = self.half(e, self.core)

            @pl.when(away)
            def _():
                if a:
                    for c in self.sums(a - 1, i, e, dest):
                        c.wait_send()
                over_cols(
                    self.widths[a],
                    lambda cols: col_encode(
                        self.g[r, own, cols] + self.t[r, e, :, cols], self.cs.at[i, e], self.sc.at[i, e], cols
                    ),
                )
                for c in self.sums(a, i, e, dest):
                    c.start()

            @pl.when(jnp.logical_not(away))
            def _():
                over_cols(self.widths[a], lambda cols: self._keep(a, r, e, own, cols))

        @pl.when(n + 2 < len(self.widths) * self.chunks)
        def _():
            pl.semaphore_signal(self.free, inc=1, device_id=self.twin, device_id_type=MESH)

    def _keep(self, a, r, e, own, cols):
        self.acc[a][:, cols] = self.g[r, own, cols] + self.t[r, e, :, cols]

    def slot(self, a, w, pieces):
        pl.when(w < self.chunks)(lambda: self.compute(a, w, pieces))
        pl.when((w >= 1) & (w <= self.chunks))(lambda: self.combine(a, w - 1))

    def collect(self, a, put):
        n = self.nc - 1
        for i in range(n):
            for c in self.sums(a, 0, 0, lax.rem(self.chip + 1 + i, self.nc)):
                c.wait_recv()

        def tile(cols):
            x = self.acc[a][:, cols]
            for i in range(n):
                x = x + col_decode(self.cr[a].at[i], self.kr[a].at[i], cols)
            put(cols, x)

        over_cols(self.widths[a], tile)

    def finish(self):
        a = len(self.widths) - 1
        for i in range(self.chunks):
            for e in range(self.m):
                if i >= self.chunks - 2:
                    self.gift(a, (a * self.chunks + i) % 2, e).wait_send()
                if i < self.slots:
                    dest = self.chunk(i) * self.m + e

                    @pl.when(dest != self.chip)
                    def _():
                        for c in self.sums(a, i, e, dest):
                            c.wait_send()


class FullSum:
    def __init__(self, st, x, out, shape):
        self.st, self.x, self.out = st, x, out
        self.ha = st.scratch(VMEM((st.nt,) + shape, jnp.float32))
        self.hm = st.scratch(VMEM(shape, jnp.float32))
        self.hb = st.scratch(VMEM((st.nd,) + shape, jnp.float32))
        self.hs = st.scratch(DMA((2, max(st.nd, st.nt))))
        self.hr = st.scratch(DMA((2, max(st.nd, st.nt))))
        st.links |= {"tp", "dp"}

    def run(self, get):
        nd, nt = self.st.nd, self.st.nt
        x, o, a, m, b, ss, rs = (get(h) for h in (self.x, self.out, self.ha, self.hm, self.hb, self.hs, self.hr))
        for k, (axis, n, src, got, dst) in enumerate((("tp", nt, x, a, m), ("dp", nd, m, b, o))):
            me = lax.axis_index(axis)
            cs = [
                remote(src, got.at[me], ss.at[k, i], rs.at[k, i], {axis: lax.rem(me + i, n)}) for i in range(1, n)
            ]
            for c in cs:
                c.start()
            got[me] = src[...]
            for c in cs:
                c.wait()
            total = got[0]
            for i in range(1, n):
                total = total + got[i]
            dst[...] = total


def lane_take(x, offset):
    base = offset // 128 * 128
    wide = min(256, x.shape[-1] - base)
    slab = x[:, base : base + wide]
    if wide % 128:
        slab = jnp.concatenate([slab, jnp.zeros((x.shape[0], -wide % 128), x.dtype)], axis=1)
        wide = slab.shape[-1]
    if offset > base:
        slab = pltpu.roll(slab, wide - (offset - base), 1)
    slab = slab[:, :128]
    return jnp.where(lax.broadcasted_iota(jnp.int32, slab.shape, 1) < HD, slab, 0.0)


def lane_place(x, offset, width):
    base = offset // 128 * 128
    wide = min(256, width - base)
    slab = x if wide == 128 else jnp.concatenate([x, jnp.zeros_like(x)], axis=1)
    if offset > base:
        slab = pltpu.roll(slab, offset - base, 1)
    slab = slab[:, :wide]
    pieces = []
    if base:
        pieces.append(jnp.zeros((x.shape[0], base), x.dtype))
    pieces.append(slab)
    if base + wide < width:
        pieces.append(jnp.zeros((x.shape[0], width - base - wide), x.dtype))
    return jnp.concatenate(pieces, axis=1) if len(pieces) > 1 else slab


def turned(u, cosine, sine):
    wide = u.shape[-1]
    lane = lax.rem(lax.broadcasted_iota(jnp.int32, u.shape, 1), HD)
    swap = jnp.where(lane < HD // 2, pltpu.roll(u, wide - HD // 2, 1), pltpu.roll(u, HD // 2, 1))
    return u * cosine + swap * sine


def nt_dot(a, b):
    return lax.dot_general(a, b, (((1,), (1,)), ((), ())), preferred_element_type=jnp.float32)


def per_tile(count, size, fn):
    def body(i, _):
        fn(pl.multiple_of(i * size, size))
        return 0

    lax.fori_loop(0, count, body, 0)


def in_turn(*lists):
    for i in range(max(len(x) for x in lists)):
        for x in lists:
            if i < len(x):
                x[i]()


class Fused(Stage):
    def body(self, fn):
        self.tasks = [lambda get: iter(fn(get) or ())]


def inverse_rms(x):
    return lax.rsqrt(jnp.mean(x * x, axis=-1, keepdims=True) + norm_eps)


def tn_dot(a, b):
    return lax.dot_general(a, b, (((0,), (0,)), ((), ())), preferred_element_type=jnp.float32)


def across(x, count):
    return jnp.concatenate([x] * count, axis=1) if count > 1 else x


def masked_scores(keys, queries, first, begin, span, group):
    s = nt_dot(keys, queries) * (1.0 / math.sqrt(HD))
    key = lax.broadcasted_iota(jnp.int32, s.shape, 0) + first
    own = lax.rem(lax.broadcasted_iota(jnp.int32, s.shape, 1), 128) + (first + 2 * span)
    return s, (key >= across(begin, group)) & (key <= own)


def layer(
    nd, nt, tokens, attn_gain, ffn_gain, out_grad, begin, cosine, sine, w_attn, w_gate, w_up, w_down_t, heads
):
    st = Fused("layer", 1, nd, nt)
    low, f32 = jnp.bfloat16, jnp.float32
    own, width = tokens.shape
    span = own * nt
    shard, units = w_gate.shape
    n_q, n_kv = heads
    group = n_q // n_kv
    tiles = span // 128
    qw, kvw = n_q * HD, n_kv * HD
    qkvw = qw + 2 * kvw
    reach = 2 * span + 128
    parts = 2
    piece = own // parts
    scale = 1.0 / math.sqrt(HD)

    h_tok, h_g1, h_g2 = st.inp(tokens), st.inp(attn_gain[None]), st.inp(ffn_gain[None])
    h_og, h_begin = st.inp(out_grad), st.inp(begin)
    h_cos, h_sin = st.inp(cosine), st.inp(sine)
    s_wa, s_wg, s_wu, s_wd = (st.inp(w, pl.ANY) for w in (w_attn, w_gate, w_up, w_down_t))

    o_out = st.out((own, width), low)
    o_tg = st.out((own, width), f32)
    o_gains = st.out((1, 2 * width), f32)
    o_dd, o_dg, o_du = (st.out((shard, units), f32) for _ in range(3))
    o_da, o_db = (st.out((shard, w), f32) for w in (2 * qw, 2 * kvw))

    def room(shape, dtype=f32):
        return st.scratch(VMEM(shape, dtype))

    h_h1, h_h2, h_gr, h_rl = (room((span, width), low) for _ in range(4))
    h_wa = room((width, qkvw + qw), low)
    h_wg, h_wu, h_wd = (room((width, units), low) for _ in range(3))
    h_q, h_dc, h_ch = (room((n_kv, tiles, group * 128, 128), low) for _ in range(3))
    h_k, h_v = (room((n_kv, 3 * span, 128), low) for _ in range(2))
    h_vt = room((n_kv, 128, 3 * span), low)
    h_win = room((3, span, 2 * kvw), low)
    h_ctx = room((span, qw), low)
    h_lse, h_delta = (room((n_kv, tiles, 1, group * 128)) for _ in range(2))
    h_res, h_rg = (room((own, width)) for _ in range(2))
    h_part = room((span, width))
    h_ia, h_gl, h_ul = (room((span, units), low) for _ in range(3))
    h_dq = room((n_kv, tiles, group * 128, 128))
    h_dk, h_dv = (room((n_kv, 3 * span, 128)) for _ in range(2))
    h_kvs, h_kvr = (room((2, span, 2 * kvw), jnp.int16) for _ in range(2))
    h_kss, h_ksr = (room((2, tiles, 1, 2 * kvw)) for _ in range(2))
    h_mine = room((1, 2 * width))
    h_fs, h_fr = (st.scratch(DMA((2,))) for _ in range(2))
    h_bs, h_br = (st.scratch(DMA((2, 2))) for _ in range(2))
    h_ready = st.scratch(pltpu.SemaphoreType.REGULAR)

    ag1 = LineGather(st, h_h1, own, parts)
    ag2 = LineGather(st, h_h2, own, parts)
    ag3 = LineGather(st, h_gr, own, parts)
    ag4 = LineGather(st, h_rl, own, parts)
    rs = LineSum(st, h_part, own, width, parts)
    wa = ChipGather(st, s_wa, h_wa, shard)
    wg = ChipGather(st, s_wg, h_wg, shard)
    wu = ChipGather(st, s_wu, h_wu, shard)
    wd = ChipGather(st, s_wd, h_wd, shard)
    gs = GradScatter(st, shard, (units, units, units, 2 * qw, 2 * kvw), (o_dd, o_dg, o_du, o_da, o_db))
    full = FullSum(st, h_mine, o_gains, (1, 2 * width))
    st.links.add("near")

    def fn(get):
        d, t = lax.axis_index("dp"), lax.axis_index("tp")
        for x in (ag1, ag2, ag3, ag4, rs, wa, wg, wu, wd, gs):
            x.bind(get)
        tok, g1, g2, og, begin_ref, cos_ref, sin_ref = (get(h) for h in (h_tok, h_g1, h_g2, h_og, h_begin, h_cos, h_sin))
        h1, h2, gr, rl = (get(h) for h in (h_h1, h_h2, h_gr, h_rl))
        wa_ref, wg_ref, wu_ref, wd_ref = (get(h) for h in (h_wa, h_wg, h_wu, h_wd))
        q, k, v, vt, win, ctx, ch, lse = (get(h) for h in (h_q, h_k, h_v, h_vt, h_win, h_ctx, h_ch, h_lse))
        dc, delta, dq, dk, dv = (get(h) for h in (h_dc, h_delta, h_dq, h_dk, h_dv))
        res, rg, part, ia, gl, ul, mine = (get(h) for h in (h_res, h_rg, h_part, h_ia, h_gl, h_ul, h_mine))
        xl = ul.at[:, pl.ds(0, qkvw)]
        kvs, kvr, kss, ksr, fs, fr, bs, br = (
            get(h) for h in (h_kvs, h_kvr, h_kss, h_ksr, h_fs, h_fr, h_bs, h_br)
        )

        def own_rows(p, r, n=16):
            return pl.ds(pl.multiple_of(t * own + p * piece + r, n), n)

        def rows_of(j):
            return pl.ds(pl.multiple_of(j * own, own), own)

        wa.start()
        wd.start()
        for p in range(parts):

            def tile(r):
                x = tok[pl.ds(p * piece + r, 16), :].astype(f32)
                h1[own_rows(p, r), :] = (x * inverse_rms(x) * g1[...]).astype(low)

            per_tile(piece // 16, 16, tile)
            ag1.start(p)
        gr[rows_of(t), :] = og[...]
        pass_a, pass_d, pass_g, pass_u = (x.forwards() for x in (wa, wd, wg, wu))
        in_turn(ag1.arrivals(), pass_a[:2] + pass_d[:2] + pass_a[2:])
        for p in range(parts):
            ag3.start(p)
        wa.arrived()

        def turn_rows(x, rows, way):
            cosine, sine = across(cos_ref[rows, :], 2), across(sin_ref[rows, :], 2)
            lane = lax.broadcasted_iota(jnp.int32, x.shape, 1)
            return jnp.where(lane < qw + kvw, turned(x, cosine, way * sine), x)

        def project(r):
            rows = pl.ds(r, 128)
            x = turn_rows(dot(h1[rows, :], wa_ref[:, :qkvw]), rows, 1.0)
            for h in range(n_q):
                q[h // group, r // 128, h % group * 128 : (h % group + 1) * 128, :] = lane_take(x, h * HD).astype(low)
            win[2, rows, :] = x[:, qw:].astype(low)

        per_tile(tiles, 128, project)

        def ahead(i):
            return remote(win.at[2], win.at[2 - i], fs.at[i - 1], fr.at[i - 1], {"dp": d + i})

        for i in (2, 1):
            when(d + i < nd, lambda: ahead(i).start())

        def unpack(b):
            def tile(r):
                x = win[b, pl.ds(r, 128), :].astype(f32)
                at = pl.ds(pl.multiple_of(b * span + r, 128), 128)
                for g in range(n_kv):
                    k[g, at, :] = lane_take(x, g * HD).astype(low)
                    y = lane_take(x, kvw + g * HD)
                    v[g, at, :] = y.astype(low)
                    vt[g, :, at] = y.T.astype(low)

            per_tile(tiles, 128, tile)

        unpack(2)
        for x in pass_d[2:]:
            x()
        for i in (1, 2):

            @pl.when(d < i)
            def _():
                win[2 - i] = jnp.zeros((span, 2 * kvw), low)

            when(d >= i, lambda: ahead(i).wait_recv())
            unpack(2 - i)
        wg.start()
        wu.start()

        def attend(u, _):
            g, i = u // tiles, lax.rem(u, tiles)
            at = pl.multiple_of(i * 128, 128)
            keys = pl.ds(at, reach)
            s, seen = masked_scores(k[g, keys, :], q[g, i], at, begin_ref[:, pl.ds(at, 128)], span, group)
            s = jnp.where(seen, s, masked_score)
            top = jnp.max(s, axis=0, keepdims=True)
            e = jnp.exp(s - top)
            total = jnp.sum(e, axis=0, keepdims=True)
            p = (e * (1.0 / total)).astype(low)
            lse[g, i] = top + jnp.log(total)
            ch[g, i] = dot(vt[g, :, keys], p).T.astype(low)
            return 0

        half = max(1, n_kv * tiles // 2)
        arrive3 = ag3.arrivals()
        lax.fori_loop(0, half, attend, 0)
        cut = len(arrive3) // 2
        in_turn(arrive3[:cut], pass_g[:2])
        lax.fori_loop(half, n_kv * tiles, attend, 0)
        in_turn(arrive3[cut:], pass_u[:2])

        def pack(r):
            x = 0.0
            for h in range(n_q):
                at = h % group * 128
                x = x + lane_place(ch[h // group, r // 128, at : at + 128, :].astype(f32), h * HD, qw)
            ctx[pl.ds(r, 128), :] = x.astype(low)

        per_tile(tiles, 128, pack)

        def out_rows(j):
            for c in range(0, width, 512):
                part[rows_of(j), c : c + 512] = nt_dot(ctx[rows_of(j), :], wa_ref[c : c + 512, qkvw:])

        rs.send(0, out_rows)
        rs.send(1)
        out_rows(t)
        kt = vt

        def keys_back(r):
            for g in range(n_kv):
                kt[g, :, pl.ds(r, 128)] = k[g, pl.ds(r, 128), :].T

        per_tile(3 * tiles, 128, keys_back)
        in_turn(pass_g[2:], pass_u[2:])

        for p in range(parts):

            def put(r, x):
                at = pl.ds(p * piece + r, 16)
                x = x + tok[at, :].astype(f32)
                res[at, :] = x
                h2[own_rows(p, r), :] = (x * inverse_rms(x) * g2[...]).astype(low)

            rs.total(p, put)
            ag2.start(p)
        wd.arrived()

        def back_act(c):
            part[:, pl.ds(c, 256)] = dot(gr[...], wd_ref[:, pl.ds(c, 256)])

        arrive2 = ag2.arrivals()
        for x in arrive2[:parts]:
            x()
        per_tile(units // 256, 256, back_act)
        for x in arrive2[parts:]:
            x()
        wg.arrived()
        wu.arrived()

        def act(c):
            cols = pl.ds(c, 256)
            gate = dot(h2[...], wg_ref[:, cols])
            up = dot(h2[...], wu_ref[:, cols])
            back = part[:, cols]
            sig = jax.nn.sigmoid(gate)
            ia[:, cols] = (gate * sig * up).astype(low)
            gl[:, cols] = (back * up * (sig * (1.0 + gate * (1.0 - sig)))).astype(low)
            ul[:, cols] = (back * gate * sig).astype(low)

        per_tile(units // 256, 256, act)

        def rows_back(j):
            rows = rows_of(j)
            for c in range(0, width, 512):
                part[rows, c : c + 512] = nt_dot(gl[rows, :], wg_ref[c : c + 512, :]) + nt_dot(
                    ul[rows, :], wu_ref[c : c + 512, :]
                )

        last_slot = gs.chunks + 1
        grads = (
            ((gr, lambda: ia[...]),),
            ((h2, lambda: gl[...]),),
            ((h2, lambda: ul[...]),),
            ((h1, lambda: xl[:, :qw]), (rl, lambda: ctx[...])),
            ((h1, lambda: xl[:, qw:]),),
        )

        def weight_grads(a, first=0):
            def one(w, _):
                gs.slot(a, w, grads[a])
                return 0

            lax.fori_loop(first, last_slot, one, 0)

        rs.finish()
        rs.send(0, rows_back, lambda o: gs.slot(0, o, grads[0]))
        rs.send(1)
        rows_back(t)
        weight_grads(0, nt - 1)
        mine[...] = jnp.zeros_like(mine)

        for p in range(parts):

            def put(r, x):
                at = pl.ds(p * piece + r, 16)
                y = res[at, :]
                inverse = inverse_rms(y)
                normed = y * inverse
                mine[:, width:] += jnp.sum(x * normed, axis=0, keepdims=True)
                e = x * g2[...]
                back = inverse * (e - normed * jnp.mean(e * normed, axis=-1, keepdims=True))
                y = og[at, :].astype(f32) + back
                rg[at, :] = y
                rl[own_rows(p, r), :] = y.astype(low)

            rs.total(p, put)
            ag4.start(p)

        def ffn_rows(r):
            cols = pl.ds(r, 512)
            part[:, cols] = nt_dot(ia[...], wd_ref[cols, :])

        def while_gathered(w, _):
            ag4.arrive_at(w)
            pl.when(w < width // 512)(lambda: ffn_rows(pl.multiple_of(w * 512, 512)))
            gs.slot(1, w, grads[1])
            return 0

        lax.fori_loop(0, max((nt - 1) * parts, last_slot, width // 512), while_gathered, 0)

        def context_back(r):
            x = dot(rl[pl.ds(r, 128), :], wa_ref[:, qkvw:])
            i = r // 128
            for h in range(n_q):
                g, at = h // group, pl.ds(h % group * 128, 128)
                y = lane_take(x, h * HD).astype(low)
                dc[g, i, at, :] = y
                z = y.astype(f32) * ch[g, i, at, :].astype(f32)
                delta[g, i, :, at] = jnp.sum(z.T, axis=0, keepdims=True)

        rs.finish()
        for p in range(parts):
            rs.send(p)
        per_tile(tiles, 128, context_back)
        dk[...] = jnp.zeros_like(dk)
        dv[...] = jnp.zeros_like(dv)
        count = n_kv * tiles

        def attend_back(u, _):
            g, i = u // tiles, lax.rem(u, tiles)
            at = pl.multiple_of(i * 128, 128)
            keys = pl.ds(at, reach)
            qq, dd = q[g, i], dc[g, i]
            s, seen = masked_scores(k[g, keys, :], qq, at, begin_ref[:, pl.ds(at, 128)], span, group)
            p = jnp.where(seen, jnp.exp(s - lse[g, i]), 0.0)
            ds = (p * (nt_dot(v[g, keys, :], dd) - delta[g, i])).astype(low)
            dv[g, keys, :] += dot(p.astype(low), dd)
            dk[g, keys, :] += dot(ds, qq)
            dq[g, i] = dot(kt[g, :, keys], ds).T
            gs.slot(2, u, grads[2])
            return 0

        lax.fori_loop(0, count, attend_back, 0)
        weight_grads(2, count)

        def kv_rows(b, r):
            at = pl.ds(pl.multiple_of(b * span + r, 128), 128)
            x = 0.0
            for g in range(n_kv):
                x = x + lane_place(dk[g, at, :] * scale, g * HD, 2 * kvw)
                x = x + lane_place(dv[g, at, :], kvw + g * HD, 2 * kvw)
            return x

        def behind(i):
            where = {"dp": d - i}
            return (
                remote(kvs.at[i - 1], kvr.at[i - 1], bs.at[0, i - 1], br.at[0, i - 1], where),
                remote(kss.at[i - 1], ksr.at[i - 1], bs.at[1, i - 1], br.at[1, i - 1], where),
            )

        for i in (2, 1):

            @pl.when(d >= i)
            def _():
                def tile(r):
                    at = kvs.at[i - 1, pl.ds(r, 128)]
                    col_encode(kv_rows(2 - i, r), at, kss.at[i - 1, r // 128], slice(None))

                per_tile(tiles, 128, tile)
                for c in behind(i):
                    c.start()

        def query_rows(r):
            rows = pl.ds(r, 128)
            x = 0.0
            for h in range(n_q):
                at = h % group * 128
                x = x + lane_place(dq[h // group, r // 128, at : at + 128, :] * scale, h * HD, qw)
            pad = jnp.zeros((128, 2 * kvw), f32)
            xl[rows, :] = turn_rows(jnp.concatenate([x, pad], axis=1), rows, -1.0).astype(low)

        per_tile(tiles, 128, query_rows)
        for p in range(parts):

            def put(r, x):
                at = pl.ds(p * piece + r, 16)
                get(o_out)[at, :] = (res[at, :] + x).astype(low)

            rs.total(p, put)
        ready = get(h_ready)
        for i in range(1, nt):
            pl.semaphore_signal(ready, inc=1, device_id={"tp": lax.rem(t + i, nt)}, device_id_type=MESH)

        def put_down(cols, x):
            get(o_dd)[:, cols] = x

        def put_gate(cols, x):
            get(o_dg)[:, cols] = x

        def put_up(cols, x):
            get(o_du)[:, cols] = x

        def put_query(cols, x):
            get(o_da)[:, cols] = x

        def put_key(cols, x):
            get(o_db)[:, cols] = x

        gs.collect(0, put_down)
        gs.collect(1, put_gate)
        gs.collect(2, put_up)
        weight_grads(3)
        for i in (1, 2):

            @pl.when(d + i < nd)
            def _():
                for c in behind(i):
                    c.wait_recv()

        near1, near2 = d + 1 < nd, d + 2 < nd

        def kv_total(r):
            rows = pl.ds(r, 128)
            x = kv_rows(2, r)
            a = col_decode(kvr.at[0, rows], ksr.at[0, r // 128], slice(None))
            b = col_decode(kvr.at[1, rows], ksr.at[1, r // 128], slice(None))
            x = x + jnp.where(near1, a, 0.0) + jnp.where(near2, b, 0.0)
            pad = jnp.zeros((128, qw), f32)
            x = turn_rows(jnp.concatenate([pad, x], axis=1), rows, -1.0)
            xl[rows, qw:] = x[:, qw:].astype(low)

        per_tile(tiles, 128, kv_total)

        def hidden_rows(j):
            for c in range(0, width, 512):
                part[rows_of(j), c : c + 512] = nt_dot(xl[rows_of(j), :], wa_ref[c : c + 512, :qkvw])

        rs.finish()
        pl.semaphore_wait(ready, nt - 1)
        rs.send(0, hidden_rows)
        rs.send(1)
        hidden_rows(t)
        weight_grads(4)

        for p in range(parts):

            def put(r, x):
                at = pl.ds(p * piece + r, 16)
                y = tok[at, :].astype(f32)
                inverse = inverse_rms(y)
                normed = y * inverse
                mine[:, :width] += jnp.sum(x * normed, axis=0, keepdims=True)
                e = x * g1[...]
                e = inverse * (e - normed * jnp.mean(e * normed, axis=-1, keepdims=True))
                get(o_tg)[at, :] = rg[at, :] + e

            rs.total(p, put)
        full.run(get)
        gs.collect(3, put_query)
        gs.collect(4, put_key)
        for x in (ag1, ag2, ag3, ag4, rs, wa, wg, wu, wd, gs):
            x.finish()
        for i in (2, 1):
            when(d + i < nd, lambda: ahead(i).wait_send())

            @pl.when(d >= i)
            def _():
                for c in behind(i):
                    c.wait_send()

    st.body(fn)
    return st.run()


def rope_tables(position_ids, head_size):
    half_size = head_size // 2
    inverse = rope_base ** (-(jnp.arange(half_size, dtype=jnp.float32) * 2.0 / head_size))
    angles = position_ids.astype(jnp.float32)[:, None] * inverse[None, :]
    return (jnp.cos(angles), jnp.sin(angles))


def dot(a, b):
    return jnp.dot(a, b, preferred_element_type=jnp.float32)


def finished(output, tokens_grad, down_sum, gate_sum, up_sum, query_sum, key_sum):
    shard, qw, kvw = query_sum.shape[0], query_sum.shape[1] // 2, key_sum.shape[1] // 2

    def columns(x, at, n):
        base = at // 128 * 128
        slab = x[:, base : base + -(-(at - base + n) // 128) * 128]
        if slab.shape[1] % 128:
            slab = jnp.concatenate([slab, jnp.zeros((shard, -slab.shape[1] % 128), slab.dtype)], axis=1)
        if at > base:
            slab = pltpu.roll(slab, slab.shape[1] - (at - base), 1)
        return slab[:, :n]

    def kernel(*refs):
        (*same, qs, ks), outs = refs[:7], refs[7:]
        for src, dst in zip(same, outs):
            dst[...] = src[...]
        q, k, v, o = outs[5:]
        q[...] = qs[:, :qw]
        o[...] = columns(qs, qw, qw)
        k[...] = ks[:, :kvw]
        v[...] = columns(ks, kvw, kvw)

    like = [output, tokens_grad, down_sum, gate_sum, up_sum]
    shapes = [(x.shape, x.dtype) for x in like]
    shapes += [((shard, qw), jnp.float32), ((shard, kvw), jnp.float32), ((shard, kvw), jnp.float32), ((shard, qw), jnp.float32)]
    return pl.pallas_call(
        kernel,
        out_shape=[jax.ShapeDtypeStruct(*x) for x in shapes],
        in_specs=[pl.BlockSpec(memory_space=VMEM)] * 7,
        out_specs=[pl.BlockSpec(memory_space=VMEM)] * 9,
        compiler_params=pltpu.CompilerParams(vmem_limit_bytes=66_000_000),
        name="finish",
    )(*like, query_sum, key_sum)


def on_device(
    nd, nt, tokens, positions, attn_gain, w_query, w_key, w_value, w_out, ffn_gain, w_gate, w_up, w_down, out_grad
):
    span = tokens.shape[0] * nt
    width = tokens.shape[1]
    heads = (w_query.shape[1] // HD, w_key.shape[1] // HD)
    qw, kvw = w_query.shape[1], w_key.shape[1]
    w_attn = jnp.concatenate([w_query, w_key, w_value, w_out.T], axis=1)
    w_down_t = w_down.T
    cosine, sine = rope_tables(positions, HD)
    cosine = jnp.tile(cosine, (1, 2 * heads[0]))
    sine = jnp.tile(jnp.concatenate([-sine, sine], axis=1), (1, heads[0]))
    begin = (2 * span + jnp.arange(span, dtype=jnp.int32) - positions)[None]
    output, tokens_grad, gains, down_sum, gate_sum, up_sum, query_sum, key_sum = layer(
        nd, nt, tokens, attn_gain, ffn_gain, out_grad, begin, cosine, sine, w_attn, w_gate, w_up, w_down_t, heads
    )
    output, tokens_grad, down_sum, gate_sum, up_sum, wq, wk, wv, wo = finished(
        output, tokens_grad, down_sum, gate_sum, up_sum, query_sum, key_sum
    )
    return (output, tokens_grad, gains[0, :width], wq, wk, wv, wo.T, gains[0, width:], gate_sum, up_sum, down_sum.T)


def solution(mesh):
    return jax.shard_map(
        functools.partial(on_device, mesh.shape["dp"], mesh.shape["tp"]),
        mesh=mesh,
        in_specs=(
            P(("dp", "tp"), None),
            P("dp"),
            P(),
            P("dp", "tp"),
            P("dp", "tp"),
            P("dp", "tp"),
            P("tp", "dp"),
            P(),
            P("dp", "tp"),
            P("dp", "tp"),
            P("tp", "dp"),
            P(("dp", "tp"), None),
        ),
        out_specs=(
            P(("dp", "tp"), None),
            P(("dp", "tp"), None),
            P(),
            P("dp", "tp"),
            P("dp", "tp"),
            P("dp", "tp"),
            P("tp", "dp"),
            P(),
            P("dp", "tp"),
            P("dp", "tp"),
            P("tp", "dp"),
        ),
        check_vma=False,
    )
```

```python
import functools
import math

import jax
import jax.numpy as jnp
from jax import lax
from jax.experimental import pallas as pl
from jax.experimental.pallas import tpu as pltpu
from jax.sharding import PartitionSpec as P

HD = 96
norm_eps = 1e-05
rope_base = 100000.0
masked_score = -1e30

MESH = pl.DeviceIdType.MESH
VMEM = pltpu.VMEM
DMA = pltpu.SemaphoreType.DMA
LEVELS = 32000.0


class Stage:
    def __init__(self, name, cid, nd, nt):
        self.name, self.cid, self.nd, self.nt = name, cid, nd, nt
        self.ins, self.outs, self.scr, self.tasks, self.links = [], [], [], [], set()

    def inp(self, x, space=VMEM):
        self.ins.append((x, space))
        return ("i", len(self.ins) - 1)

    def out(self, shape, dtype, space=VMEM):
        self.outs.append((shape, dtype, space))
        return ("o", len(self.outs) - 1)

    def scratch(self, spec):
        self.scr.append(spec)
        return ("s", len(self.scr) - 1)

    def task(self, links, gen):
        self.links |= set(links)
        self.tasks.append(gen)

    def _barrier(self):
        d, t = lax.axis_index("dp"), lax.axis_index("tp")
        nd, nt = self.nd, self.nt
        sem = pltpu.get_barrier_semaphore()
        count = 0

        def greet(ok, where):
            if ok is True:
                pl.semaphore_signal(sem, inc=1, device_id=where, device_id_type=MESH)
                return 1

            @pl.when(ok)
            def _():
                pl.semaphore_signal(sem, inc=1, device_id=where, device_id_type=MESH)

            return ok.astype(jnp.int32)

        if "line" in self.links:
            count += greet(t > 0, {"tp": t - 1})
            count += greet(t < nt - 1, {"tp": t + 1})
        if "chips" in self.links:
            for i in range(1, nd // 2):
                count += greet(True, {"dp": lax.rem(d + 2 * i, nd)})
        if "twin" in self.links:
            count += greet(True, {"dp": d + 1 - 2 * lax.rem(d, 2)})
        if "near" in self.links:
            for i in (1, 2):
                count += greet(d >= i, {"dp": d - i})
                count += greet(d < nd - i, {"dp": d + i})
        if "tp" in self.links:
            for i in range(1, nt):
                count += greet(True, {"tp": lax.rem(t + i, nt)})
        if "dp" in self.links:
            for i in range(1, nd):
                count += greet(True, {"dp": lax.rem(d + i, nd)})
        pl.semaphore_wait(sem, count)

    def run(self):
        n_in, n_out = len(self.ins), len(self.outs)

        def kernel(*refs):
            def get(h):
                kind, i = h
                return refs[i + {"i": 0, "o": n_in, "s": n_in + n_out}[kind]]

            self._barrier()
            live = [g(get) for g in self.tasks]
            while live:
                still = []
                for g in live:
                    try:
                        next(g)
                        still.append(g)
                    except StopIteration:
                        pass
                live = still

        return pl.pallas_call(
            kernel,
            out_shape=[jax.ShapeDtypeStruct(s, t) for s, t, _ in self.outs],
            in_specs=[pl.BlockSpec(memory_space=sp) for _, sp in self.ins],
            out_specs=[pl.BlockSpec(memory_space=sp) for _, _, sp in self.outs],
            scratch_shapes=self.scr,
            compiler_params=pltpu.CompilerParams(
                collective_id=self.cid, has_side_effects=True, vmem_limit_bytes=67_000_000
            ),
            name=self.name,
        )(*[x for x, _ in self.ins])


def remote(src, dst, send, recv, where):
    return pltpu.make_async_remote_copy(
        src_ref=src, dst_ref=dst, send_sem=send, recv_sem=recv, device_id=where, device_id_type=MESH
    )


def when(ok, fn):
    if ok is True:
        fn()
    elif ok is not False:
        pl.when(ok)(fn)


def over_cols(width, fn):
    def body(c, _):
        fn(pl.ds(pl.multiple_of(c * 128, 128), 128))
        return 0

    lax.fori_loop(0, width // 128, body, 0)
    if width % 128:
        fn(pl.ds(width // 128 * 128, width % 128))


def row_encode(read, code, scale, rows):
    step = 16

    def body(i, held):
        r = pl.multiple_of(i * step, step)
        x = read(r, step)
        top = jnp.max(jnp.abs(x), axis=-1, keepdims=True)
        code[pl.ds(r, step), :] = jnp.round(x * (LEVELS / jnp.maximum(top, 1e-30))).astype(jnp.int32).astype(jnp.int16)
        lane = lax.broadcasted_iota(jnp.int32, (step, 128), 1)
        row = lax.broadcasted_iota(jnp.int32, (step, 128), 0) + r
        mine = jnp.sum(jnp.where(lane == row, jnp.maximum(top, 1e-30) * (1.0 / LEVELS), 0.0), axis=0, keepdims=True)
        return held + jnp.broadcast_to(mine, (8, 128))

    scale[...] = lax.fori_loop(0, rows // step, body, jnp.zeros((8, 128), jnp.float32))


def row_decode(code, scale, r, step):
    lane = lax.broadcasted_iota(jnp.int32, (step, 128), 1)
    row = lax.broadcasted_iota(jnp.int32, (step, 128), 0) + r
    col = jnp.sum(jnp.where(lane == row, jnp.broadcast_to(scale[0:1, :], (step, 128)), 0.0), axis=-1, keepdims=True)
    return code[pl.ds(r, step), :].astype(jnp.int32).astype(jnp.float32) * col


def col_encode(x, code, scale, cols):
    top = jnp.maximum(jnp.max(jnp.abs(x), axis=0, keepdims=True), 1e-30)
    code[:, cols] = jnp.round(x * (LEVELS / top)).astype(jnp.int32).astype(jnp.int16)
    scale[:, cols] = top * (1.0 / LEVELS)


def col_decode(code, scale, cols):
    return code[:, cols].astype(jnp.int32).astype(jnp.float32) * scale[:, cols]


class LineGather:
    def __init__(self, st, full, rows, parts):
        self.st, self.full, self.rows, self.parts = st, full, rows, parts
        self.hs = st.scratch(DMA((2, st.nt, parts)))
        self.hr = st.scratch(DMA((2, st.nt, parts)))
        st.links.add("line")

    def bind(self, get):
        self.ref, self.ss, self.rs = get(self.full), get(self.hs), get(self.hr)
        self.t = lax.axis_index("tp")
        return self

    def piece(self, owner, p):
        chunk = self.rows // self.parts
        return self.ref.at[pl.ds(pl.multiple_of(owner * self.rows + p * chunk, chunk), chunk)]

    def hop(self, owner, k, s, p, where):
        at = self.piece(owner, p)
        return remote(at, at, self.ss.at[k, s, p], self.rs.at[k, s, p], {"tp": where})

    def _send(self, s, p, k, way):
        nt, t = self.st.nt, self.t
        owner, where = t - s * way, t + way
        ok = (owner >= 0) & (owner < nt) & (where >= 0) & (where < nt)
        when(ok, lambda: self.hop(owner, k, s, p, where).start())

    def start(self, p):
        for k, way in enumerate((1, -1)):
            self._send(0, p, k, way)

    def arrive(self, s, p):
        nt, t = self.st.nt, self.t
        for k, way in enumerate((1, -1)):
            owner = t - way * (s + 1)
            ok = (owner >= 0) & (owner < nt)
            when(ok, lambda: self.hop(owner, k, s, p, t).wait_recv())
            if s < nt - 2:
                self._send(s + 1, p, k, way)

    def arrive_at(self, v):
        nt, t = self.st.nt, self.t
        s, p = v // self.parts, lax.rem(v, self.parts)
        for k, way in enumerate((1, -1)):
            owner = t - way * (s + 1)
            ok = (owner >= 0) & (owner < nt) & (s < nt - 1)
            where = t + way

            @pl.when(ok)
            def _():
                self.hop(owner, k, s, p, t).wait_recv()
                when((where >= 0) & (where < nt) & (s < nt - 2), lambda: self.hop(owner, k, s + 1, p, where).start())

    def arrivals(self):
        return [
            functools.partial(self.arrive, s, p) for s in range(self.st.nt - 1) for p in range(self.parts)
        ]

    def finish(self):
        nt, t = self.st.nt, self.t
        for s in range(nt - 1):
            for p in range(self.parts):
                for k, way in enumerate((1, -1)):
                    owner, where = t - s * way, t + way
                    ok = (owner >= 0) & (owner < nt) & (where >= 0) & (where < nt)
                    when(ok, lambda: self.hop(owner, k, s, p, where).wait_send())


class LineSum:
    def __init__(self, st, part, rows, width, parts):
        self.st, self.part, self.rows, self.width, self.parts = st, part, rows, width, parts
        nt = st.nt
        self.chunk = rows // parts
        shape = (nt, parts, self.chunk, width)
        self.hc = [st.scratch(VMEM(shape, jnp.int16)) for _ in range(2)]
        self.hk = [st.scratch(VMEM(shape[:2] + (8, 128), jnp.float32)) for _ in range(2)]
        self.hd = [st.scratch(DMA((2, nt, parts))) for _ in range(2)]
        st.links.add("tp")

    def bind(self, get):
        self.x = get(self.part)
        (self.cs, self.cr), (self.sc, self.sr), (self.ss, self.rs) = (
            [get(h) for h in hs] for hs in (self.hc, self.hk, self.hd)
        )
        self.t = lax.axis_index("tp")
        return self

    def far(self, i, j):
        return (jnp.abs(i - j) == 3) if self.st.nt == 4 else (i != i)

    def sends(self, j, p):
        t = self.t
        where = jnp.where(self.far(t, j), jnp.where(j > t, t + 1, t - 1), j)
        slot = jnp.where(self.far(t, j), where, t)
        return (
            remote(self.cs.at[j, p], self.cr.at[slot, p], self.ss.at[0, j, p], self.rs.at[0, slot, p], {"tp": where}),
            remote(self.sc.at[j, p], self.sr.at[slot, p], self.ss.at[1, j, p], self.rs.at[1, slot, p], {"tp": where}),
        )

    def arrival(self, slot, p):
        for k, (x, y) in enumerate(((self.cs, self.cr), (self.sc, self.sr))):
            remote(x.at[slot, p], y.at[slot, p], self.ss.at[k, slot, p], self.rs.at[k, slot, p], {"tp": self.t}).wait_recv()

    def dest(self, o):
        nt, t = self.st.nt, self.t
        if nt != 4:
            return lax.rem(t + 1 + o, nt)
        inner = jnp.where(o == 2, 2, 1 + 2 * o)
        x = jnp.where((t == 0) | (t == nt - 1), 3 - o, inner)
        lo = lax.rem(lax.rem(t, 2) + lax.rem(x, 2), 2)
        return 2 * lax.rem(t // 2 + x // 2, 2) + lo

    def _rows(self, base, r, n):
        return self.x[pl.ds(pl.multiple_of(base + r, n), n), :]

    def send(self, p, produce=None, beside=None):
        nt, t, chunk = self.st.nt, self.t, self.chunk

        def one(o, _):
            j = self.dest(o)
            if produce is not None:
                produce(j)
            base = j * self.rows + p * chunk
            if nt == 4:
                relay = ((t == 1) & (j == 3)) | ((t == 2) & (j == 0))

                @pl.when(relay)
                def _():
                    self.arrival(t, p)
                    row_encode(
                        lambda r, n: self._rows(base, r, n) + row_decode(self.cr.at[t, p], self.sr.at[t, p], r, n),
                        self.cs.at[j, p],
                        self.sc.at[j, p],
                        chunk,
                    )

                plain = jnp.logical_not(relay)
            else:
                plain = True
            when(plain, lambda: row_encode(lambda r, n: self._rows(base, r, n), self.cs.at[j, p], self.sc.at[j, p], chunk))
            for c in self.sends(j, p):
                c.start()
            if beside is not None:
                beside(o)
            return 0

        lax.fori_loop(0, nt - 1, one, 0)

    def total(self, p, put):
        nt, t, chunk = self.st.nt, self.t, self.chunk
        sources = [lax.rem(t + 1 + i, nt) for i in range(nt - 1)]
        for i in sources:
            pl.when(jnp.logical_not(self.far(i, t)))(lambda: self.arrival(i, p))
        base = t * self.rows + p * chunk

        def body(n, _):
            r = pl.multiple_of(n * 16, 16)
            x = self._rows(base, r, 16)
            for i in sources:
                y = row_decode(self.cr.at[i, p], self.sr.at[i, p], r, 16)
                x = x + (jnp.where(self.far(i, t), 0.0, y) if nt == 4 else y)
            put(r, x)
            return 0

        lax.fori_loop(0, chunk // 16, body, 0)

    def finish(self):
        def one(o, _):
            for p in range(self.parts):
                for c in self.sends(self.dest(o), p):
                    c.wait_send()
            return 0

        lax.fori_loop(0, self.st.nt - 1, one, 0)


class ChipGather:
    def __init__(self, st, w, full, rows):
        self.st, self.w, self.full, self.rows = st, w, full, rows
        self.square = st.nd == 8
        self.hops = 4 if self.square else st.nd // 2 - 1
        self.hs, self.hr = (st.scratch(DMA((2 * self.hops + 1,))) for _ in range(2))
        self.hl = st.scratch(DMA((1,)))
        st.links |= {"chips", "twin"}

    def bind(self, get):
        self.x, self.o, self.ss, self.rs, ls = (get(h) for h in (self.w, self.full, self.hs, self.hr, self.hl))
        nd, rows, n = self.st.nd, self.rows, self.hops
        d = lax.axis_index("dp")
        core, chip = lax.rem(d, 2), d // 2
        twin = {"dp": d + 1 - 2 * core}

        def at(i, part=None):
            if part is None:
                return self.o.at[pl.ds(pl.multiple_of(i * rows, rows), rows)]
            return self.o.at[pl.ds(pl.multiple_of(i * rows + part * (rows // 2), rows // 2), rows // 2)]

        beside = [chip + 1 - 2 * lax.rem(chip, 2), lax.rem(chip + 2, 4)]
        near = [2 * c + core for c in beside]
        diagonal = 2 * lax.rem(beside[0] + 2, 4) + core

        def came(i):
            if not self.square:
                return at(lax.rem(d - 2 * i - 2 + nd, nd))
            return at(near[i]) if i < 2 else at(diagonal, i - 2)

        def hop(i):
            if not self.square:
                src, dst, where = self.x, at(d), lax.rem(d + 2 * i + 2, nd)
            elif i < 2:
                src, dst, where = self.x, at(d), near[i]
            else:
                src = dst = at(near[i - 2], i - 2)
                where = near[3 - i]
            return remote(src, dst, self.ss.at[i], self.rs.at[i], {"dp": where})

        def landed(i):
            return remote(came(i), came(i), self.ss.at[i], self.rs.at[i], twin)

        def give(i):
            src, dst = (self.x, at(d)) if i == 0 else (came(i - 1), came(i - 1))
            return remote(src, dst, self.ss.at[n + i], self.rs.at[n + i], twin)

        self.own = lambda: pltpu.make_async_copy(self.x, at(d), ls.at[0])
        self.hop, self.landed, self.give = hop, landed, give
        return self

    def start(self):
        for i in range(2 if self.square else self.hops):
            self.hop(i).start()
        self.give(0).start()
        self.own().start()

    def forward(self, i):
        self.landed(i).wait_recv()
        if self.square and i < 2:
            self.hop(i + 2).start()
        self.give(i + 1).start()

    def forwards(self):
        return [functools.partial(self.forward, i) for i in range(self.hops)]

    def arrived(self):
        for i in range(self.hops + 1):
            self.give(i).wait_recv()
        self.own().wait()

    def finish(self):
        for i in range(self.hops + 1):
            self.give(i).wait_send()
        for i in range(self.hops):
            self.hop(i).wait_send()


class GradScatter:
    def __init__(self, st, shard, widths, sums):
        nc = self.nc = st.nd // 2
        self.st, self.shard, self.widths = st, shard, widths
        self.m = math.lcm(2 * shard, 128) // (2 * shard)
        self.chunks = nc // self.m
        self.padded = [-(-w // 128) * 128 for w in widths]
        wide = max(self.padded)
        self.hg = st.scratch(VMEM((2, 2 * self.m * shard, wide), jnp.float32))
        self.ht = st.scratch(VMEM((2, self.m, shard, wide), jnp.float32))
        self.slots = self.chunks - (self.m == 1)
        self.hs = st.scratch(VMEM((self.slots, self.m, shard, wide), jnp.int16))
        self.hk = st.scratch(VMEM((self.slots, self.m, 1, wide), jnp.float32))
        self.hcr = [st.scratch(VMEM((nc - 1, shard, w), jnp.int16)) for w in self.padded]
        self.hkr = [st.scratch(VMEM((nc - 1, 1, w), jnp.float32)) for w in self.padded]
        self.ha = sums
        self.hgs = [st.scratch(DMA((2, self.m))) for _ in range(2)]
        self.hss = st.scratch(DMA((2, self.slots, self.m)))
        self.hsr = st.scratch(DMA((len(widths), 2, nc - 1)))
        self.hf = st.scratch(pltpu.SemaphoreType.REGULAR)
        st.links |= {"chips", "twin"}

    def bind(self, get):
        self.g, self.t, self.cs, self.sc, self.ss, self.sr, self.free = (
            get(h) for h in (self.hg, self.ht, self.hs, self.hk, self.hss, self.hsr, self.hf)
        )
        self.cr, self.kr, self.acc = ([get(h) for h in hs] for hs in (self.hcr, self.hkr, self.ha))
        self.gs, self.gr = (get(h) for h in self.hgs)
        d = self.d = lax.axis_index("dp")
        self.core, self.chip = lax.rem(d, 2), d // 2
        self.twin = {"dp": d + 1 - 2 * self.core}
        return self

    def chunk(self, i):
        return lax.rem(self.chip // self.m + 1 + i, self.chunks)

    def half(self, e, core):
        return pl.ds(pl.multiple_of((2 * e + core) * self.shard, self.shard), self.shard)

    def gift(self, a, r, e):
        cols = pl.ds(0, self.padded[a])
        return remote(
            self.g.at[r, self.half(e, 1 - self.core), cols], self.t.at[r, e, :, cols], self.gs.at[r, e], self.gr.at[r, e],
            self.twin,
        )

    def sums(self, a, i, e, dest):
        cols, nc = pl.ds(0, self.padded[a]), self.nc
        slot = jnp.maximum(lax.rem(dest - self.chip + nc, nc) - 1, 0)
        where = {"dp": 2 * dest + self.core}
        return (
            remote(self.cs.at[i, e, :, cols], self.cr[a].at[slot], self.ss.at[0, i, e], self.sr.at[a, 0, slot], where),
            remote(self.sc.at[i, e, :, cols], self.kr[a].at[slot], self.ss.at[1, i, e], self.sr.at[a, 1, slot], where),
        )

    def compute(self, a, i, pieces):
        n = a * self.chunks + i
        r = lax.rem(n, 2)
        rows = 2 * self.m * self.shard

        @pl.when(n >= 2)
        def _():
            for e in range(self.m):
                self.gift(a, r, e).wait_send() if a == 0 else self._sent(a, i, r, e)
            pl.semaphore_wait(self.free, 1)

        cols = pl.ds(pl.multiple_of(self.chunk(i) * rows, 128), rows)
        at = 0
        for x, y in pieces:
            z = y()
            self.g[r, :, at : at + z.shape[1]] = tn_dot(x[:, cols], z)
            at += z.shape[1]
        for e in range(self.m):
            self.gift(a, r, e).start()

    def _sent(self, a, i, r, e):
        pl.when(i >= 2)(lambda: self.gift(a, r, e).wait_send())
        pl.when(i < 2)(lambda: self.gift(a - 1, r, e).wait_send())

    def combine(self, a, i):
        n = a * self.chunks + i
        r = lax.rem(n, 2)
        for e in range(self.m):
            self.gift(a, r, e).wait_recv()
            dest = self.chunk(i) * self.m + e
            away = dest != self.chip
            own = self.half(e, self.core)

            @pl.when(away)
            def _():
                if a:
                    for c in self.sums(a - 1, i, e, dest):
                        c.wait_send()
                over_cols(
                    self.widths[a],
                    lambda cols: col_encode(
                        self.g[r, own, cols] + self.t[r, e, :, cols], self.cs.at[i, e], self.sc.at[i, e], cols
                    ),
                )
                for c in self.sums(a, i, e, dest):
                    c.start()

            @pl.when(jnp.logical_not(away))
            def _():
                over_cols(self.widths[a], lambda cols: self._keep(a, r, e, own, cols))

        @pl.when(n + 2 < len(self.widths) * self.chunks)
        def _():
            pl.semaphore_signal(self.free, inc=1, device_id=self.twin, device_id_type=MESH)

    def _keep(self, a, r, e, own, cols):
        self.acc[a][:, cols] = self.g[r, own, cols] + self.t[r, e, :, cols]

    def slot(self, a, w, pieces):
        pl.when(w < self.chunks)(lambda: self.compute(a, w, pieces))
        pl.when((w >= 1) & (w <= self.chunks))(lambda: self.combine(a, w - 1))

    def collect(self, a, put):
        n = self.nc - 1
        for i in range(n):
            for c in self.sums(a, 0, 0, lax.rem(self.chip + 1 + i, self.nc)):
                c.wait_recv()

        def tile(cols):
            x = self.acc[a][:, cols]
            for i in range(n):
                x = x + col_decode(self.cr[a].at[i], self.kr[a].at[i], cols)
            put(cols, x)

        over_cols(self.widths[a], tile)

    def finish(self):
        a = len(self.widths) - 1
        for i in range(self.chunks):
            for e in range(self.m):
                if i >= self.chunks - 2:
                    self.gift(a, (a * self.chunks + i) % 2, e).wait_send()
                if i < self.slots:
                    dest = self.chunk(i) * self.m + e

                    @pl.when(dest != self.chip)
                    def _():
                        for c in self.sums(a, i, e, dest):
                            c.wait_send()


class FullSum:
    def __init__(self, st, x, out, shape):
        self.st, self.x, self.out = st, x, out
        self.ha = st.scratch(VMEM((st.nt,) + shape, jnp.float32))
        self.hm = st.scratch(VMEM(shape, jnp.float32))
        self.hb = st.scratch(VMEM((st.nd,) + shape, jnp.float32))
        self.hs = st.scratch(DMA((2, max(st.nd, st.nt))))
        self.hr = st.scratch(DMA((2, max(st.nd, st.nt))))
        st.links |= {"tp", "dp"}

    def run(self, get):
        nd, nt = self.st.nd, self.st.nt
        x, o, a, m, b, ss, rs = (get(h) for h in (self.x, self.out, self.ha, self.hm, self.hb, self.hs, self.hr))
        for k, (axis, n, src, got, dst) in enumerate((("tp", nt, x, a, m), ("dp", nd, m, b, o))):
            me = lax.axis_index(axis)
            cs = [
                remote(src, got.at[me], ss.at[k, i], rs.at[k, i], {axis: lax.rem(me + i, n)}) for i in range(1, n)
            ]
            for c in cs:
                c.start()
            got[me] = src[...]
            for c in cs:
                c.wait()
            total = got[0]
            for i in range(1, n):
                total = total + got[i]
            dst[...] = total


def lane_take(x, offset):
    base = offset // 128 * 128
    wide = min(256, x.shape[-1] - base)
    slab = x[:, base : base + wide]
    if wide % 128:
        slab = jnp.concatenate([slab, jnp.zeros((x.shape[0], -wide % 128), x.dtype)], axis=1)
        wide = slab.shape[-1]
    if offset > base:
        slab = pltpu.roll(slab, wide - (offset - base), 1)
    slab = slab[:, :128]
    return jnp.where(lax.broadcasted_iota(jnp.int32, slab.shape, 1) < HD, slab, 0.0)


def lane_place(x, offset, width):
    base = offset // 128 * 128
    wide = min(256, width - base)
    slab = x if wide == 128 else jnp.concatenate([x, jnp.zeros_like(x)], axis=1)
    if offset > base:
        slab = pltpu.roll(slab, offset - base, 1)
    slab = slab[:, :wide]
    pieces = []
    if base:
        pieces.append(jnp.zeros((x.shape[0], base), x.dtype))
    pieces.append(slab)
    if base + wide < width:
        pieces.append(jnp.zeros((x.shape[0], width - base - wide), x.dtype))
    return jnp.concatenate(pieces, axis=1) if len(pieces) > 1 else slab


def turned(u, cosine, sine):
    wide = u.shape[-1]
    lane = lax.rem(lax.broadcasted_iota(jnp.int32, u.shape, 1), HD)
    swap = jnp.where(lane < HD // 2, pltpu.roll(u, wide - HD // 2, 1), pltpu.roll(u, HD // 2, 1))
    return u * cosine + swap * sine


def nt_dot(a, b):
    return lax.dot_general(a, b, (((1,), (1,)), ((), ())), preferred_element_type=jnp.float32)


def per_tile(count, size, fn):
    def body(i, _):
        fn(pl.multiple_of(i * size, size))
        return 0

    lax.fori_loop(0, count, body, 0)


def in_turn(*lists):
    for i in range(max(len(x) for x in lists)):
        for x in lists:
            if i < len(x):
                x[i]()


class Fused(Stage):
    def body(self, fn):
        self.tasks = [lambda get: iter(fn(get) or ())]


def inverse_rms(x):
    return lax.rsqrt(jnp.mean(x * x, axis=-1, keepdims=True) + norm_eps)


def tn_dot(a, b):
    return lax.dot_general(a, b, (((0,), (0,)), ((), ())), preferred_element_type=jnp.float32)


def across(x, count):
    return jnp.concatenate([x] * count, axis=1) if count > 1 else x


def masked_scores(keys, queries, first, begin, span, group):
    s = nt_dot(keys, queries) * (1.0 / math.sqrt(HD))
    key = lax.broadcasted_iota(jnp.int32, s.shape, 0) + first
    own = lax.rem(lax.broadcasted_iota(jnp.int32, s.shape, 1), 128) + (first + 2 * span)
    return s, (key >= across(begin, group)) & (key <= own)


def layer(
    nd, nt, tokens, attn_gain, ffn_gain, out_grad, begin, cosine, sine, w_attn, w_gate, w_up, w_down_t, heads
):
    st = Fused("layer", 1, nd, nt)
    low, f32 = jnp.bfloat16, jnp.float32
    own, width = tokens.shape
    span = own * nt
    shard, units = w_gate.shape
    n_q, n_kv = heads
    group = n_q // n_kv
    tiles = span // 128
    qw, kvw = n_q * HD, n_kv * HD
    qkvw = qw + 2 * kvw
    reach = 2 * span + 128
    parts = 2
    piece = own // parts
    scale = 1.0 / math.sqrt(HD)

    h_tok, h_g1, h_g2 = st.inp(tokens), st.inp(attn_gain[None]), st.inp(ffn_gain[None])
    h_og, h_begin = st.inp(out_grad), st.inp(begin)
    h_cos, h_sin = st.inp(cosine), st.inp(sine)
    s_wa, s_wg, s_wu, s_wd = (st.inp(w, pl.ANY) for w in (w_attn, w_gate, w_up, w_down_t))

    o_out = st.out((own, width), low)
    o_tg = st.out((own, width), f32)
    o_gains = st.out((1, 2 * width), f32)
    o_dd, o_dg, o_du = (st.out((shard, units), f32) for _ in range(3))
    o_da, o_db = (st.out((shard, w), f32) for w in (2 * qw, 2 * kvw))

    def room(shape, dtype=f32):
        return st.scratch(VMEM(shape, dtype))

    h_h1, h_h2, h_gr, h_rl = (room((span, width), low) for _ in range(4))
    h_wa = room((width, qkvw + qw), low)
    h_wg, h_wu, h_wd = (room((width, units), low) for _ in range(3))
    h_q, h_dc, h_ch = (room((n_kv, tiles, group * 128, 128), low) for _ in range(3))
    h_k, h_v = (room((n_kv, 3 * span, 128), low) for _ in range(2))
    h_vt = room((n_kv, 128, 3 * span), low)
    h_win = room((3, span, 2 * kvw), low)
    h_ctx = room((span, qw), low)
    h_lse, h_delta = (room((n_kv, tiles, 1, group * 128)) for _ in range(2))
    h_res, h_rg = (room((own, width)) for _ in range(2))
    h_part = room((span, width))
    h_ia, h_gl, h_ul = (room((span, units), low) for _ in range(3))
    h_dq = room((n_kv, tiles, group * 128, 128))
    h_dk, h_dv = (room((n_kv, 3 * span, 128)) for _ in range(2))
    h_kvs, h_kvr = (room((2, span, 2 * kvw), jnp.int16) for _ in range(2))
    h_kss, h_ksr = (room((2, tiles, 1, 2 * kvw)) for _ in range(2))
    h_mine = room((1, 2 * width))
    h_fs, h_fr = (st.scratch(DMA((2,))) for _ in range(2))
    h_bs, h_br = (st.scratch(DMA((2, 2))) for _ in range(2))
    h_ready = st.scratch(pltpu.SemaphoreType.REGULAR)

    ag1 = LineGather(st, h_h1, own, parts)
    ag2 = LineGather(st, h_h2, own, parts)
    ag3 = LineGather(st, h_gr, own, parts)
    ag4 = LineGather(st, h_rl, own, parts)
    rs = LineSum(st, h_part, own, width, parts)
    wa = ChipGather(st, s_wa, h_wa, shard)
    wg = ChipGather(st, s_wg, h_wg, shard)
    wu = ChipGather(st, s_wu, h_wu, shard)
    wd = ChipGather(st, s_wd, h_wd, shard)
    gs = GradScatter(st, shard, (units, units, units, 2 * qw, 2 * kvw), (o_dd, o_dg, o_du, o_da, o_db))
    full = FullSum(st, h_mine, o_gains, (1, 2 * width))
    st.links.add("near")

    def fn(get):
        d, t = lax.axis_index("dp"), lax.axis_index("tp")
        for x in (ag1, ag2, ag3, ag4, rs, wa, wg, wu, wd, gs):
            x.bind(get)
        tok, g1, g2, og, begin_ref, cos_ref, sin_ref = (get(h) for h in (h_tok, h_g1, h_g2, h_og, h_begin, h_cos, h_sin))
        h1, h2, gr, rl = (get(h) for h in (h_h1, h_h2, h_gr, h_rl))
        wa_ref, wg_ref, wu_ref, wd_ref = (get(h) for h in (h_wa, h_wg, h_wu, h_wd))
        q, k, v, vt, win, ctx, ch, lse = (get(h) for h in (h_q, h_k, h_v, h_vt, h_win, h_ctx, h_ch, h_lse))
        dc, delta, dq, dk, dv = (get(h) for h in (h_dc, h_delta, h_dq, h_dk, h_dv))
        res, rg, part, ia, gl, ul, mine = (get(h) for h in (h_res, h_rg, h_part, h_ia, h_gl, h_ul, h_mine))
        xl = ul.at[:, pl.ds(0, qkvw)]
        kvs, kvr, kss, ksr, fs, fr, bs, br = (
            get(h) for h in (h_kvs, h_kvr, h_kss, h_ksr, h_fs, h_fr, h_bs, h_br)
        )

        def own_rows(p, r, n=16):
            return pl.ds(pl.multiple_of(t * own + p * piece + r, n), n)

        def rows_of(j):
            return pl.ds(pl.multiple_of(j * own, own), own)

        wa.start()
        wd.start()
        for p in range(parts):

            def tile(r):
                x = tok[pl.ds(p * piece + r, 16), :].astype(f32)
                h1[own_rows(p, r), :] = (x * inverse_rms(x) * g1[...]).astype(low)

            per_tile(piece // 16, 16, tile)
            ag1.start(p)
        gr[rows_of(t), :] = og[...]
        pass_a, pass_d, pass_g, pass_u = (x.forwards() for x in (wa, wd, wg, wu))
        in_turn(ag1.arrivals(), pass_a[:2] + pass_d[:2] + pass_a[2:])
        for p in range(parts):
            ag3.start(p)
        wa.arrived()

        def turn_rows(x, rows, way):
            cosine, sine = across(cos_ref[rows, :], 2), across(sin_ref[rows, :], 2)
            lane = lax.broadcasted_iota(jnp.int32, x.shape, 1)
            return jnp.where(lane < qw + kvw, turned(x, cosine, way * sine), x)

        def project(r):
            rows = pl.ds(r, 128)
            x = turn_rows(dot(h1[rows, :], wa_ref[:, :qkvw]), rows, 1.0)
            for h in range(n_q):
                q[h // group, r // 128, h % group * 128 : (h % group + 1) * 128, :] = lane_take(x, h * HD).astype(low)
            win[2, rows, :] = x[:, qw:].astype(low)

        per_tile(tiles, 128, project)

        def ahead(i):
            return remote(win.at[2], win.at[2 - i], fs.at[i - 1], fr.at[i - 1], {"dp": d + i})

        for i in (2, 1):
            when(d + i < nd, lambda: ahead(i).start())

        def unpack(b):
            def tile(r):
                x = win[b, pl.ds(r, 128), :].astype(f32)
                at = pl.ds(pl.multiple_of(b * span + r, 128), 128)
                for g in range(n_kv):
                    k[g, at, :] = lane_take(x, g * HD).astype(low)
                    y = lane_take(x, kvw + g * HD)
                    v[g, at, :] = y.astype(low)
                    vt[g, :, at] = y.T.astype(low)

            per_tile(tiles, 128, tile)

        unpack(2)
        for x in pass_d[2:]:
            x()
        for i in (1, 2):

            @pl.when(d < i)
            def _():
                win[2 - i] = jnp.zeros((span, 2 * kvw), low)

            when(d >= i, lambda: ahead(i).wait_recv())
            unpack(2 - i)
        wg.start()
        wu.start()

        def attend(u, _):
            g, i = u // tiles, lax.rem(u, tiles)
            at = pl.multiple_of(i * 128, 128)
            keys = pl.ds(at, reach)
            s, seen = masked_scores(k[g, keys, :], q[g, i], at, begin_ref[:, pl.ds(at, 128)], span, group)
            s = jnp.where(seen, s, masked_score)
            top = jnp.max(s, axis=0, keepdims=True)
            e = jnp.exp(s - top)
            total = jnp.sum(e, axis=0, keepdims=True)
            p = (e * (1.0 / total)).astype(low)
            lse[g, i] = top + jnp.log(total)
            ch[g, i] = dot(vt[g, :, keys], p).T.astype(low)
            return 0

        half = max(1, n_kv * tiles // 2)
        arrive3 = ag3.arrivals()
        lax.fori_loop(0, half, attend, 0)
        cut = len(arrive3) // 2
        in_turn(arrive3[:cut], pass_g[:2])
        lax.fori_loop(half, n_kv * tiles, attend, 0)
        in_turn(arrive3[cut:], pass_u[:2])

        def pack(r):
            x = 0.0
            for h in range(n_q):
                at = h % group * 128
                x = x + lane_place(ch[h // group, r // 128, at : at + 128, :].astype(f32), h * HD, qw)
            ctx[pl.ds(r, 128), :] = x.astype(low)

        per_tile(tiles, 128, pack)

        def out_rows(j):
            for c in range(0, width, 512):
                part[rows_of(j), c : c + 512] = nt_dot(ctx[rows_of(j), :], wa_ref[c : c + 512, qkvw:])

        rs.send(0, out_rows)
        rs.send(1)
        out_rows(t)
        kt = vt

        def keys_back(r):
            for g in range(n_kv):
                kt[g, :, pl.ds(r, 128)] = k[g, pl.ds(r, 128), :].T

        per_tile(3 * tiles, 128, keys_back)
        in_turn(pass_g[2:], pass_u[2:])

        for p in range(parts):

            def put(r, x):
                at = pl.ds(p * piece + r, 16)
                x = x + tok[at, :].astype(f32)
                res[at, :] = x
                h2[own_rows(p, r), :] = (x * inverse_rms(x) * g2[...]).astype(low)

            rs.total(p, put)
            ag2.start(p)
        wd.arrived()

        def back_act(c):
            part[:, pl.ds(c, 512)] = dot(gr[...], wd_ref[:, pl.ds(c, 512)])

        arrive2 = ag2.arrivals()
        for x in arrive2[:parts]:
            x()
        per_tile(units // 512, 512, back_act)
        for x in arrive2[parts:]:
            x()
        wg.arrived()
        wu.arrived()

        def act(c):
            cols = pl.ds(c, 256)
            gate = dot(h2[...], wg_ref[:, cols])
            up = dot(h2[...], wu_ref[:, cols])
            back = part[:, cols]
            sig = jax.nn.sigmoid(gate)
            ia[:, cols] = (gate * sig * up).astype(low)
            gl[:, cols] = (back * up * (sig * (1.0 + gate * (1.0 - sig)))).astype(low)
            ul[:, cols] = (back * gate * sig).astype(low)

        per_tile(units // 256, 256, act)

        def rows_back(j):
            rows = rows_of(j)
            for c in range(0, width, 512):
                part[rows, c : c + 512] = nt_dot(gl[rows, :], wg_ref[c : c + 512, :]) + nt_dot(
                    ul[rows, :], wu_ref[c : c + 512, :]
                )

        last_slot = gs.chunks + 1
        grads = (
            ((gr, lambda: ia[...]),),
            ((h2, lambda: gl[...]),),
            ((h2, lambda: ul[...]),),
            ((h1, lambda: xl[:, :qw]), (rl, lambda: ctx[...])),
            ((h1, lambda: xl[:, qw:]),),
        )

        def weight_grads(a, first=0):
            def one(w, _):
                gs.slot(a, w, grads[a])
                return 0

            lax.fori_loop(first, last_slot, one, 0)

        rs.finish()
        rs.send(0, rows_back, lambda o: gs.slot(0, o, grads[0]))
        rs.send(1)
        rows_back(t)
        weight_grads(0, nt - 1)
        mine[...] = jnp.zeros_like(mine)

        for p in range(parts):

            def put(r, x):
                at = pl.ds(p * piece + r, 16)
                y = res[at, :]
                inverse = inverse_rms(y)
                normed = y * inverse
                mine[:, width:] += jnp.sum(x * normed, axis=0, keepdims=True)
                e = x * g2[...]
                back = inverse * (e - normed * jnp.mean(e * normed, axis=-1, keepdims=True))
                y = og[at, :].astype(f32) + back
                rg[at, :] = y
                rl[own_rows(p, r), :] = y.astype(low)

            rs.total(p, put)
            ag4.start(p)

        def ffn_rows(r):
            cols = pl.ds(r, 512)
            part[:, cols] = nt_dot(ia[...], wd_ref[cols, :])

        def while_gathered(w, _):
            ag4.arrive_at(w)
            pl.when(w < width // 512)(lambda: ffn_rows(pl.multiple_of(w * 512, 512)))
            gs.slot(1, w, grads[1])
            return 0

        lax.fori_loop(0, max((nt - 1) * parts, last_slot, width // 512), while_gathered, 0)

        def context_back(r):
            x = dot(rl[pl.ds(r, 128), :], wa_ref[:, qkvw:])
            i = r // 128
            for h in range(n_q):
                g, at = h // group, pl.ds(h % group * 128, 128)
                y = lane_take(x, h * HD).astype(low)
                dc[g, i, at, :] = y
                z = y.astype(f32) * ch[g, i, at, :].astype(f32)
                delta[g, i, :, at] = jnp.sum(z.T, axis=0, keepdims=True)

        rs.finish()
        for p in range(parts):
            rs.send(p)
        per_tile(tiles, 128, context_back)
        dk[...] = jnp.zeros_like(dk)
        dv[...] = jnp.zeros_like(dv)
        count = n_kv * tiles

        def attend_back(u, _):
            g, i = u // tiles, lax.rem(u, tiles)
            at = pl.multiple_of(i * 128, 128)
            keys = pl.ds(at, reach)
            qq, dd = q[g, i], dc[g, i]
            s, seen = masked_scores(k[g, keys, :], qq, at, begin_ref[:, pl.ds(at, 128)], span, group)
            p = jnp.where(seen, jnp.exp(s - lse[g, i]), 0.0)
            ds = (p * (nt_dot(v[g, keys, :], dd) - delta[g, i])).astype(low)
            dv[g, keys, :] += dot(p.astype(low), dd)
            dk[g, keys, :] += dot(ds, qq)
            dq[g, i] = dot(kt[g, :, keys], ds).T
            gs.slot(2, u, grads[2])
            return 0

        lax.fori_loop(0, count, attend_back, 0)
        weight_grads(2, count)

        def kv_rows(b, r):
            at = pl.ds(pl.multiple_of(b * span + r, 128), 128)
            x = 0.0
            for g in range(n_kv):
                x = x + lane_place(dk[g, at, :] * scale, g * HD, 2 * kvw)
                x = x + lane_place(dv[g, at, :], kvw + g * HD, 2 * kvw)
            return x

        def behind(i):
            where = {"dp": d - i}
            return (
                remote(kvs.at[i - 1], kvr.at[i - 1], bs.at[0, i - 1], br.at[0, i - 1], where),
                remote(kss.at[i - 1], ksr.at[i - 1], bs.at[1, i - 1], br.at[1, i - 1], where),
            )

        for i in (2, 1):

            @pl.when(d >= i)
            def _():
                def tile(r):
                    at = kvs.at[i - 1, pl.ds(r, 128)]
                    col_encode(kv_rows(2 - i, r), at, kss.at[i - 1, r // 128], slice(None))

                per_tile(tiles, 128, tile)
                for c in behind(i):
                    c.start()

        def query_rows(r):
            rows = pl.ds(r, 128)
            x = 0.0
            for h in range(n_q):
                at = h % group * 128
                x = x + lane_place(dq[h // group, r // 128, at : at + 128, :] * scale, h * HD, qw)
            pad = jnp.zeros((128, 2 * kvw), f32)
            xl[rows, :] = turn_rows(jnp.concatenate([x, pad], axis=1), rows, -1.0).astype(low)

        per_tile(tiles, 128, query_rows)
        for p in range(parts):

            def put(r, x):
                at = pl.ds(p * piece + r, 16)
                get(o_out)[at, :] = (res[at, :] + x).astype(low)

            rs.total(p, put)
        ready = get(h_ready)
        for i in range(1, nt):
            pl.semaphore_signal(ready, inc=1, device_id={"tp": lax.rem(t + i, nt)}, device_id_type=MESH)

        def put_down(cols, x):
            get(o_dd)[:, cols] = x

        def put_gate(cols, x):
            get(o_dg)[:, cols] = x

        def put_up(cols, x):
            get(o_du)[:, cols] = x

        def put_query(cols, x):
            get(o_da)[:, cols] = x

        def put_key(cols, x):
            get(o_db)[:, cols] = x

        gs.collect(0, put_down)
        gs.collect(1, put_gate)
        gs.collect(2, put_up)
        weight_grads(3)
        for i in (1, 2):

            @pl.when(d + i < nd)
            def _():
                for c in behind(i):
                    c.wait_recv()

        near1, near2 = d + 1 < nd, d + 2 < nd

        def kv_total(r):
            rows = pl.ds(r, 128)
            x = kv_rows(2, r)
            a = col_decode(kvr.at[0, rows], ksr.at[0, r // 128], slice(None))
            b = col_decode(kvr.at[1, rows], ksr.at[1, r // 128], slice(None))
            x = x + jnp.where(near1, a, 0.0) + jnp.where(near2, b, 0.0)
            pad = jnp.zeros((128, qw), f32)
            x = turn_rows(jnp.concatenate([pad, x], axis=1), rows, -1.0)
            xl[rows, qw:] = x[:, qw:].astype(low)

        per_tile(tiles, 128, kv_total)

        def hidden_rows(j):
            for c in range(0, width, 512):
                part[rows_of(j), c : c + 512] = nt_dot(xl[rows_of(j), :], wa_ref[c : c + 512, :qkvw])

        rs.finish()
        pl.semaphore_wait(ready, nt - 1)
        rs.send(0, hidden_rows)
        rs.send(1)
        hidden_rows(t)
        weight_grads(4)

        for p in range(parts):

            def put(r, x):
                at = pl.ds(p * piece + r, 16)
                y = tok[at, :].astype(f32)
                inverse = inverse_rms(y)
                normed = y * inverse
                mine[:, :width] += jnp.sum(x * normed, axis=0, keepdims=True)
                e = x * g1[...]
                e = inverse * (e - normed * jnp.mean(e * normed, axis=-1, keepdims=True))
                get(o_tg)[at, :] = rg[at, :] + e

            rs.total(p, put)
        full.run(get)
        gs.collect(3, put_query)
        gs.collect(4, put_key)
        for x in (ag1, ag2, ag3, ag4, rs, wa, wg, wu, wd, gs):
            x.finish()
        for i in (2, 1):
            when(d + i < nd, lambda: ahead(i).wait_send())

            @pl.when(d >= i)
            def _():
                for c in behind(i):
                    c.wait_send()

    st.body(fn)
    return st.run()


def rope_tables(position_ids, head_size):
    half_size = head_size // 2
    inverse = rope_base ** (-(jnp.arange(half_size, dtype=jnp.float32) * 2.0 / head_size))
    angles = position_ids.astype(jnp.float32)[:, None] * inverse[None, :]
    return (jnp.cos(angles), jnp.sin(angles))


def dot(a, b):
    return jnp.dot(a, b, preferred_element_type=jnp.float32)


def finished(output, tokens_grad, down_sum, gate_sum, up_sum, query_sum, key_sum):
    shard, qw, kvw = query_sum.shape[0], query_sum.shape[1] // 2, key_sum.shape[1] // 2

    def columns(x, at, n):
        base = at // 128 * 128
        slab = x[:, base : base + -(-(at - base + n) // 128) * 128]
        if slab.shape[1] % 128:
            slab = jnp.concatenate([slab, jnp.zeros((shard, -slab.shape[1] % 128), slab.dtype)], axis=1)
        if at > base:
            slab = pltpu.roll(slab, slab.shape[1] - (at - base), 1)
        return slab[:, :n]

    def kernel(*refs):
        (*same, qs, ks), outs = refs[:7], refs[7:]
        for src, dst in zip(same, outs):
            dst[...] = src[...]
        q, k, v, o = outs[5:]
        q[...] = qs[:, :qw]
        o[...] = columns(qs, qw, qw)
        k[...] = ks[:, :kvw]
        v[...] = columns(ks, kvw, kvw)

    like = [output, tokens_grad, down_sum, gate_sum, up_sum]
    shapes = [(x.shape, x.dtype) for x in like]
    shapes += [((shard, qw), jnp.float32), ((shard, kvw), jnp.float32), ((shard, kvw), jnp.float32), ((shard, qw), jnp.float32)]
    return pl.pallas_call(
        kernel,
        out_shape=[jax.ShapeDtypeStruct(*x) for x in shapes],
        in_specs=[pl.BlockSpec(memory_space=VMEM)] * 7,
        out_specs=[pl.BlockSpec(memory_space=VMEM)] * 9,
        compiler_params=pltpu.CompilerParams(vmem_limit_bytes=66_000_000),
        name="finish",
    )(*like, query_sum, key_sum)


def on_device(
    nd, nt, tokens, positions, attn_gain, w_query, w_key, w_value, w_out, ffn_gain, w_gate, w_up, w_down, out_grad
):
    span = tokens.shape[0] * nt
    width = tokens.shape[1]
    heads = (w_query.shape[1] // HD, w_key.shape[1] // HD)
    qw, kvw = w_query.shape[1], w_key.shape[1]
    w_attn = jnp.concatenate([w_query, w_key, w_value, w_out.T], axis=1)
    w_down_t = w_down.T
    cosine, sine = rope_tables(positions, HD)
    cosine = jnp.tile(cosine, (1, 2 * heads[0]))
    sine = jnp.tile(jnp.concatenate([-sine, sine], axis=1), (1, heads[0]))
    begin = (2 * span + jnp.arange(span, dtype=jnp.int32) - positions)[None]
    output, tokens_grad, gains, down_sum, gate_sum, up_sum, query_sum, key_sum = layer(
        nd, nt, tokens, attn_gain, ffn_gain, out_grad, begin, cosine, sine, w_attn, w_gate, w_up, w_down_t, heads
    )
    output, tokens_grad, down_sum, gate_sum, up_sum, wq, wk, wv, wo = finished(
        output, tokens_grad, down_sum, gate_sum, up_sum, query_sum, key_sum
    )
    return (output, tokens_grad, gains[0, :width], wq, wk, wv, wo.T, gains[0, width:], gate_sum, up_sum, down_sum.T)


def solution(mesh):
    return jax.shard_map(
        functools.partial(on_device, mesh.shape["dp"], mesh.shape["tp"]),
        mesh=mesh,
        in_specs=(
            P(("dp", "tp"), None),
            P("dp"),
            P(),
            P("dp", "tp"),
            P("dp", "tp"),
            P("dp", "tp"),
            P("tp", "dp"),
            P(),
            P("dp", "tp"),
            P("dp", "tp"),
            P("tp", "dp"),
            P(("dp", "tp"), None),
        ),
        out_specs=(
            P(("dp", "tp"), None),
            P(("dp", "tp"), None),
            P(),
            P("dp", "tp"),
            P("dp", "tp"),
            P("dp", "tp"),
            P("tp", "dp"),
            P(),
            P("dp", "tp"),
            P("dp", "tp"),
            P("tp", "dp"),
        ),
        check_vma=False,
    )
```
